8 devices in a mesh: data: 2 (over z, y), model: 4 (over x, core).
Axes of the slice: x: 2, y: 2, z: 1, core: 2. Of those that a mesh axis runs over, the one named last changes fastest.
Arguments:
- x_saved: bfloat16 [2, 32, 2048, 768], P(None, 'data', 'model')
- h_saved: bfloat16 [2, 32, 2048, 3072], P(None, 'data', None, 'model')
- w_up: bfloat16 [2, 768, 3072], P(None, None, 'model')
- w_down: bfloat16 [2, 3072, 768], P(None, 'model')
- grad_out: bfloat16 [32, 2048, 768], P('data', 'model')
Outputs:
- output 1: bfloat16 [32, 2048, 768], P('data', 'model')
- output 2: float32 [2, 768, 3072], P(None, None, 'model')
- output 3: float32 [2, 3072, 768], P(None, 'model')
All inputs are finite; a program needn't handle non-finite values.
Results may differ from the reference program's by a relative error of at most 0.0126265.
Values are sent between devices in bfloat16 or wider.
A program may use at most 1 GiB of HBM per device.

```python
import jax
import jax.numpy as jnp
from jax import lax

HIDDEN = 768
FFN_DIM = 3072
BATCH_SIZE = 32
SEQ_LEN = 2048
LAYERS = 2


def setup_inputs(seed: int = 0) -> dict:
    keys = jax.random.split(jax.random.key(seed), 5)
    x_saved = jax.random.normal(keys[0], (LAYERS, BATCH_SIZE, SEQ_LEN, HIDDEN), jnp.float32)
    h_saved = jax.random.normal(keys[1], (LAYERS, BATCH_SIZE, SEQ_LEN, FFN_DIM), jnp.float32)
    w_up = jax.random.normal(keys[2], (LAYERS, HIDDEN, FFN_DIM), jnp.float32) * HIDDEN ** -0.5
    w_down = jax.random.normal(keys[3], (LAYERS, FFN_DIM, HIDDEN), jnp.float32) * FFN_DIM ** -0.5
    grad_out = jax.random.normal(keys[4], (BATCH_SIZE, SEQ_LEN, HIDDEN), jnp.float32)
    return {
        "x_saved": x_saved.astype(jnp.bfloat16),
        "h_saved": h_saved.astype(jnp.bfloat16),
        "w_up": w_up.astype(jnp.bfloat16),
        "w_down": w_down.astype(jnp.bfloat16),
        "grad_out": grad_out.astype(jnp.bfloat16),
    }


def gelu_parts(pre_act):
    inner = 0.7978845608028654 * (pre_act + 0.044715 * pre_act * pre_act * pre_act)
    tanh_val = jnp.tanh(inner)
    gelu_out = 0.5 * pre_act * (1.0 + tanh_val)
    gelu_slope = 0.5 * (1.0 + tanh_val) + 0.5 * pre_act * (1.0 - tanh_val * tanh_val) * 0.7978845608028654 * (1.0 + 0.134145 * pre_act * pre_act)
    return gelu_out, gelu_slope


def reference(x_saved, h_saved, w_up, w_down, grad_out):
    def block_back(grad_next, layer_in):
        x_layer, h_layer, up_layer, down_layer = layer_in
        grad_f32 = grad_next.astype(jnp.float32)
        d_act = jnp.einsum("bsd,fd->bsf", grad_f32, down_layer.astype(jnp.float32))
        gelu_out, gelu_slope = gelu_parts(h_layer.astype(jnp.float32))
        d_pre = (d_act * gelu_slope).astype(jnp.bfloat16).astype(jnp.float32)
        branch = jnp.einsum("bsf,df->bsd", d_pre, up_layer.astype(jnp.float32))
        grad_in = (grad_f32 + branch).astype(jnp.bfloat16)
        act_rounded = gelu_out.astype(jnp.bfloat16).astype(jnp.float32)
        grad_down = jnp.einsum("bsf,bsd->fd", act_rounded, grad_f32)
        grad_up = jnp.einsum("bsd,bsf->df", x_layer.astype(jnp.float32), d_pre)
        return grad_in, (grad_up, grad_down)

    grad_x, (grad_up, grad_down) = lax.scan(block_back, grad_out, (x_saved, h_saved, w_up, w_down), reverse=True)
    return grad_x, grad_up, grad_down
```

```python
import functools

import jax
import jax.numpy as jnp
from jax import lax
from jax.experimental import pallas as pl
from jax.experimental.pallas import tpu as pltpu
from jax.sharding import PartitionSpec as P


BF16 = jnp.bfloat16
F32 = jnp.float32
BLOCKS = (256, 256, 256)


def gelu_parts(pre_act):
    inner = 0.7978845608028654 * (pre_act + 0.044715 * pre_act * pre_act * pre_act)
    tanh_val = jnp.tanh(inner)
    gelu_out = 0.5 * pre_act * (1.0 + tanh_val)
    gelu_slope = 0.5 * (1.0 + tanh_val) + 0.5 * pre_act * (1.0 - tanh_val * tanh_val) * 0.7978845608028654 * (1.0 + 0.134145 * pre_act * pre_act)
    return gelu_out, gelu_slope


def dot(lhs, rhs, lhs_dim, rhs_dim):
    return lax.dot_general(lhs, rhs, (((lhs_dim,), (rhs_dim,)), ((), ())), preferred_element_type=F32)


def block_body(sources, has_carry, final, _, *refs):
    refs = list(refs)
    grad_ref, x_ref = refs.pop(0), refs.pop(0)
    h_refs = [refs.pop(0) for _ in range(sources)]
    up_refs = [refs.pop(0) for _ in range(sources)]
    down_refs = [refs.pop(0) for _ in range(sources)]
    carry_ref = refs.pop(0) if has_carry else None
    out_ref = refs.pop(0)
    dw_refs = [refs.pop(0) for _ in range(sources)]
    pre_refs = [refs.pop(0) for _ in range(sources)]

    @pl.when(pl.program_id(0) == 0)
    def _():
        for dw_ref in dw_refs:
            dw_ref[...] = jnp.zeros_like(dw_ref)

    grad = grad_ref[0]
    x = x_ref[0, 0]
    total = None
    for s in range(sources):
        width = dw_refs[s].shape[1]
        for start in range(0, width, 256):
            cols = slice(start, min(start + 256, width))
            d_act = dot(grad, down_refs[s][cols, :], 1, 1)
            h = h_refs[s][(0,) * (len(h_refs[s].shape) - 2) + (slice(None), cols)].astype(F32)
            gelu_out, gelu_slope = gelu_parts(h)
            d_pre = (d_act * gelu_slope).astype(BF16)
            pre_refs[s][:, cols] = d_pre
            dw_refs[s][0, cols, :] += dot(d_pre, x, 0, 0)
            dw_refs[s][1, cols, :] += dot(gelu_out.astype(BF16), grad, 0, 0)
        part = dot(pre_refs[s][...], up_refs[s][...], 1, 1)
        total = part if total is None else total + part
    if has_carry:
        total = total + carry_ref[0]
    if final:
        out_ref[0] = (grad.astype(F32) + total).astype(BF16)
    else:
        out_ref[0] = total


def block_call(quarter, layer, grad, x_saved, h_list, up_list, down_list, carry, final):
    rows, seq, hidden = grad.shape
    sources = len(h_list)
    widths = [down.shape[0] for down in down_list]

    def h_spec(h):
        if h.ndim == 4:
            return pl.BlockSpec((1, 1, seq, h.shape[-1]), lambda b, ids: (layer, b, ids[0], 0))
        return pl.BlockSpec((1, seq, h.shape[-1]), lambda b, ids: (b, 0, 0))

    def whole(shape):
        return pl.BlockSpec(shape, lambda b, ids: (0,) * len(shape), pipeline_mode=pl.Buffered(1))

    row_spec = pl.BlockSpec((1, seq, hidden), lambda b, ids: (b, 0, 0))
    in_specs = [row_spec, pl.BlockSpec((1, 1, seq, hidden), lambda b, ids: (layer, b, 0, 0))]
    in_specs += [h_spec(h) for h in h_list]
    in_specs += [whole(up.shape) for up in up_list]
    in_specs += [whole(down.shape) for down in down_list]
    operands = [grad, x_saved, *h_list, *up_list, *down_list]
    if carry is not None:
        in_specs.append(row_spec)
        operands.append(carry)
    flops = 8 * rows * seq * hidden * sum(widths)
    return pl.pallas_call(
        functools.partial(block_body, sources, carry is not None, final),
        out_shape=[jax.ShapeDtypeStruct(grad.shape, BF16 if final else F32)]
        + [jax.ShapeDtypeStruct((2, w, hidden), F32) for w in widths],
        grid_spec=pltpu.PrefetchScalarGridSpec(
            num_scalar_prefetch=1,
            grid=(rows,),
            in_specs=in_specs,
            out_specs=[row_spec] + [whole((2, w, hidden)) for w in widths],
            scratch_shapes=[pltpu.VMEM((seq, w), BF16) for w in widths],
        ),
        compiler_params=pltpu.CompilerParams(dimension_semantics=("arbitrary",), vmem_limit_bytes=60 * 2**20),
        cost_estimate=pl.CostEstimate(flops=flops, bytes_accessed=8 * rows * seq * hidden, transcendentals=rows * seq * sum(widths)),
    )(quarter, *operands)


def solution(mesh):
    n_model = mesh.shape["model"]

    def to_model(value, flip):
        return lax.ppermute(value, "model", [(i, i ^ flip) for i in range(n_model)])

    def to_data(value):
        return lax.ppermute(value, "data", [(0, 1), (1, 0)])

    def device_step(x_saved, h_saved, w_up, w_down, grad_out):
        me = lax.axis_index("model")
        half = lax.axis_index("data")
        first = half == 0
        quarter = jnp.reshape(me, (1,)).astype(jnp.int32)
        rows, seq = grad_out.shape[:2]
        width = h_saved.shape[-1]

        def h_slice(layer, flip, start=0, size=width):
            begin = (me ^ flip) * seq
            return lax.dynamic_slice(h_saved, (layer, 0, begin, start), (1, rows, seq, size))[0]

        mine = jnp.where(first, w_up, w_down)
        from_x = to_model(mine, 2)
        h_one = [to_model(h_slice(1, flip), flip) for flip in (2, 3)]
        h_zero = []
        for j, size in enumerate(BLOCKS):
            start = sum(BLOCKS[:j])
            h_zero.append([to_model(h_slice(0, flip, start, size), flip) for flip in (2, 3)])
        from_y = to_data(from_x)
        up = {0: w_up, 2: jnp.where(first, from_x, from_y)}
        down = {0: w_down, 2: jnp.where(first, from_y, from_x)}
        for flip in (0, 2):
            up[flip + 1] = to_model(up[flip], 1)
            down[flip + 1] = to_model(down[flip], 1)
        h_near = [to_model(h_slice(layer, 1), 1) for layer in (0, 1)]

        def call(layer, grad, hs, flips, carry, final, cols=slice(None)):
            return block_call(
                quarter, layer, grad, x_saved, hs,
                [up[f][layer][:, cols] for f in flips], [down[f][layer][cols] for f in flips], carry, final)

        def pair_sum(keep, give):
            return keep + to_model(give, 1)

        def half_sum(value):
            give = jnp.where(first, value[1], value[0])
            keep = jnp.where(first, value[0], value[1])
            return keep + to_data(give)

        carry, dw_0, dw_1 = call(1, grad_out, [h_saved, h_near[1]], (0, 1), None, False)
        grad_mid, dw_2, dw_3 = call(1, grad_out, h_one, (2, 3), carry, True)
        near = half_sum(pair_sum(dw_0, dw_1))
        far = half_sum(pair_sum(dw_2, dw_3))
        one = [near + to_model(far, 2)]

        carry, dw_0, dw_1 = call(0, grad_mid, [h_saved, h_near[0]], (0, 1), None, False)
        near = half_sum(pair_sum(dw_0, dw_1))
        zero = []
        for j, size in enumerate(BLOCKS):
            start = sum(BLOCKS[:j])
            cols = slice(start, start + size)
            carry, dw_2, dw_3 = call(0, grad_mid, h_zero[j], (2, 3), carry, j == len(BLOCKS) - 1, cols)
            far = half_sum(pair_sum(dw_2, dw_3))
            zero.append(near[cols] + to_model(far, 2))

        def both(kept):
            other = [to_data(k) for k in kept]
            up_grad = jnp.concatenate([jnp.where(first, k, o) for k, o in zip(kept, other)])
            down_grad = jnp.concatenate([jnp.where(first, o, k) for k, o in zip(kept, other)])
            return up_grad.T, down_grad

        up_zero, down_zero = both(zero)
        up_one, down_one = both(one)
        return carry, jnp.stack([up_zero, up_one]), jnp.stack([down_zero, down_one])

    return jax.shard_map(
        device_step,
        mesh=mesh,
        in_specs=(P(None, "data", "model", None), P(None, "data", None, "model"), P(None, None, "model"), P(None, "model", None), P("data", "model", None)),
        out_specs=(P("data", "model", None), P(None, None, "model"), P(None, "model", None)),
        check_vma=False,
    )
```

```python
import functools

import jax
import jax.numpy as jnp
from jax import lax
from jax.experimental import pallas as pl
from jax.experimental.pallas import tpu as pltpu
from jax.sharding import PartitionSpec as P


BF16 = jnp.bfloat16
F32 = jnp.float32
BLOCKS = (384, 256, 128)
LANES = 128


def gelu_parts(pre_act):
    root = 0.7978845608028654
    cubic = (0.134145 * pre_act) * pre_act
    gate = 0.5 + 0.5 * jnp.tanh(pre_act * (root + (root / 3) * cubic))
    gelu_out = pre_act * gate
    gelu_slope = gate + gelu_out * (1.0 - gate) * (2 * root + (2 * root) * cubic)
    return gelu_out, gelu_slope


def dot(lhs, rhs, lhs_dim, rhs_dim):
    return lax.dot_general(lhs, rhs, (((lhs_dim,), (rhs_dim,)), ((), ())), preferred_element_type=F32)


def block_body(sources, has_carry, final, _, *refs):
    refs = list(refs)
    grad_ref, x_ref = refs.pop(0), refs.pop(0)
    h_refs = [refs.pop(0) for _ in range(sources)]
    up_refs = [refs.pop(0) for _ in range(sources)]
    down_refs = [refs.pop(0) for _ in range(sources)]
    carry_ref = refs.pop(0) if has_carry else None
    out_ref = refs.pop(0)
    dw_refs = [refs.pop(0) for _ in range(sources)]
    pre_refs = [refs.pop(0) for _ in range(sources)]

    @pl.when(pl.program_id(0) == 0)
    def _():
        for dw_ref in dw_refs:
            dw_ref[...] = jnp.zeros_like(dw_ref)

    grad = grad_ref[0]
    x = x_ref[0, 0]
    total = None
    for s in range(sources):
        width = dw_refs[s].shape[1]
        for start in range(0, width, 256):
            cols = slice(start, min(start + 256, width))
            d_act = dot(grad, down_refs[s][cols, :], 1, 1)
            h = h_refs[s][(0,) * (len(h_refs[s].shape) - 2) + (slice(None), cols)].astype(F32)
            gelu_out, gelu_slope = gelu_parts(h)
            d_pre = (d_act * gelu_slope).astype(BF16)
            pre_refs[s][:, cols] = d_pre
            dw_refs[s][0, cols, :] += dot(d_pre, x, 0, 0)
            dw_refs[s][1, cols, :] += dot(gelu_out.astype(BF16), grad, 0, 0)
        part = dot(pre_refs[s][...], up_refs[s][...], 1, 1)
        total = part if total is None else total + part
    if has_carry:
        total = total + carry_ref[0]
    if final:
        out_ref[0] = (grad.astype(F32) + total).astype(BF16)
    else:
        out_ref[0] = total


def block_call(quarter, layer, grad, x_saved, h_list, up_list, down_list, carry, final):
    rows, seq, hidden = grad.shape
    sources = len(h_list)
    widths = [down.shape[0] for down in down_list]

    def h_spec(h):
        if h.ndim == 4:
            return pl.BlockSpec((1, 1, seq, h.shape[-1]), lambda b, ids: (layer, b, ids[0], 0))
        return pl.BlockSpec((1, seq, h.shape[-1]), lambda b, ids: (b, 0, 0))

    def whole(shape):
        return pl.BlockSpec(shape, lambda b, ids: (0,) * len(shape), pipeline_mode=pl.Buffered(1))

    row_spec = pl.BlockSpec((1, seq, hidden), lambda b, ids: (b, 0, 0))
    in_specs = [row_spec, pl.BlockSpec((1, 1, seq, hidden), lambda b, ids: (layer, b, 0, 0))]
    in_specs += [h_spec(h) for h in h_list]
    in_specs += [whole(up.shape) for up in up_list]
    in_specs += [whole(down.shape) for down in down_list]
    operands = [grad, x_saved, *h_list, *up_list, *down_list]
    if carry is not None:
        in_specs.append(row_spec)
        operands.append(carry)
    flops = 8 * rows * seq * hidden * sum(widths)
    return pl.pallas_call(
        functools.partial(block_body, sources, carry is not None, final),
        out_shape=[jax.ShapeDtypeStruct(grad.shape, BF16 if final else F32)]
        + [jax.ShapeDtypeStruct((2, w, hidden), F32) for w in widths],
        grid_spec=pltpu.PrefetchScalarGridSpec(
            num_scalar_prefetch=1,
            grid=(rows,),
            in_specs=in_specs,
            out_specs=[row_spec] + [whole((2, w, hidden)) for w in widths],
            scratch_shapes=[pltpu.VMEM((seq, w), BF16) for w in widths],
        ),
        compiler_params=pltpu.CompilerParams(dimension_semantics=("arbitrary",), vmem_limit_bytes=60 * 2**20),
        cost_estimate=pl.CostEstimate(flops=flops, bytes_accessed=8 * rows * seq * hidden, transcendentals=rows * seq * sum(widths)),
    )(quarter, *operands)


def place_body(first_ref, kept_ref, other_ref, *refs):
    up_ref, down_ref = refs[-2:]
    first = first_ref[0] == 1
    kept, other = kept_ref[...], other_ref[...]
    up_ref[0] = jnp.where(first, kept, other).T
    down_ref[0] = jnp.where(first, other, kept)


def place_call(first, kept, other, layer, start, layers, bufs):
    size, hidden = kept.shape
    width = 768
    row_spec = pl.BlockSpec((LANES, hidden), lambda i, first: (i, 0))
    out_shape = [jax.ShapeDtypeStruct((layers, hidden, width), F32), jax.ShapeDtypeStruct((layers, width, hidden), F32)]
    any_spec = pl.BlockSpec(memory_space=pl.ANY)
    return pl.pallas_call(
        place_body,
        out_shape=out_shape,
        grid_spec=pltpu.PrefetchScalarGridSpec(
            num_scalar_prefetch=1,
            grid=(size // LANES,),
            in_specs=[row_spec, row_spec] + ([any_spec, any_spec] if bufs is not None else []),
            out_specs=[
                pl.BlockSpec((1, hidden, LANES), lambda i, first: (layer, 0, start // LANES + i)),
                pl.BlockSpec((1, LANES, hidden), lambda i, first: (layer, start // LANES + i, 0)),
            ],
        ),
        input_output_aliases={3: 0, 4: 1} if bufs is not None else {},
        compiler_params=pltpu.CompilerParams(dimension_semantics=("arbitrary",)),
        cost_estimate=pl.CostEstimate(flops=4 * size * hidden, bytes_accessed=16 * size * hidden, transcendentals=0),
    )(first, kept, other, *(bufs or ()))


def solution(mesh):
    n_model = mesh.shape["model"]

    def to_model(value, flip):
        return lax.ppermute(value, "model", [(i, i ^ flip) for i in range(n_model)])

    def to_data(value):
        return lax.ppermute(value, "data", [(0, 1), (1, 0)])

    def all_blocks(x_saved, h_saved, w_up, w_down, grad_out):
        me = lax.axis_index("model")
        half = lax.axis_index("data")
        first = half == 0
        first_flag = jnp.reshape(first, (1,)).astype(jnp.int32)
        quarter = jnp.reshape(me, (1,)).astype(jnp.int32)
        layers = w_up.shape[0]
        rows, seq = grad_out.shape[:2]
        width = h_saved.shape[-1]

        mine = jnp.where(first, w_up, w_down)
        from_x = to_model(mine, 2)

        held = [h_saved, mine]

        def h_from(layer, flip, start=0, size=width):
            held[0], held[1] = lax.optimization_barrier((held[0], held[1]))
            begin = (me ^ flip) * seq
            held[1] = lax.dynamic_slice(held[0], (layer, 0, begin, start), (1, rows, seq, size))[0]
            return to_model(held[1], flip)

        h_one = [h_from(1, 2), h_from(1, 3)]
        h_near = {1: h_from(1, 1), 0: h_from(0, 1)}
        h_zero = []
        for j, size in enumerate(BLOCKS):
            start = sum(BLOCKS[:j])
            h_zero.append([h_from(0, 2, start, size), h_from(0, 3, start, size)])

        from_y = to_data(from_x)
        up = {0: w_up, 2: jnp.where(first, from_x, from_y)}
        down = {0: w_down, 2: jnp.where(first, from_y, from_x)}
        for flip in (0, 2):
            up[flip + 1] = to_model(up[flip], 1)
            down[flip + 1] = to_model(down[flip], 1)

        def call(layer, grad, hs, flips, carry, final, cols=slice(None)):
            return block_call(
                quarter, layer, grad, x_saved, hs,
                [up[f][layer][:, cols] for f in flips], [down[f][layer][cols] for f in flips], carry, final)

        def partial_sum(keep, give):
            value = keep + to_model(give, 1)
            away = jnp.where(first, value[1], value[0])
            stay = jnp.where(first, value[0], value[1])
            return stay + to_data(away)

        carry, dw_0, dw_1 = call(1, grad_out, [h_saved, h_near[1]], (0, 1), None, False)
        near = partial_sum(dw_0, dw_1)
        grad_mid, dw_2, dw_3 = call(1, grad_out, h_one, (2, 3), carry, True)
        far = partial_sum(dw_2, dw_3)
        kept = near + to_model(far, 2)
        bufs = place_call(first_flag, kept, to_data(kept), 1, 0, layers, None)

        carry, dw_0, dw_1 = call(0, grad_mid, [h_saved, h_near[0]], (0, 1), None, False)
        near = partial_sum(dw_0, dw_1)
        for j, size in enumerate(BLOCKS):
            start = sum(BLOCKS[:j])
            cols = slice(start, start + size)
            carry, dw_2, dw_3 = call(0, grad_mid, h_zero[j], (2, 3), carry, j == len(BLOCKS) - 1, cols)
            far = partial_sum(dw_2, dw_3)
            kept = near[cols] + to_model(far, 2)
            bufs = place_call(first_flag, kept, to_data(kept), 0, start, layers, bufs)
        return carry, bufs[0], bufs[1]

    return jax.shard_map(
        all_blocks,
        mesh=mesh,
        in_specs=(P(None, "data", "model", None), P(None, "data", None, "model"), P(None, None, "model"), P(None, "model", None), P("data", "model", None)),
        out_specs=(P("data", "model", None), P(None, None, "model"), P(None, "model", None)),
        check_vma=False,
    )
```

```python
import functools

import jax
import jax.numpy as jnp
from jax import lax
from jax.experimental import pallas as pl
from jax.experimental.pallas import tpu as pltpu
from jax.sharding import PartitionSpec as P


BF16 = jnp.bfloat16
F32 = jnp.float32
BLOCKS = (384, 256)
LANES = 128
SMALL = 64


def gelu_parts(pre_act):
    root = 0.7978845608028654
    cubic = (0.134145 * pre_act) * pre_act
    gate = 0.5 + 0.5 * jnp.tanh(pre_act * (root + (root / 3) * cubic))
    gelu_out = pre_act * gate
    gelu_slope = gate + gelu_out * (1.0 - gate) * (2 * root + (2 * root) * cubic)
    return gelu_out, gelu_slope


def dot(lhs, rhs, lhs_dim, rhs_dim):
    return lax.dot_general(lhs, rhs, (((lhs_dim,), (rhs_dim,)), ((), ())), preferred_element_type=F32)


def unit_grads(grad, h, down):
    d_act = dot(grad, down, 1, 1)
    gelu_out, gelu_slope = gelu_parts(h.astype(F32))
    return (d_act * gelu_slope).astype(BF16), gelu_out.astype(BF16)


def block_body(has_carry, final, rows, start, _, *refs):
    refs = list(refs)
    grad_ref, x_ref, h_a, h_b, up_a, up_b, down_a, down_b = (refs.pop(0) for _ in range(8))
    carry_ref = refs.pop(0) if has_carry else None
    out_ref, dw_a, dw_b, h_ref, pre_ref, act_ref, sum_ref, dw_ref, up_ref, down_ref, sem = refs
    row, source = pl.program_id(0), pl.program_id(1)
    width = pre_ref.shape[1]

    @pl.when((row == 0) & (source == 0))
    def _():
        dw_ref[...] = jnp.zeros_like(dw_ref)
        for s, (up, down) in enumerate(((up_a, down_a), (up_b, down_b))):
            up_ref[s] = up[(0,) * (len(up.shape) - 2) + (slice(None), slice(start, start + width))]
            down_ref[s] = down[(0,) * (len(down.shape) - 2) + (slice(start, start + width),)]

    for s, ref in enumerate((h_a, h_b)):
        @pl.when(source == s)
        def _():
            h_ref[...] = ref[(0,) * (len(ref.shape) - 2)]

    grad = grad_ref[0]
    x = x_ref[0, 0]
    for low in range(0, width, 256):
        cols = slice(low, min(low + 256, width))
        pre_ref[:, cols], act_ref[:, cols] = unit_grads(grad, h_ref[:, cols], down_ref[source, cols, :])
    pre, act = pre_ref[...], act_ref[...]
    dw_ref[source, 0] += dot(pre, x, 0, 0)
    dw_ref[source, 1] += dot(act, grad, 0, 0)
    part = dot(pre, up_ref[source], 1, 1)

    @pl.when(source == 0)
    def _():
        sum_ref[...] = part + carry_ref[0] if has_carry else part

    @pl.when(source == 1)
    def _():
        total = sum_ref[...] + part
        out_ref[0] = (grad.astype(F32) + total).astype(BF16) if final else total

    copies = [pltpu.make_async_copy(dw_ref.at[s], dw, sem.at[s]) for s, dw in enumerate((dw_a, dw_b))]
    for s in range(2):
        @pl.when((row == rows - 1) & (source == s))
        def _():
            copies[s].start()

    @pl.when((row == rows - 1) & (source == 1))
    def _():
        copies[0].wait()
        copies[1].wait()


def block_call(quarter, layer, grad, x_saved, h_pair, ups, downs, start, width, carry, final):
    rows, seq, hidden = grad.shape

    def h_spec(h):
        if h.ndim == 4:
            return pl.BlockSpec((1, 1, seq, width), lambda b, s, ids: (layer, b, ids[0], 0))
        return pl.BlockSpec((1, seq, width), lambda b, s, ids: (b, 0, 0))

    def w_spec(w):
        shape = (1,) * (w.ndim - 2) + w.shape[-2:]
        return pl.BlockSpec(shape, lambda b, s, ids: (layer,) * (w.ndim - 2) + (0, 0), pipeline_mode=pl.Buffered(1))

    row_spec = pl.BlockSpec((1, seq, hidden), lambda b, s, ids: (b, 0, 0))
    any_spec = pl.BlockSpec(memory_space=pl.ANY)
    in_specs = [row_spec, pl.BlockSpec((1, 1, seq, hidden), lambda b, s, ids: (layer, b, 0, 0))]
    in_specs += [h_spec(h) for h in h_pair]
    in_specs += [w_spec(w) for w in (*ups, *downs)]
    operands = [grad, x_saved, *h_pair, *ups, *downs]
    if carry is not None:
        in_specs.append(row_spec)
        operands.append(carry)
    dw_shape = (2, width, hidden)
    return pl.pallas_call(
        functools.partial(block_body, carry is not None, final, rows, start),
        out_shape=[jax.ShapeDtypeStruct(grad.shape, BF16 if final else F32)] + [jax.ShapeDtypeStruct(dw_shape, F32)] * 2,
        grid_spec=pltpu.PrefetchScalarGridSpec(
            num_scalar_prefetch=1,
            grid=(rows, 2),
            in_specs=in_specs,
            out_specs=[row_spec, any_spec, any_spec],
            scratch_shapes=[pltpu.VMEM((seq, width), BF16)] * 3
            + [pltpu.VMEM((seq, hidden), F32), pltpu.VMEM((2,) + dw_shape, F32)]
            + [pltpu.VMEM((2, hidden, width), BF16), pltpu.VMEM((2, width, hidden), BF16), pltpu.SemaphoreType.DMA((2,))],
        ),
        compiler_params=pltpu.CompilerParams(dimension_semantics=("arbitrary", "arbitrary"), vmem_limit_bytes=56 * 2**20),
        cost_estimate=pl.CostEstimate(
            flops=16 * rows * seq * hidden * width, bytes_accessed=8 * rows * seq * hidden, transcendentals=2 * rows * seq * width),
    )(quarter, *operands)


def swap_lanes(a, b):
    left = lax.broadcasted_iota(jnp.int32, a.shape, 1) < SMALL
    return jnp.where(left, a, pltpu.roll(b, SMALL, 1)), jnp.where(left, pltpu.roll(a, SMALL, 1), b)


def pack_body(_, lo_ref, hi_ref, left_ref, right_ref):
    left, right = swap_lanes(lo_ref[0, 0].astype(F32), hi_ref[0, 0].astype(F32))
    left_ref[0], right_ref[0] = left.astype(BF16), right.astype(BF16)


def pack_call(target, h_saved, layer, start, seq):
    pairs = h_saved.shape[1] // 2
    specs = [pl.BlockSpec((1, 1, seq, LANES), lambda b, ids, r=r: (layer, b + r * pairs, ids[0], start // LANES)) for r in range(2)]
    return pl.pallas_call(
        pack_body,
        out_shape=[jax.ShapeDtypeStruct((pairs, seq, LANES), BF16)] * 2,
        grid_spec=pltpu.PrefetchScalarGridSpec(
            num_scalar_prefetch=1,
            grid=(pairs,),
            in_specs=specs,
            out_specs=[pl.BlockSpec((1, seq, LANES), lambda b, ids: (b, 0, 0))] * 2,
        ),
        compiler_params=pltpu.CompilerParams(dimension_semantics=("arbitrary",)),
        cost_estimate=pl.CostEstimate(flops=pairs * seq * LANES, bytes_accessed=8 * pairs * seq * LANES, transcendentals=0),
    )(target, h_saved, h_saved)


def small_body(grad_lo, grad_hi, x_lo, x_hi, h_a, h_b, down_a, down_b, dw_ref, pre_ref):
    @pl.when(pl.program_id(0) == 0)
    def _():
        dw_ref[...] = jnp.zeros_like(dw_ref)

    h_pair = swap_lanes(h_a[0].astype(F32), h_b[0].astype(F32))
    down = jnp.concatenate([down_a[...], down_b[...]])
    for r, (h, grad_ref, x_ref) in enumerate(zip(h_pair, (grad_lo, grad_hi), (x_lo, x_hi))):
        grad, x = grad_ref[0], x_ref[0, 0]
        pre, act = unit_grads(grad, h, down)
        pre_ref[r, 0] = pre
        dw_ref[0] += dot(pre, x, 0, 0)
        dw_ref[1] += dot(act, grad, 0, 0)


def small_call(layer, grad, x_saved, h_pair, down_pair, start):
    rows, seq, hidden = grad.shape
    pairs = rows // 2

    def row_specs(lead, index):
        return [pl.BlockSpec(lead + (1, seq, hidden), lambda b, r=r: index + (b + r * pairs, 0, 0)) for r in range(2)]

    h_spec = pl.BlockSpec((1, seq, LANES), lambda b: (b, 0, 0))
    down_spec = pl.BlockSpec((SMALL, hidden), lambda b: (start // SMALL, 0))
    dw_shape = (2, LANES, hidden)
    return pl.pallas_call(
        small_body,
        out_shape=[jax.ShapeDtypeStruct(dw_shape, F32), jax.ShapeDtypeStruct((2, pairs, seq, LANES), BF16)],
        grid=(pairs,),
        in_specs=row_specs((), ()) + row_specs((1,), (layer,)) + [h_spec, h_spec, down_spec, down_spec],
        out_specs=[pl.BlockSpec(dw_shape, lambda b: (0, 0, 0)), pl.BlockSpec((2, 1, seq, LANES), lambda b: (0, b, 0, 0))],
        compiler_params=pltpu.CompilerParams(dimension_semantics=("arbitrary",), vmem_limit_bytes=40 * 2**20),
        cost_estimate=pl.CostEstimate(
            flops=12 * rows * seq * hidden * SMALL, bytes_accessed=4 * rows * seq * hidden, transcendentals=2 * rows * seq * SMALL),
    )(grad, grad, x_saved, x_saved, *h_pair, *down_pair)


def finish_body(grad_ref, carry_ref, pre_a, pre_b, up_a, up_b, *refs):
    out_ref, up_ref = refs[-2:]

    @pl.when(pl.program_id(0) == 0)
    def _():
        first, second = swap_lanes(up_a[...].astype(F32), up_b[...].astype(F32))
        up_ref[:, :LANES], up_ref[:, LANES:] = first.astype(BF16), second.astype(BF16)

    total = carry_ref[0] + dot(jnp.concatenate([pre_a[0, 0], pre_b[0, 0]], axis=1), up_ref[...], 1, 1)
    out_ref[0] = (grad_ref[0].astype(F32) + total).astype(BF16)


def finish_call(grad, carry, pre_pair, up_pair, start, half, out):
    rows, seq, hidden = grad.shape
    pairs = rows // 2
    row_spec = pl.BlockSpec((1, seq, hidden), lambda b: (b + half * pairs, 0, 0))
    pre_spec = pl.BlockSpec((1, 1, seq, LANES), lambda b: (half, b, 0, 0))
    up_spec = pl.BlockSpec((hidden, LANES), lambda b: (0, start // LANES))
    return pl.pallas_call(
        finish_body,
        out_shape=jax.ShapeDtypeStruct(grad.shape, BF16),
        grid=(pairs,),
        in_specs=[row_spec, row_spec, pre_spec, pre_spec, up_spec, up_spec]
        + ([pl.BlockSpec(memory_space=pl.ANY)] if out is not None else []),
        out_specs=row_spec,
        scratch_shapes=[pltpu.VMEM((hidden, 2 * LANES), BF16)],
        input_output_aliases={6: 0} if out is not None else {},
        compiler_params=pltpu.CompilerParams(dimension_semantics=("arbitrary",), vmem_limit_bytes=40 * 2**20),
        cost_estimate=pl.CostEstimate(flops=4 * rows * seq * hidden * SMALL, bytes_accessed=4 * rows * seq * hidden, transcendentals=0),
    )(grad, carry, *pre_pair, *up_pair, *(() if out is None else (out,)))


def place_body(pieces, first_ref, *refs):
    up_ref, down_ref = refs[-2:]
    first = first_ref[0] == 1
    kept = jnp.concatenate([r[...] for r in refs[:pieces]])
    other = jnp.concatenate([r[...] for r in refs[pieces : 2 * pieces]])
    up_ref[0] = jnp.where(first, kept, other).T
    down_ref[0] = jnp.where(first, other, kept)


def place_call(first, kept, other, layer, start, layers, width, bufs):
    size, hidden = kept[0].shape
    step = min(size, LANES)
    row_spec = pl.BlockSpec((step, hidden), lambda i, first: (i, 0))
    out_shape = [jax.ShapeDtypeStruct((layers, hidden, width), F32), jax.ShapeDtypeStruct((layers, width, hidden), F32)]
    any_spec = pl.BlockSpec(memory_space=pl.ANY)
    count = 2 * len(kept)
    return pl.pallas_call(
        functools.partial(place_body, len(kept)),
        out_shape=out_shape,
        grid_spec=pltpu.PrefetchScalarGridSpec(
            num_scalar_prefetch=1,
            grid=(size // step,),
            in_specs=[row_spec] * count + ([any_spec, any_spec] if bufs is not None else []),
            out_specs=[
                pl.BlockSpec((1, hidden, LANES), lambda i, first: (layer, 0, start // LANES + i)),
                pl.BlockSpec((1, LANES, hidden), lambda i, first: (layer, start // LANES + i, 0)),
            ],
        ),
        input_output_aliases={1 + count: 0, 2 + count: 1} if bufs is not None else {},
        compiler_params=pltpu.CompilerParams(dimension_semantics=("arbitrary",)),
        cost_estimate=pl.CostEstimate(flops=4 * size * hidden, bytes_accessed=16 * size * hidden, transcendentals=0),
    )(first, *kept, *other, *(bufs or ()))


def solution(mesh):
    n_model = mesh.shape["model"]

    def to_model(value, flip):
        return lax.ppermute(value, "model", [(i, i ^ flip) for i in range(n_model)])

    def to_data(value):
        return lax.ppermute(value, "data", [(0, 1), (1, 0)])

    def all_blocks(x_saved, h_saved, w_up, w_down, grad_out):
        me = lax.axis_index("model")
        first = lax.axis_index("data") == 0
        first_flag = jnp.reshape(first, (1,)).astype(jnp.int32)
        quarter = jnp.reshape(me, (1,)).astype(jnp.int32)
        layers = w_up.shape[0]
        rows, seq = grad_out.shape[:2]
        width = h_saved.shape[-1]

        held = [h_saved, None]

        def h_from(layer, flip, start=0, size=width):
            held[0], held[1] = lax.optimization_barrier((held[0], held[1]))
            begin = (me ^ flip) * seq
            held[1] = lax.dynamic_slice(held[0], (layer, 0, begin, start), (1, rows, seq, size))[0]
            return to_model(held[1], flip)

        held[1] = jnp.where(first, w_up[1], w_down[1])
        far_w = [None, to_model(held[1], 2)]
        h_one = [h_from(1, 2), h_from(1, 3)]
        h_near = [None, h_from(1, 1)]
        w_pair = lax.optimization_barrier((w_up, w_down, held[1]))
        far_w[0] = jnp.where(first, w_pair[0][0], w_pair[1][0])
        far_w[0] = to_model(far_w[0], 2)
        h_near[0] = h_from(0, 1)
        h_zero = []
        for j, size in enumerate(BLOCKS):
            start = sum(BLOCKS[:j])
            h_zero.append([h_from(0, 2, start, size), h_from(0, 3, start, size)])
        small_start = width - LANES
        packed = []
        for flip in (2, 3):
            packed.append(pack_call(jnp.reshape(me ^ flip, (1,)).astype(jnp.int32), h_saved, 0, small_start, seq))
        h_small = [[to_model(packed[0][j], 2), to_model(packed[1][j], 3)] for j in range(2)]

        up, down = [{0: w_up} for _ in range(layers)], [{0: w_down} for _ in range(layers)]
        near_up, near_down = to_model(w_up, 1), to_model(w_down, 1)
        for layer in range(layers):
            other = to_data(far_w[layer])
            up[layer][1], down[layer][1] = near_up, near_down
            up[layer][2], down[layer][2] = jnp.where(first, far_w[layer], other), jnp.where(first, other, far_w[layer])
            up[layer][3] = to_model(up[layer][2], 1)
            down[layer][3] = to_model(down[layer][2], 1)

        def call(layer, grad, hs, flips, carry, final, start=0, size=width):
            ups, downs = [up[layer][f] for f in flips], [down[layer][f] for f in flips]
            return block_call(quarter, layer, grad, x_saved, hs, ups, downs, start, size, carry, final)

        def partial_sum(keep, give):
            value = keep + to_model(give, 1)
            away = jnp.where(first, value[1], value[0])
            stay = jnp.where(first, value[0], value[1])
            return stay + to_data(away)

        def place(pieces, layer, start, bufs):
            kept, other = zip(*pieces)
            return place_call(first_flag, kept, other, layer, start, layers, width, bufs)

        carry, dw_0, dw_1 = call(1, grad_out, [h_saved, h_near[1]], (0, 1), None, False)
        near = partial_sum(dw_0, dw_1)
        grad_mid, dw_2, dw_3 = call(1, grad_out, h_one, (2, 3), carry, True)
        far = partial_sum(dw_2, dw_3)
        kept = near + to_model(far, 2)
        bufs = place([(kept, to_data(kept))], 1, 0, None)

        carry, dw_0, dw_1 = call(0, grad_mid, [h_saved, h_near[0]], (0, 1), None, False)
        near = partial_sum(dw_0, dw_1)
        units = [(0, 0, 384), (1, 384, 128), (1, 512, 128), (2, small_start, SMALL), (3, small_start + SMALL, SMALL)]
        near_part = lax.optimization_barrier(tuple(near[start : start + size] for _, start, size in units))
        pres, pieces = [], []
        for j in range(4):
            base = sum(BLOCKS[:j]) if j < 2 else small_start + (j - 2) * SMALL
            if j < 2:
                flips = (2, 3)
                carry, dw_2, dw_3 = call(0, grad_mid, h_zero[j], flips, carry, False, base, BLOCKS[j])
            else:
                dw, pre = small_call(0, grad_mid, x_saved, h_small[j - 2], [down[0][f] for f in (2, 3)], base)
                dw_2, dw_3 = dw[:, :SMALL], dw[:, SMALL:]
                pres.append(pre)
            far = partial_sum(dw_2, dw_3)
            for u, (block, start, size) in enumerate(units):
                if block == j:
                    kept = near_part[u] + to_model(far[start - base : start - base + size], 2)
                    pieces.append((kept, to_data(kept)))
        for u in range(3):
            bufs = place([pieces[u]], 0, units[u][1], bufs)
        grad_x = None
        for half in range(2):
            grad_x = finish_call(grad_mid, carry, pres, [up[0][f] for f in (2, 3)], small_start, half, grad_x)
        bufs = place(pieces[3:], 0, small_start, bufs)
        return grad_x, bufs[0], bufs[1]

    return jax.shard_map(
        all_blocks,
        mesh=mesh,
        in_specs=(P(None, "data", "model", None), P(None, "data", None, "model"), P(None, None, "model"), P(None, "model", None), P("data", "model", None)),
        out_specs=(P("data", "model", None), P(None, None, "model"), P(None, "model", None)),
        check_vma=False,
    )
```

```python
import functools

import jax
import jax.numpy as jnp
from jax import lax
from jax.experimental import pallas as pl
from jax.experimental.pallas import tpu as pltpu
from jax.sharding import PartitionSpec as P


BF16 = jnp.bfloat16
F32 = jnp.float32
BLOCKS = (384, 256)
LANES = 128
SMALL = 64
ALL_VMEM = 66_000_000


def gelu_parts(pre_act):
    root = 0.7978845608028654
    cubic = (0.134145 * pre_act) * pre_act
    gate = 0.5 + 0.5 * jnp.tanh(pre_act * (root + (root / 3) * cubic))
    gelu_out = pre_act * gate
    gelu_slope = gate + gelu_out * (1.0 - gate) * (2 * root + (2 * root) * cubic)
    return gelu_out, gelu_slope


def dot(lhs, rhs, lhs_dim, rhs_dim):
    return lax.dot_general(lhs, rhs, (((lhs_dim,), (rhs_dim,)), ((), ())), preferred_element_type=F32)


def unit_grads(grad, h, down):
    d_act = dot(grad, down, 1, 1)
    gelu_out, gelu_slope = gelu_parts(h.astype(F32))
    return (d_act * gelu_slope).astype(BF16), gelu_out.astype(BF16)


def block_body(has_carry, final, rows, start, _, *refs):
    refs = list(refs)
    grad_ref, x_ref, h_a, h_b, up_a, up_b, down_a, down_b = (refs.pop(0) for _ in range(8))
    carry_ref = refs.pop(0) if has_carry else None
    out_ref, dw_a, dw_b, h_ref, pre_ref, act_ref, sum_ref, dw_ref, up_ref, down_ref, sem = refs
    row, source = pl.program_id(0), pl.program_id(1)
    width = pre_ref.shape[1]

    @pl.when((row == 0) & (source == 0))
    def _():
        dw_ref[...] = jnp.zeros_like(dw_ref)
        for s, (up, down) in enumerate(((up_a, down_a), (up_b, down_b))):
            up_ref[s] = up[(0,) * (len(up.shape) - 2) + (slice(None), slice(start, start + width))]
            down_ref[s] = down[(0,) * (len(down.shape) - 2) + (slice(start, start + width),)]

    for s, ref in enumerate((h_a, h_b)):
        @pl.when(source == s)
        def _():
            h_ref[...] = ref[(0,) * (len(ref.shape) - 2)]

    grad = grad_ref[0]
    x = x_ref[0, 0]
    for low in range(0, width, 256):
        cols = slice(low, min(low + 256, width))
        pre_ref[:, cols], act_ref[:, cols] = unit_grads(grad, h_ref[:, cols], down_ref[source, cols, :])
    pre, act = pre_ref[...], act_ref[...]
    dw_ref[source, 0] += dot(pre, x, 0, 0)
    dw_ref[source, 1] += dot(act, grad, 0, 0)
    part = dot(pre, up_ref[source], 1, 1)

    @pl.when(source == 0)
    def _():
        sum_ref[...] = part + carry_ref[0] if has_carry else part

    @pl.when(source == 1)
    def _():
        total = sum_ref[...] + part
        out_ref[0] = (grad.astype(F32) + total).astype(BF16) if final else total

    copies = [pltpu.make_async_copy(dw_ref.at[s], dw, sem.at[s]) for s, dw in enumerate((dw_a, dw_b))]
    for s in range(2):
        @pl.when((row == rows - 1) & (source == s))
        def _():
            copies[s].start()

    @pl.when((row == rows - 1) & (source == 1))
    def _():
        copies[0].wait()
        copies[1].wait()


def block_call(quarter, layer, grad, x_saved, h_pair, ups, downs, start, width, carry, final):
    rows, seq, hidden = grad.shape

    def h_spec(h):
        if h.ndim == 4:
            return pl.BlockSpec((1, 1, seq, width), lambda b, s, ids: (layer, b, ids[0], 0))
        return pl.BlockSpec((1, seq, width), lambda b, s, ids: (b, 0, 0))

    def w_spec(w):
        shape = (1,) * (w.ndim - 2) + w.shape[-2:]
        return pl.BlockSpec(shape, lambda b, s, ids: (layer,) * (w.ndim - 2) + (0, 0), pipeline_mode=pl.Buffered(1))

    row_spec = pl.BlockSpec((1, seq, hidden), lambda b, s, ids: (b, 0, 0))
    any_spec = pl.BlockSpec(memory_space=pl.ANY)
    in_specs = [row_spec, pl.BlockSpec((1, 1, seq, hidden), lambda b, s, ids: (layer, b, 0, 0))]
    in_specs += [h_spec(h) for h in h_pair]
    in_specs += [w_spec(w) for w in (*ups, *downs)]
    operands = [grad, x_saved, *h_pair, *ups, *downs]
    if carry is not None:
        in_specs.append(row_spec)
        operands.append(carry)
    dw_shape = (2, width, hidden)
    return pl.pallas_call(
        functools.partial(block_body, carry is not None, final, rows, start),
        out_shape=[jax.ShapeDtypeStruct(grad.shape, BF16 if final else F32)] + [jax.ShapeDtypeStruct(dw_shape, F32)] * 2,
        grid_spec=pltpu.PrefetchScalarGridSpec(
            num_scalar_prefetch=1,
            grid=(rows, 2),
            in_specs=in_specs,
            out_specs=[row_spec, any_spec, any_spec],
            scratch_shapes=[pltpu.VMEM((seq, width), BF16)] * 3
            + [pltpu.VMEM((seq, hidden), F32), pltpu.VMEM((2,) + dw_shape, F32)]
            + [pltpu.VMEM((2, hidden, width), BF16), pltpu.VMEM((2, width, hidden), BF16), pltpu.SemaphoreType.DMA((2,))],
        ),
        compiler_params=pltpu.CompilerParams(dimension_semantics=("arbitrary", "arbitrary"), vmem_limit_bytes=ALL_VMEM),
        cost_estimate=pl.CostEstimate(
            flops=16 * rows * seq * hidden * width, bytes_accessed=8 * rows * seq * hidden, transcendentals=2 * rows * seq * width),
    )(quarter, *operands)


def swap_lanes(a, b):
    left = lax.broadcasted_iota(jnp.int32, a.shape, 1) < SMALL
    return jnp.where(left, a, pltpu.roll(b, SMALL, 1)), jnp.where(left, pltpu.roll(a, SMALL, 1), b)


def pack_body(chunk, _, lo_ref, hi_ref, left_ref, right_a, right_b):
    left, right = swap_lanes(lo_ref[0, 0].astype(F32), hi_ref[0, 0].astype(F32))
    left_ref[0] = left.astype(BF16)

    @pl.when(pl.program_id(0) < chunk)
    def _():
        right_a[0] = right.astype(BF16)

    @pl.when(pl.program_id(0) >= chunk)
    def _():
        right_b[0] = right.astype(BF16)


def pack_call(target, h_saved, layer, start, seq):
    pairs = h_saved.shape[1] // 2
    chunk = pairs // 2
    specs = [pl.BlockSpec((1, 1, seq, LANES), lambda b, ids, r=r: (layer, b + r * pairs, ids[0], start // LANES)) for r in range(2)]
    block = (1, seq, LANES)
    return pl.pallas_call(
        functools.partial(pack_body, chunk),
        out_shape=[jax.ShapeDtypeStruct((n, seq, LANES), BF16) for n in (pairs, chunk, chunk)],
        grid_spec=pltpu.PrefetchScalarGridSpec(
            num_scalar_prefetch=1,
            grid=(pairs,),
            in_specs=specs,
            out_specs=[
                pl.BlockSpec(block, lambda b, ids: (b, 0, 0)),
                pl.BlockSpec(block, lambda b, ids: (jnp.minimum(b, chunk - 1), 0, 0)),
                pl.BlockSpec(block, lambda b, ids: (jnp.maximum(b - chunk, 0), 0, 0)),
            ],
        ),
        compiler_params=pltpu.CompilerParams(dimension_semantics=("arbitrary",), vmem_limit_bytes=ALL_VMEM),
        cost_estimate=pl.CostEstimate(flops=pairs * seq * LANES, bytes_accessed=8 * pairs * seq * LANES, transcendentals=0),
    )(target, h_saved, h_saved)


def wide_body(start, grad_ref, x_ref, h_a, h_b, up_a, up_b, down_a, down_b, carry_ref, out_ref, dw_a, dw_b):
    @pl.when(pl.program_id(0) == 0)
    def _():
        dw_a[...] = jnp.zeros_like(dw_a)
        dw_b[...] = jnp.zeros_like(dw_b)

    grad, x = grad_ref[0], x_ref[0, 0]
    cols = slice(start, start + h_a.shape[2])
    total = grad.astype(F32) + carry_ref[0]
    for h, up, down, dw in ((h_a, up_a, down_a, dw_a), (h_b, up_b, down_b, dw_b)):
        pre, act = unit_grads(grad, h[0], down[cols, :])
        dw[0] += dot(pre, x, 0, 0)
        dw[1] += dot(act, grad, 0, 0)
        total += dot(pre, up[:, cols], 1, 1)
    out_ref[0] = total


def wide_call(layer, grad, x_saved, h_pair, ups, downs, start, carry):
    rows, seq, hidden = grad.shape
    width = h_pair[0].shape[2]
    row_spec = pl.BlockSpec((1, seq, hidden), lambda b: (b, 0, 0))
    h_spec = pl.BlockSpec((1, seq, width), lambda b: (b, 0, 0))
    w_spec = pl.BlockSpec(ups[0].shape, lambda b: (0, 0), pipeline_mode=pl.Buffered(1))
    dw_shape = (2, width, hidden)
    return pl.pallas_call(
        functools.partial(wide_body, start),
        out_shape=[jax.ShapeDtypeStruct(grad.shape, F32)] + [jax.ShapeDtypeStruct(dw_shape, F32)] * 2,
        grid=(rows,),
        in_specs=[row_spec, pl.BlockSpec((1, 1, seq, hidden), lambda b: (layer, b, 0, 0)), h_spec, h_spec]
        + [w_spec] * 4 + [row_spec],
        out_specs=[row_spec] + [pl.BlockSpec(dw_shape, lambda b: (0, 0, 0), pipeline_mode=pl.Buffered(1))] * 2,
        compiler_params=pltpu.CompilerParams(dimension_semantics=("arbitrary",), vmem_limit_bytes=ALL_VMEM),
        cost_estimate=pl.CostEstimate(
            flops=16 * rows * seq * hidden * width, bytes_accessed=12 * rows * seq * hidden, transcendentals=2 * rows * seq * width),
    )(grad, x_saved, *h_pair, *ups, *downs, carry)


def small_body(has_init, grad_ref, x_ref, h_a, h_b, down_a, down_b, *refs):
    dw_pair, pre_ref, h_ref = refs[-4:-2], refs[-2], refs[-1]

    @pl.when(pl.program_id(0) == 0)
    def _():
        for i, dw in enumerate(dw_pair):
            dw[...] = refs[i][...] if has_init else jnp.zeros_like(dw)

    h_ref[0], h_ref[1] = swap_lanes(h_a[0].astype(F32), h_b[0].astype(F32))
    down = jnp.concatenate([down_a[...], down_b[...]])

    @pl.loop(0, 2)
    def _(r):
        grad, x = grad_ref[r, 0], x_ref[0, r, 0]
        pre, act = unit_grads(grad, h_ref[r], down)
        pre_ref[r, 0] = pre
        for kind, part in enumerate((dot(pre, x, 0, 0), dot(act, grad, 0, 0))):
            dw_pair[0][kind] += part[:SMALL]
            dw_pair[1][kind] += part[SMALL:]


def small_call(layer, grad, x_saved, h_pair, down_pair, start, first_pair, init):
    rows, seq, hidden = grad.shape
    pairs = h_pair[0].shape[0]
    grad = grad.reshape(2, rows // 2, seq, hidden)
    x_saved = x_saved.reshape(-1, 2, rows // 2, seq, hidden)
    h_spec = pl.BlockSpec((1, seq, LANES), lambda b: (b, 0, 0))
    down_spec = pl.BlockSpec((SMALL, hidden), lambda b: (start // SMALL, 0))
    dw_shape = (2, SMALL, hidden)
    dw_spec = pl.BlockSpec(dw_shape, lambda b: (0, 0, 0))
    return pl.pallas_call(
        functools.partial(small_body, init is not None),
        out_shape=[jax.ShapeDtypeStruct(dw_shape, F32)] * 2 + [jax.ShapeDtypeStruct((2, pairs, seq, LANES), BF16)],
        grid=(pairs,),
        in_specs=[
            pl.BlockSpec((2, 1, seq, hidden), lambda b: (0, b + first_pair, 0, 0)),
            pl.BlockSpec((1, 2, 1, seq, hidden), lambda b: (layer, 0, b + first_pair, 0, 0)),
            h_spec, h_spec, down_spec, down_spec,
        ]
        + ([dw_spec] * 2 if init is not None else []),
        out_specs=[dw_spec, dw_spec, pl.BlockSpec((2, 1, seq, LANES), lambda b: (0, b, 0, 0))],
        scratch_shapes=[pltpu.VMEM((2, seq, LANES), F32)],
        compiler_params=pltpu.CompilerParams(dimension_semantics=("arbitrary",), vmem_limit_bytes=ALL_VMEM),
        cost_estimate=pl.CostEstimate(
            flops=24 * pairs * seq * hidden * SMALL, bytes_accessed=8 * pairs * seq * hidden, transcendentals=4 * pairs * seq * SMALL),
    )(grad, x_saved, *h_pair, *down_pair, *(init or ()))


def finish_body(carry_ref, pre_a, pre_b, up_a, up_b, *refs):
    out_ref, up_ref = refs[-2:]

    @pl.when((pl.program_id(0) == 0) & (pl.program_id(1) == 0))
    def _():
        first, second = swap_lanes(up_a[...].astype(F32), up_b[...].astype(F32))
        up_ref[:, :LANES], up_ref[:, LANES:] = first.astype(BF16), second.astype(BF16)

    total = carry_ref[0] + dot(jnp.concatenate([pre_a[0, 0], pre_b[0, 0]], axis=1), up_ref[...], 1, 1)
    out_ref[0] = total.astype(BF16)


def finish_call(carry, pre_pair, up_pair, start, pairs, offset, out):
    rows, seq, hidden = carry.shape
    row_spec = pl.BlockSpec((1, seq, hidden), lambda r, b: (b + pairs[0] + r * rows // 2, 0, 0))
    pre_specs = [pl.BlockSpec((1, 1, seq, LANES), lambda r, b, first=first: (r, b + first, 0, 0)) for first in (pairs[0], pairs[0] - offset)]
    up_spec = pl.BlockSpec((hidden, LANES), lambda r, b: (0, start // LANES))
    count = 2 * (pairs[1] - pairs[0])
    return pl.pallas_call(
        finish_body,
        out_shape=jax.ShapeDtypeStruct(carry.shape, BF16),
        grid=(2, pairs[1] - pairs[0]),
        in_specs=[row_spec, *pre_specs, up_spec, up_spec] + ([pl.BlockSpec(memory_space=pl.ANY)] if out is not None else []),
        out_specs=row_spec,
        scratch_shapes=[pltpu.VMEM((hidden, 2 * LANES), BF16)],
        input_output_aliases={5: 0} if out is not None else {},
        compiler_params=pltpu.CompilerParams(dimension_semantics=("arbitrary", "arbitrary"), vmem_limit_bytes=ALL_VMEM),
        cost_estimate=pl.CostEstimate(flops=4 * count * seq * hidden * LANES, bytes_accessed=7 * count * seq * hidden, transcendentals=0),
    )(carry, *pre_pair, *up_pair, *(() if out is None else (out,)))


def pair_body(first_ref, mine_ref, theirs_ref, stay_ref, away_ref):
    first = first_ref[0] == 1
    up, down = mine_ref[0] + theirs_ref[0], mine_ref[1] + theirs_ref[1]
    stay_ref[...] = jnp.where(first, up, down)
    away_ref[...] = jnp.where(first, down, up)


def pair_call(first, mine, theirs):
    shape = mine.shape[1:]
    return pl.pallas_call(
        pair_body,
        out_shape=[jax.ShapeDtypeStruct(shape, F32)] * 2,
        grid_spec=pltpu.PrefetchScalarGridSpec(
            num_scalar_prefetch=1,
            grid=(1,),
            in_specs=[pl.BlockSpec(mine.shape, lambda i, first: (0, 0, 0))] * 2,
            out_specs=[pl.BlockSpec(shape, lambda i, first: (0, 0))] * 2,
        ),
        compiler_params=pltpu.CompilerParams(dimension_semantics=("arbitrary",), vmem_limit_bytes=ALL_VMEM),
        cost_estimate=pl.CostEstimate(flops=4 * mine.size, bytes_accessed=12 * mine.size, transcendentals=0),
    )(first, mine, theirs)


def place_body(pieces, first_ref, *refs):
    up_ref, down_ref = refs[-2:]
    first = first_ref[0] == 1
    kept = jnp.concatenate([r[...] for r in refs[:pieces]])
    other = jnp.concatenate([r[...] for r in refs[pieces : 2 * pieces]])
    up_ref[0] = jnp.where(first, kept, other).T
    down_ref[0] = jnp.where(first, other, kept)


def place_call(first, kept, other, layer, start, layers, width, bufs):
    size, hidden = kept[0].shape
    step = min(size, LANES)
    row_spec = pl.BlockSpec((step, hidden), lambda i, first: (i, 0))
    out_shape = [jax.ShapeDtypeStruct((layers, hidden, width), F32), jax.ShapeDtypeStruct((layers, width, hidden), F32)]
    any_spec = pl.BlockSpec(memory_space=pl.ANY)
    count = 2 * len(kept)
    return pl.pallas_call(
        functools.partial(place_body, len(kept)),
        out_shape=out_shape,
        grid_spec=pltpu.PrefetchScalarGridSpec(
            num_scalar_prefetch=1,
            grid=(size // step,),
            in_specs=[row_spec] * count + ([any_spec, any_spec] if bufs is not None else []),
            out_specs=[
                pl.BlockSpec((1, hidden, LANES), lambda i, first: (layer, 0, start // LANES + i)),
                pl.BlockSpec((1, LANES, hidden), lambda i, first: (layer, start // LANES + i, 0)),
            ],
        ),
        input_output_aliases={1 + count: 0, 2 + count: 1} if bufs is not None else {},
        compiler_params=pltpu.CompilerParams(dimension_semantics=("arbitrary",), vmem_limit_bytes=ALL_VMEM),
        cost_estimate=pl.CostEstimate(flops=4 * size * hidden, bytes_accessed=16 * size * hidden, transcendentals=0),
    )(first, *kept, *other, *(bufs or ()))


def solution(mesh):
    n_model = mesh.shape["model"]

    def to_model(value, flip):
        return lax.ppermute(value, "model", [(i, i ^ flip) for i in range(n_model)])

    def to_data(value):
        return lax.ppermute(value, "data", [(0, 1), (1, 0)])

    def all_blocks(x_saved, h_saved, w_up, w_down, grad_out):
        me = lax.axis_index("model")
        first = lax.axis_index("data") == 0
        first_flag = jnp.reshape(first, (1,)).astype(jnp.int32)
        quarter = jnp.reshape(me, (1,)).astype(jnp.int32)
        layers = w_up.shape[0]
        rows, seq = grad_out.shape[:2]
        width = h_saved.shape[-1]

        held = [h_saved, None]

        def h_from(layer, flip, start=0, size=width):
            held[0], held[1] = lax.optimization_barrier((held[0], held[1]))
            begin = (me ^ flip) * seq
            held[1] = lax.dynamic_slice(held[0], (layer, 0, begin, start), (1, rows, seq, size))[0]
            return to_model(held[1], flip)

        held[1] = jnp.where(first, w_up[1], w_down[1])
        far_w = [None, to_model(held[1], 2)]
        h_one = [h_from(1, 2), h_from(1, 3)]
        h_near = [None, h_from(1, 1)]
        w_pair = lax.optimization_barrier((w_up, w_down, held[1]))
        far_w[0] = jnp.where(first, w_pair[0][0], w_pair[1][0])
        far_w[0] = to_model(far_w[0], 2)
        h_near[0] = h_from(0, 1)
        h_zero = []
        for j, size in enumerate(BLOCKS):
            start = sum(BLOCKS[:j])
            h_zero.append([h_from(0, 2, start, size), h_from(0, 3, start, size)])
        small_start = width - LANES
        packed = []
        for flip in (2, 3):
            packed.append(pack_call(jnp.reshape(me ^ flip, (1,)).astype(jnp.int32), h_saved, 0, small_start, seq))
        h_small = [[to_model(packed[0][j], 2), to_model(packed[1][j], 3)] for j in range(3)]

        up, down = [{0: w_up} for _ in range(layers)], [{0: w_down} for _ in range(layers)]
        near_up, near_down = to_model(w_up, 1), to_model(w_down, 1)
        for layer in range(layers):
            other = to_data(far_w[layer])
            up[layer][1], down[layer][1] = near_up, near_down
            up[layer][2], down[layer][2] = jnp.where(first, far_w[layer], other), jnp.where(first, other, far_w[layer])
            up[layer][3] = to_model(up[layer][2], 1)
            down[layer][3] = to_model(down[layer][2], 1)

        def call(layer, grad, hs, flips, carry, final, start=0, size=width):
            ups, downs = [up[layer][f] for f in flips], [down[layer][f] for f in flips]
            return block_call(quarter, layer, grad, x_saved, hs, ups, downs, start, size, carry, final)

        def partial_sum(keep, give, fused=False):
            theirs = to_model(give, 1)
            if fused:
                stay, away = pair_call(first_flag, keep, theirs)
            else:
                value = keep + theirs
                away = jnp.where(first, value[1], value[0])
                stay = jnp.where(first, value[0], value[1])
            return stay + to_data(away)

        def place(pieces, layer, start, bufs):
            kept, other = zip(*pieces)
            return place_call(first_flag, kept, other, layer, start, layers, width, bufs)

        carry, dw_0, dw_1 = call(1, grad_out, [h_saved, h_near[1]], (0, 1), None, False)
        near = partial_sum(dw_0, dw_1)
        grad_mid, dw_2, dw_3 = call(1, grad_out, h_one, (2, 3), carry, True)
        far = partial_sum(dw_2, dw_3)
        kept = near + to_model(far, 2)
        bufs = place([(kept, to_data(kept))], 1, 0, None)

        carry, dw_0, dw_1 = call(0, grad_mid, [h_saved, h_near[0]], (0, 1), None, False)
        near = partial_sum(dw_0, dw_1)
        units = [(0, 0, 384), (1, 384, 128), (1, 512, 128), (2, small_start, SMALL), (3, small_start + SMALL, SMALL)]
        near_part = lax.optimization_barrier(tuple(near[start : start + size] for _, start, size in units))
        down_pair, up_pair = [down[0][f] for f in (2, 3)], [up[0][f] for f in (2, 3)]
        chunk = rows // 4
        pieces = []
        for j in range(4):
            base = sum(BLOCKS[:j]) if j < 2 else small_start + (j - 2) * SMALL
            if j == 0:
                carry, dw_2, dw_3 = call(0, grad_mid, h_zero[j], (2, 3), carry, False, base, BLOCKS[j])
            elif j == 1:
                carry, dw_2, dw_3 = wide_call(0, grad_mid, x_saved, h_zero[j], up_pair, down_pair, base, carry)
            elif j == 2:
                dw_2, dw_3, pre_1 = small_call(0, grad_mid, x_saved, h_small[0], down_pair, base, 0, None)
            else:
                dw_2, dw_3, pre_2 = small_call(0, grad_mid, x_saved, h_small[1], down_pair, base, 0, None)
                grad_x = finish_call(carry, (pre_1, pre_2), up_pair, small_start, (0, chunk), 0, None)
                dw_2, dw_3, pre_2 = small_call(0, grad_mid, x_saved, h_small[2], down_pair, base, chunk, (dw_2, dw_3))
            far = partial_sum(dw_2, dw_3, j >= 2)
            for u, (block, start, size) in enumerate(units):
                if block == j:
                    part = to_model(far[start - base : start - base + size], 2)
                    kept = near_part[u] + part
                    pieces.append((kept, to_data(kept)))
        for u in range(3):
            bufs = place([pieces[u]], 0, units[u][1], bufs)
        for half in range(2):
            low = chunk + half * chunk // 2
            grad_x = finish_call(carry, (pre_1, pre_2), up_pair, small_start, (low, low + chunk // 2), chunk, grad_x)
        bufs = place(pieces[3:], 0, small_start, bufs)
        return grad_x, bufs[0], bufs[1]

    return jax.shard_map(
        all_blocks,
        mesh=mesh,
        in_specs=(P(None, "data", "model", None), P(None, "data", None, "model"), P(None, None, "model"), P(None, "model", None), P("data", "model", None)),
        out_specs=(P("data", "model", None), P(None, None, "model"), P(None, "model", None)),
        check_vma=False,
    )
```

```python
import functools

import jax
import jax.numpy as jnp
from jax import lax
from jax.experimental import pallas as pl
from jax.experimental.pallas import tpu as pltpu
from jax.sharding import PartitionSpec as P


BF16 = jnp.bfloat16
F32 = jnp.float32
BLOCKS = (384, 256)
LANES = 128
SMALL = 64
EARLY = 5
ALL_VMEM = 66_000_000


def gelu_parts(pre_act):
    root = 0.7978845608028654
    cubic = (0.134145 * pre_act) * pre_act
    gate = 0.5 + 0.5 * jnp.tanh(pre_act * (root + (root / 3) * cubic))
    gelu_out = pre_act * gate
    gelu_slope = gate + gelu_out * (1.0 - gate) * (2 * root + (2 * root) * cubic)
    return gelu_out, gelu_slope


def dot(lhs, rhs, lhs_dim, rhs_dim):
    return lax.dot_general(lhs, rhs, (((lhs_dim,), (rhs_dim,)), ((), ())), preferred_element_type=F32)


def unit_grads(grad, h, down):
    d_act = dot(grad, down, 1, 1)
    gelu_out, gelu_slope = gelu_parts(h.astype(F32))
    return (d_act * gelu_slope).astype(BF16), gelu_out.astype(BF16)


def block_body(has_carry, final, rows, start, _, *refs):
    refs = list(refs)
    grad_ref, x_ref, h_a, h_b, up_a, up_b, down_a, down_b = (refs.pop(0) for _ in range(8))
    carry_ref = refs.pop(0) if has_carry else None
    out_ref, dw_a, dw_b, h_ref, pre_ref, act_ref, sum_ref, dw_ref, up_ref, down_ref, sem = refs
    row, source = pl.program_id(0), pl.program_id(1)
    width = pre_ref.shape[1]

    @pl.when((row == 0) & (source == 0))
    def _():
        dw_ref[...] = jnp.zeros_like(dw_ref)
        for s, (up, down) in enumerate(((up_a, down_a), (up_b, down_b))):
            up_ref[s] = up[(0,) * (len(up.shape) - 2) + (slice(None), slice(start, start + width))]
            down_ref[s] = down[(0,) * (len(down.shape) - 2) + (slice(start, start + width),)]

    for s, ref in enumerate((h_a, h_b)):
        @pl.when(source == s)
        def _():
            h_ref[...] = ref[(0,) * (len(ref.shape) - 2)]

    grad = grad_ref[0]
    x = x_ref[0, 0]
    for low in range(0, width, 256):
        cols = slice(low, min(low + 256, width))
        pre_ref[:, cols], act_ref[:, cols] = unit_grads(grad, h_ref[:, cols], down_ref[source, cols, :])
    pre, act = pre_ref[...], act_ref[...]
    dw_ref[source, 0] += dot(pre, x, 0, 0)
    dw_ref[source, 1] += dot(act, grad, 0, 0)
    part = dot(pre, up_ref[source], 1, 1)

    @pl.when(source == 0)
    def _():
        sum_ref[...] = part + carry_ref[0] if has_carry else part

    @pl.when(source == 1)
    def _():
        total = sum_ref[...] + part
        out_ref[0] = (grad.astype(F32) + total).astype(BF16) if final else total

    copies = [pltpu.make_async_copy(dw_ref.at[s], dw, sem.at[s]) for s, dw in enumerate((dw_a, dw_b))]
    for s in range(2):
        @pl.when((row == rows - 1) & (source == s))
        def _():
            copies[s].start()

    @pl.when((row == rows - 1) & (source == 1))
    def _():
        copies[0].wait()
        copies[1].wait()


def block_call(quarter, layer, grad, x_saved, h_pair, ups, downs, start, width, carry, final):
    rows, seq, hidden = grad.shape

    def h_spec(h):
        if h.ndim == 4:
            return pl.BlockSpec((1, 1, seq, width), lambda b, s, ids: (layer, b, ids[0], 0))
        return pl.BlockSpec((1, seq, width), lambda b, s, ids: (b, 0, 0))

    def w_spec(w):
        shape = (1,) * (w.ndim - 2) + w.shape[-2:]
        return pl.BlockSpec(shape, lambda b, s, ids: (layer,) * (w.ndim - 2) + (0, 0), pipeline_mode=pl.Buffered(1))

    row_spec = pl.BlockSpec((1, seq, hidden), lambda b, s, ids: (b, 0, 0))
    any_spec = pl.BlockSpec(memory_space=pl.ANY)
    in_specs = [row_spec, pl.BlockSpec((1, 1, seq, hidden), lambda b, s, ids: (layer, b, 0, 0))]
    in_specs += [h_spec(h) for h in h_pair]
    in_specs += [w_spec(w) for w in (*ups, *downs)]
    operands = [grad, x_saved, *h_pair, *ups, *downs]
    if carry is not None:
        in_specs.append(row_spec)
        operands.append(carry)
    dw_shape = (2, width, hidden)
    return pl.pallas_call(
        functools.partial(block_body, carry is not None, final, rows, start),
        out_shape=[jax.ShapeDtypeStruct(grad.shape, BF16 if final else F32)] + [jax.ShapeDtypeStruct(dw_shape, F32)] * 2,
        grid_spec=pltpu.PrefetchScalarGridSpec(
            num_scalar_prefetch=1,
            grid=(rows, 2),
            in_specs=in_specs,
            out_specs=[row_spec, any_spec, any_spec],
            scratch_shapes=[pltpu.VMEM((seq, width), BF16)] * 3
            + [pltpu.VMEM((seq, hidden), F32), pltpu.VMEM((2,) + dw_shape, F32)]
            + [pltpu.VMEM((2, hidden, width), BF16), pltpu.VMEM((2, width, hidden), BF16), pltpu.SemaphoreType.DMA((2,))],
        ),
        compiler_params=pltpu.CompilerParams(dimension_semantics=("arbitrary", "arbitrary"), vmem_limit_bytes=ALL_VMEM),
        cost_estimate=pl.CostEstimate(
            flops=16 * rows * seq * hidden * width, bytes_accessed=8 * rows * seq * hidden, transcendentals=2 * rows * seq * width),
    )(quarter, *operands)


def swap_lanes(a, b):
    left = lax.broadcasted_iota(jnp.int32, a.shape, 1) < SMALL
    return jnp.where(left, a, pltpu.roll(b, SMALL, 1)), jnp.where(left, pltpu.roll(a, SMALL, 1), b)


def pack_body(chunk, _, lo_ref, hi_ref, left_ref, right_a, right_b):
    left, right = swap_lanes(lo_ref[0, 0].astype(F32), hi_ref[0, 0].astype(F32))
    left_ref[0] = left.astype(BF16)

    @pl.when(pl.program_id(0) < chunk)
    def _():
        right_a[0] = right.astype(BF16)

    @pl.when(pl.program_id(0) >= chunk)
    def _():
        right_b[0] = right.astype(BF16)


def pack_call(target, h_saved, layer, start, seq):
    pairs = h_saved.shape[1] // 2
    chunk = EARLY
    specs = [pl.BlockSpec((1, 1, seq, LANES), lambda b, ids, r=r: (layer, b + r * pairs, ids[0], start // LANES)) for r in range(2)]
    block = (1, seq, LANES)
    return pl.pallas_call(
        functools.partial(pack_body, chunk),
        out_shape=[jax.ShapeDtypeStruct((n, seq, LANES), BF16) for n in (pairs, chunk, pairs - chunk)],
        grid_spec=pltpu.PrefetchScalarGridSpec(
            num_scalar_prefetch=1,
            grid=(pairs,),
            in_specs=specs,
            out_specs=[
                pl.BlockSpec(block, lambda b, ids: (b, 0, 0)),
                pl.BlockSpec(block, lambda b, ids: (jnp.minimum(b, chunk - 1), 0, 0)),
                pl.BlockSpec(block, lambda b, ids: (jnp.maximum(b - chunk, 0), 0, 0)),
            ],
        ),
        compiler_params=pltpu.CompilerParams(dimension_semantics=("arbitrary",), vmem_limit_bytes=ALL_VMEM),
        cost_estimate=pl.CostEstimate(flops=pairs * seq * LANES, bytes_accessed=8 * pairs * seq * LANES, transcendentals=0),
    )(target, h_saved, h_saved)


def wide_body(start, grad_ref, x_ref, h_a, h_b, up_a, up_b, down_a, down_b, carry_ref, out_ref, dw_a, dw_b):
    @pl.when(pl.program_id(0) == 0)
    def _():
        dw_a[...] = jnp.zeros_like(dw_a)
        dw_b[...] = jnp.zeros_like(dw_b)

    grad, x = grad_ref[0], x_ref[0, 0]
    cols = slice(start, start + h_a.shape[2])
    total = grad.astype(F32) + carry_ref[0]
    for h, up, down, dw in ((h_a, up_a, down_a, dw_a), (h_b, up_b, down_b, dw_b)):
        pre, act = unit_grads(grad, h[0], down[cols, :])
        dw[0] += dot(pre, x, 0, 0)
        dw[1] += dot(act, grad, 0, 0)
        total += dot(pre, up[:, cols], 1, 1)
    out_ref[0] = total


def wide_call(layer, grad, x_saved, h_pair, ups, downs, start, carry):
    rows, seq, hidden = grad.shape
    width = h_pair[0].shape[2]
    row_spec = pl.BlockSpec((1, seq, hidden), lambda b: (b, 0, 0))
    h_spec = pl.BlockSpec((1, seq, width), lambda b: (b, 0, 0))
    w_spec = pl.BlockSpec(ups[0].shape, lambda b: (0, 0), pipeline_mode=pl.Buffered(1))
    dw_shape = (2, width, hidden)
    return pl.pallas_call(
        functools.partial(wide_body, start),
        out_shape=[jax.ShapeDtypeStruct(grad.shape, F32)] + [jax.ShapeDtypeStruct(dw_shape, F32)] * 2,
        grid=(rows,),
        in_specs=[row_spec, pl.BlockSpec((1, 1, seq, hidden), lambda b: (layer, b, 0, 0)), h_spec, h_spec]
        + [w_spec] * 4 + [row_spec],
        out_specs=[row_spec] + [pl.BlockSpec(dw_shape, lambda b: (0, 0, 0), pipeline_mode=pl.Buffered(1))] * 2,
        compiler_params=pltpu.CompilerParams(dimension_semantics=("arbitrary",), vmem_limit_bytes=ALL_VMEM),
        cost_estimate=pl.CostEstimate(
            flops=16 * rows * seq * hidden * width, bytes_accessed=12 * rows * seq * hidden, transcendentals=2 * rows * seq * width),
    )(grad, x_saved, *h_pair, *ups, *downs, carry)


def small_body(has_init, finish, grad_ref, x_ref, h_a, h_b, down_a, down_b, *refs):
    refs = list(refs)
    carry_ref, early_ref, up_ref = (refs.pop(0) for _ in range(3)) if finish else (None,) * 3
    dw_pair, out_ref = refs[-3:-1], refs[-1]
    second = pl.program_id(1)

    @pl.when((pl.program_id(0) == 0) & (second == 0))
    def _():
        for i, dw in enumerate(dw_pair):
            dw[...] = refs[i][...] if has_init else jnp.zeros_like(dw)

    h_pair = swap_lanes(h_a[0].astype(F32), h_b[0].astype(F32))
    grad, x = grad_ref[0], x_ref[0, 0]
    pre, act = unit_grads(grad, jnp.where(second == 0, *h_pair), jnp.concatenate([down_a[...], down_b[...]]))
    for kind, part in enumerate((dot(pre, x, 0, 0), dot(act, grad, 0, 0))):
        dw_pair[0][kind] += part[:SMALL]
        dw_pair[1][kind] += part[SMALL:]
    if finish:
        total = carry_ref[0] + dot(jnp.concatenate([early_ref[0, 0], pre], axis=1), up_ref[...], 1, 1)
        out_ref[0] = total.astype(BF16)
    else:
        out_ref[0, 0] = pre


def small_call(layer, grad, x_saved, h_pair, down_pair, start, first_pair, init, finish):
    rows, seq, hidden = grad.shape
    pairs = h_pair[0].shape[0]
    half = rows // 2
    row_spec = pl.BlockSpec((1, seq, hidden), lambda b, r: (b + first_pair + r * half, 0, 0))
    pre_spec = pl.BlockSpec((1, 1, seq, LANES), lambda b, r: (r, b, 0, 0))
    h_spec = pl.BlockSpec((1, seq, LANES), lambda b, r: (b, 0, 0))
    down_spec = pl.BlockSpec((SMALL, hidden), lambda b, r: (start // SMALL, 0))
    dw_shape = (2, SMALL, hidden)
    dw_spec = pl.BlockSpec(dw_shape, lambda b, r: (0, 0, 0))
    in_specs = [row_spec, pl.BlockSpec((1, 1, seq, hidden), lambda b, r: (layer, b + first_pair + r * half, 0, 0)), h_spec, h_spec, down_spec, down_spec]
    if finish:
        in_specs += [row_spec, pre_spec, pl.BlockSpec(finish[2].shape, lambda b, r: (0, 0))]
    if init:
        in_specs += [dw_spec] * 2
    return pl.pallas_call(
        functools.partial(small_body, init is not None, finish is not None),
        out_shape=[jax.ShapeDtypeStruct(dw_shape, F32)] * 2
        + [jax.ShapeDtypeStruct(grad.shape if finish else (2, pairs, seq, LANES), BF16)],
        grid=(pairs, 2),
        in_specs=in_specs,
        out_specs=[dw_spec, dw_spec, row_spec if finish else pre_spec],
        compiler_params=pltpu.CompilerParams(dimension_semantics=("arbitrary", "arbitrary"), vmem_limit_bytes=ALL_VMEM),
        cost_estimate=pl.CostEstimate(
            flops=24 * pairs * seq * hidden * SMALL, bytes_accessed=8 * pairs * seq * hidden, transcendentals=4 * pairs * seq * SMALL),
    )(grad, x_saved, *h_pair, *down_pair, *(finish or ()), *(init or ()))


def join_body(up_a, up_b, out_ref):
    first, second = swap_lanes(up_a[...].astype(F32), up_b[...].astype(F32))
    out_ref[:, :LANES], out_ref[:, LANES:] = first.astype(BF16), second.astype(BF16)


def join_call(up_pair, start):
    hidden = up_pair[0].shape[0]
    up_spec = pl.BlockSpec((hidden, LANES), lambda i: (0, start // LANES))
    return pl.pallas_call(
        join_body,
        out_shape=jax.ShapeDtypeStruct((hidden, 2 * LANES), BF16),
        grid=(1,),
        in_specs=[up_spec, up_spec],
        out_specs=pl.BlockSpec((hidden, 2 * LANES), lambda i: (0, 0)),
        compiler_params=pltpu.CompilerParams(dimension_semantics=("arbitrary",), vmem_limit_bytes=ALL_VMEM),
        cost_estimate=pl.CostEstimate(flops=hidden * LANES, bytes_accessed=8 * hidden * LANES, transcendentals=0),
    )(*up_pair)


def finish_body(carry_ref, pre_a, pre_b, up_ref, _, out_ref):
    total = carry_ref[0] + dot(jnp.concatenate([pre_a[0, 0], pre_b[0, 0]], axis=1), up_ref[...], 1, 1)
    out_ref[0] = total.astype(BF16)


def finish_call(carry, pre_pair, ups, half, out):
    rows, seq, hidden = carry.shape
    count = rows // 2 - EARLY
    row_spec = pl.BlockSpec((1, seq, hidden), lambda b: (b + EARLY + half * rows // 2, 0, 0))
    pre_specs = [pl.BlockSpec((1, 1, seq, LANES), lambda b, first=first: (half, b + first, 0, 0)) for first in (EARLY, 0)]
    return pl.pallas_call(
        finish_body,
        out_shape=jax.ShapeDtypeStruct(carry.shape, BF16),
        grid=(count,),
        in_specs=[row_spec, *pre_specs, pl.BlockSpec(ups.shape, lambda b: (0, 0)), pl.BlockSpec(memory_space=pl.ANY)],
        out_specs=row_spec,
        input_output_aliases={4: 0},
        compiler_params=pltpu.CompilerParams(dimension_semantics=("arbitrary",), vmem_limit_bytes=ALL_VMEM),
        cost_estimate=pl.CostEstimate(flops=4 * count * seq * hidden * LANES, bytes_accessed=7 * count * seq * hidden, transcendentals=0),
    )(carry, *pre_pair, ups, out)


def pair_body(first_ref, mine_ref, theirs_ref, stay_ref, away_ref):
    first = first_ref[0] == 1
    up, down = mine_ref[0] + theirs_ref[0], mine_ref[1] + theirs_ref[1]
    stay_ref[...] = jnp.where(first, up, down)
    away_ref[...] = jnp.where(first, down, up)


def pair_call(first, mine, theirs):
    _, size, hidden = mine.shape
    step = min(size, LANES)
    both_spec = pl.BlockSpec((2, step, hidden), lambda i, first: (0, i, 0))
    one_spec = pl.BlockSpec((step, hidden), lambda i, first: (i, 0))
    return pl.pallas_call(
        pair_body,
        out_shape=[jax.ShapeDtypeStruct((size, hidden), F32)] * 2,
        grid_spec=pltpu.PrefetchScalarGridSpec(
            num_scalar_prefetch=1, grid=(size // step,), in_specs=[both_spec] * 2, out_specs=[one_spec] * 2),
        compiler_params=pltpu.CompilerParams(dimension_semantics=("arbitrary",), vmem_limit_bytes=ALL_VMEM),
        cost_estimate=pl.CostEstimate(flops=4 * mine.size, bytes_accessed=12 * mine.size, transcendentals=0),
    )(first, mine, theirs)


def place_body(pieces, first_ref, *refs):
    up_ref, down_ref = refs[-2:]
    first = first_ref[0] == 1
    kept = jnp.concatenate([r[...] for r in refs[:pieces]])
    other = jnp.concatenate([r[...] for r in refs[pieces : 2 * pieces]])
    up_ref[0] = jnp.where(first, kept, other).T
    down_ref[0] = jnp.where(first, other, kept)


def place_call(first, kept, other, layer, start, layers, width, bufs):
    size, hidden = kept[0].shape
    step = min(size, LANES)
    row_spec = pl.BlockSpec((step, hidden), lambda i, first: (i, 0))
    out_shape = [jax.ShapeDtypeStruct((layers, hidden, width), F32), jax.ShapeDtypeStruct((layers, width, hidden), F32)]
    any_spec = pl.BlockSpec(memory_space=pl.ANY)
    count = 2 * len(kept)
    return pl.pallas_call(
        functools.partial(place_body, len(kept)),
        out_shape=out_shape,
        grid_spec=pltpu.PrefetchScalarGridSpec(
            num_scalar_prefetch=1,
            grid=(size // step,),
            in_specs=[row_spec] * count + ([any_spec, any_spec] if bufs is not None else []),
            out_specs=[
                pl.BlockSpec((1, hidden, LANES), lambda i, first: (layer, 0, start // LANES + i)),
                pl.BlockSpec((1, LANES, hidden), lambda i, first: (layer, start // LANES + i, 0)),
            ],
        ),
        input_output_aliases={1 + count: 0, 2 + count: 1} if bufs is not None else {},
        compiler_params=pltpu.CompilerParams(dimension_semantics=("arbitrary",), vmem_limit_bytes=ALL_VMEM),
        cost_estimate=pl.CostEstimate(flops=4 * size * hidden, bytes_accessed=16 * size * hidden, transcendentals=0),
    )(first, *kept, *other, *(bufs or ()))


def solution(mesh):
    n_model = mesh.shape["model"]

    def to_model(value, flip):
        return lax.ppermute(value, "model", [(i, i ^ flip) for i in range(n_model)])

    def to_data(value):
        return lax.ppermute(value, "data", [(0, 1), (1, 0)])

    def all_blocks(x_saved, h_saved, w_up, w_down, grad_out):
        me = lax.axis_index("model")
        first = lax.axis_index("data") == 0
        first_flag = jnp.reshape(first, (1,)).astype(jnp.int32)
        quarter = jnp.reshape(me, (1,)).astype(jnp.int32)
        layers = w_up.shape[0]
        rows, seq = grad_out.shape[:2]
        width = h_saved.shape[-1]

        held = [h_saved, None]

        def h_from(layer, flip, start=0, size=width):
            held[0], held[1] = lax.optimization_barrier((held[0], held[1]))
            begin = (me ^ flip) * seq
            held[1] = lax.dynamic_slice(held[0], (layer, 0, begin, start), (1, rows, seq, size))[0]
            return to_model(held[1], flip)

        held[1] = jnp.where(first, w_up[1], w_down[1])
        far_w = [None, to_model(held[1], 2)]
        h_one = [h_from(1, 2), h_from(1, 3)]
        h_near = [None, h_from(1, 1)]
        w_pair = lax.optimization_barrier((w_up, w_down, held[1]))
        far_w[0] = jnp.where(first, w_pair[0][0], w_pair[1][0])
        far_w[0] = to_model(far_w[0], 2)
        h_near[0] = h_from(0, 1)
        h_zero = []
        for j, size in enumerate(BLOCKS):
            start = sum(BLOCKS[:j])
            h_zero.append([h_from(0, 2, start, size), h_from(0, 3, start, size)])
        small_start = width - LANES
        packed = []
        for flip in (2, 3):
            packed.append(pack_call(jnp.reshape(me ^ flip, (1,)).astype(jnp.int32), h_saved, 0, small_start, seq))
        h_small = [[to_model(packed[0][j], 2), to_model(packed[1][j], 3)] for j in range(3)]

        up, down = [{0: w_up} for _ in range(layers)], [{0: w_down} for _ in range(layers)]
        near_up, near_down = to_model(w_up, 1), to_model(w_down, 1)
        for layer in range(layers):
            other = to_data(far_w[layer])
            up[layer][1], down[layer][1] = near_up, near_down
            up[layer][2], down[layer][2] = jnp.where(first, far_w[layer], other), jnp.where(first, other, far_w[layer])
            up[layer][3] = to_model(up[layer][2], 1)
            down[layer][3] = to_model(down[layer][2], 1)

        def call(layer, grad, hs, flips, carry, final, start=0, size=width):
            ups, downs = [up[layer][f] for f in flips], [down[layer][f] for f in flips]
            return block_call(quarter, layer, grad, x_saved, hs, ups, downs, start, size, carry, final)

        def partial_sum(keep, give):
            theirs = to_model(give, 1)
            stay, away = pair_call(first_flag, keep, theirs)
            return stay + to_data(away)

        def place(pieces, layer, start, bufs):
            kept, other = zip(*pieces)
            return place_call(first_flag, kept, other, layer, start, layers, width, bufs)

        carry, dw_0, dw_1 = call(1, grad_out, [h_saved, h_near[1]], (0, 1), None, False)
        near = partial_sum(dw_0, dw_1)
        grad_mid, dw_2, dw_3 = call(1, grad_out, h_one, (2, 3), carry, True)
        far = partial_sum(dw_2, dw_3)
        kept = near + to_model(far, 2)
        bufs = place([(kept, to_data(kept))], 1, 0, None)

        carry, dw_0, dw_1 = call(0, grad_mid, [h_saved, h_near[0]], (0, 1), None, False)
        near = partial_sum(dw_0, dw_1)
        units = [(0, 0, 384), (1, 384, 128), (1, 512, 128), (2, small_start, SMALL), (3, small_start + SMALL, SMALL)]
        near_part = lax.optimization_barrier(tuple(near[start : start + size] for _, start, size in units))
        down_pair, up_pair = [down[0][f] for f in (2, 3)], [up[0][f] for f in (2, 3)]
        small_up = join_call(up_pair, small_start)
        pieces = []
        for j in range(4):
            base = sum(BLOCKS[:j]) if j < 2 else small_start + (j - 2) * SMALL
            if j == 0:
                carry, dw_2, dw_3 = call(0, grad_mid, h_zero[j], (2, 3), carry, False, base, BLOCKS[j])
            elif j == 1:
                carry, dw_2, dw_3 = wide_call(0, grad_mid, x_saved, h_zero[j], up_pair, down_pair, base, carry)
            elif j == 2:
                dw_2, dw_3, pre_1 = small_call(0, grad_mid, x_saved, h_small[0], down_pair, base, 0, None, None)
            else:
                dw_2, dw_3, grad_x = small_call(
                    0, grad_mid, x_saved, h_small[1], down_pair, base, 0, None, (carry, pre_1, small_up))
                dw_2, dw_3, pre_2 = small_call(0, grad_mid, x_saved, h_small[2], down_pair, base, EARLY, (dw_2, dw_3), None)
            far = partial_sum(dw_2, dw_3)
            for u, (block, start, size) in enumerate(units):
                if block == j:
                    part = to_model(far[start - base : start - base + size], 2)
                    kept = near_part[u] + part
                    pieces.append((kept, to_data(kept)))
        for u in range(3):
            bufs = place([pieces[u]], 0, units[u][1], bufs)
        for half in range(2):
            grad_x = finish_call(carry, (pre_1, pre_2), small_up, half, grad_x)
        bufs = place(pieces[3:], 0, small_start, bufs)
        return grad_x, bufs[0], bufs[1]

    return jax.shard_map(
        all_blocks,
        mesh=mesh,
        in_specs=(P(None, "data", "model", None), P(None, "data", None, "model"), P(None, None, "model"), P(None, "model", None), P("data", "model", None)),
        out_specs=(P("data", "model", None), P(None, None, "model"), P(None, "model", None)),
        check_vma=False,
    )
```

```python
import functools

import jax
import jax.numpy as jnp
from jax import lax
from jax.experimental import pallas as pl
from jax.experimental.pallas import tpu as pltpu
from jax.sharding import PartitionSpec as P


BF16 = jnp.bfloat16
F32 = jnp.float32
BLOCKS = (384, 256)
LANES = 128
SMALL = 64
EARLY = 5
ALL_VMEM = 66_000_000


def gelu_parts(pre_act):
    root = 0.7978845608028654
    cubic = (0.134145 * pre_act) * pre_act
    gate = 0.5 + 0.5 * jnp.tanh(pre_act * (root + (root / 3) * cubic))
    gelu_out = pre_act * gate
    gelu_slope = gate + gelu_out * (1.0 - gate) * (2 * root + (2 * root) * cubic)
    return gelu_out, gelu_slope


def dot(lhs, rhs, lhs_dim, rhs_dim):
    return lax.dot_general(lhs, rhs, (((lhs_dim,), (rhs_dim,)), ((), ())), preferred_element_type=F32)


def unit_grads(grad, h, down):
    d_act = dot(grad, down, 1, 1)
    gelu_out, gelu_slope = gelu_parts(h.astype(F32))
    return (d_act * gelu_slope).astype(BF16), gelu_out.astype(BF16)


def block_body(has_carry, final, rows, start, _, *refs):
    refs = list(refs)
    grad_ref, x_ref, h_a, h_b, up_a, up_b, down_a, down_b = (refs.pop(0) for _ in range(8))
    carry_ref = refs.pop(0) if has_carry else None
    out_ref, dw_a, dw_b, h_ref, pre_ref, act_ref, sum_ref, dw_ref, up_ref, down_ref, sem = refs
    row, source = pl.program_id(0), pl.program_id(1)
    width = pre_ref.shape[1]

    @pl.when((row == 0) & (source == 0))
    def _():
        dw_ref[...] = jnp.zeros_like(dw_ref)
        for s, (up, down) in enumerate(((up_a, down_a), (up_b, down_b))):
            up_ref[s] = up[(0,) * (len(up.shape) - 2) + (slice(None), slice(start, start + width))]
            down_ref[s] = down[(0,) * (len(down.shape) - 2) + (slice(start, start + width),)]

    for s, ref in enumerate((h_a, h_b)):
        @pl.when(source == s)
        def _():
            h_ref[...] = ref[(0,) * (len(ref.shape) - 2)]

    grad = grad_ref[0]
    x = x_ref[0, 0]
    for low in range(0, width, 256):
        cols = slice(low, min(low + 256, width))
        pre_ref[:, cols], act_ref[:, cols] = unit_grads(grad, h_ref[:, cols], down_ref[source, cols, :])
    pre, act = pre_ref[...], act_ref[...]
    dw_ref[source, 0] += dot(pre, x, 0, 0)
    dw_ref[source, 1] += dot(act, grad, 0, 0)
    part = dot(pre, up_ref[source], 1, 1)

    @pl.when(source == 0)
    def _():
        sum_ref[...] = part + carry_ref[0] if has_carry else part

    @pl.when(source == 1)
    def _():
        total = sum_ref[...] + part
        out_ref[0] = (grad.astype(F32) + total).astype(BF16) if final else total

    copies = [pltpu.make_async_copy(dw_ref.at[s], dw, sem.at[s]) for s, dw in enumerate((dw_a, dw_b))]
    for s in range(2):
        @pl.when((row == rows - 1) & (source == s))
        def _():
            copies[s].start()

    @pl.when((row == rows - 1) & (source == 1))
    def _():
        copies[0].wait()
        copies[1].wait()


def block_call(quarter, layer, grad, x_saved, h_pair, ups, downs, start, width, carry, final):
    rows, seq, hidden = grad.shape

    def h_spec(h):
        if h.ndim == 4:
            return pl.BlockSpec((1, 1, seq, width), lambda b, s, ids: (layer, b, ids[0], 0))
        return pl.BlockSpec((1, seq, width), lambda b, s, ids: (b, 0, 0))

    def w_spec(w):
        shape = (1,) * (w.ndim - 2) + w.shape[-2:]
        return pl.BlockSpec(shape, lambda b, s, ids: (layer,) * (w.ndim - 2) + (0, 0), pipeline_mode=pl.Buffered(1))

    row_spec = pl.BlockSpec((1, seq, hidden), lambda b, s, ids: (b, 0, 0))
    any_spec = pl.BlockSpec(memory_space=pl.ANY)
    in_specs = [row_spec, pl.BlockSpec((1, 1, seq, hidden), lambda b, s, ids: (layer, b, 0, 0))]
    in_specs += [h_spec(h) for h in h_pair]
    in_specs += [w_spec(w) for w in (*ups, *downs)]
    operands = [grad, x_saved, *h_pair, *ups, *downs]
    if carry is not None:
        in_specs.append(row_spec)
        operands.append(carry)
    dw_shape = (2, width, hidden)
    return pl.pallas_call(
        functools.partial(block_body, carry is not None, final, rows, start),
        out_shape=[jax.ShapeDtypeStruct(grad.shape, BF16 if final else F32)] + [jax.ShapeDtypeStruct(dw_shape, F32)] * 2,
        grid_spec=pltpu.PrefetchScalarGridSpec(
            num_scalar_prefetch=1,
            grid=(rows, 2),
            in_specs=in_specs,
            out_specs=[row_spec, any_spec, any_spec],
            scratch_shapes=[pltpu.VMEM((seq, width), BF16)] * 3
            + [pltpu.VMEM((seq, hidden), F32), pltpu.VMEM((2,) + dw_shape, F32)]
            + [pltpu.VMEM((2, hidden, width), BF16), pltpu.VMEM((2, width, hidden), BF16), pltpu.SemaphoreType.DMA((2,))],
        ),
        compiler_params=pltpu.CompilerParams(dimension_semantics=("arbitrary", "arbitrary"), vmem_limit_bytes=ALL_VMEM),
        cost_estimate=pl.CostEstimate(
            flops=16 * rows * seq * hidden * width, bytes_accessed=8 * rows * seq * hidden, transcendentals=2 * rows * seq * width),
    )(quarter, *operands)


def swap_lanes(a, b):
    left = lax.broadcasted_iota(jnp.int32, a.shape, 1) < SMALL
    return jnp.where(left, a, pltpu.roll(b, SMALL, 1)), jnp.where(left, pltpu.roll(a, SMALL, 1), b)


def pack_body(chunk, _, lo_ref, hi_ref, left_ref, right_a, right_b):
    left, right = swap_lanes(lo_ref[0, 0].astype(F32), hi_ref[0, 0].astype(F32))
    left_ref[0] = left.astype(BF16)

    @pl.when(pl.program_id(0) < chunk)
    def _():
        right_a[0] = right.astype(BF16)

    @pl.when(pl.program_id(0) >= chunk)
    def _():
        right_b[0] = right.astype(BF16)


def pack_call(target, h_saved, layer, start, seq):
    pairs = h_saved.shape[1] // 2
    chunk = EARLY
    specs = [pl.BlockSpec((1, 1, seq, LANES), lambda b, ids, r=r: (layer, b + r * pairs, ids[0], start // LANES)) for r in range(2)]
    block = (1, seq, LANES)
    return pl.pallas_call(
        functools.partial(pack_body, chunk),
        out_shape=[jax.ShapeDtypeStruct((n, seq, LANES), BF16) for n in (pairs, chunk, pairs - chunk)],
        grid_spec=pltpu.PrefetchScalarGridSpec(
            num_scalar_prefetch=1,
            grid=(pairs,),
            in_specs=specs,
            out_specs=[
                pl.BlockSpec(block, lambda b, ids: (b, 0, 0)),
                pl.BlockSpec(block, lambda b, ids: (jnp.minimum(b, chunk - 1), 0, 0)),
                pl.BlockSpec(block, lambda b, ids: (jnp.maximum(b - chunk, 0), 0, 0)),
            ],
        ),
        compiler_params=pltpu.CompilerParams(dimension_semantics=("arbitrary",), vmem_limit_bytes=ALL_VMEM),
        cost_estimate=pl.CostEstimate(flops=pairs * seq * LANES, bytes_accessed=8 * pairs * seq * LANES, transcendentals=0),
    )(target, h_saved, h_saved)


def wide_body(start, grad_ref, x_ref, h_a, h_b, up_a, up_b, down_a, down_b, carry_ref, out_ref, dw_a, dw_b):
    @pl.when(pl.program_id(0) == 0)
    def _():
        dw_a[...] = jnp.zeros_like(dw_a)
        dw_b[...] = jnp.zeros_like(dw_b)

    grad, x = grad_ref[0], x_ref[0, 0]
    cols = slice(start, start + h_a.shape[2])
    total = grad.astype(F32) + carry_ref[0]
    for h, up, down, dw in ((h_a, up_a, down_a, dw_a), (h_b, up_b, down_b, dw_b)):
        pre, act = unit_grads(grad, h[0], down[cols, :])
        dw[0] += dot(pre, x, 0, 0)
        dw[1] += dot(act, grad, 0, 0)
        total += dot(pre, up[:, cols], 1, 1)
    out_ref[0] = total


def wide_call(layer, grad, x_saved, h_pair, ups, downs, start, carry):
    rows, seq, hidden = grad.shape
    width = h_pair[0].shape[2]
    row_spec = pl.BlockSpec((1, seq, hidden), lambda b: (b, 0, 0))
    h_spec = pl.BlockSpec((1, seq, width), lambda b: (b, 0, 0))
    w_spec = pl.BlockSpec(ups[0].shape, lambda b: (0, 0), pipeline_mode=pl.Buffered(1))
    dw_shape = (2, width, hidden)
    return pl.pallas_call(
        functools.partial(wide_body, start),
        out_shape=[jax.ShapeDtypeStruct(grad.shape, F32)] + [jax.ShapeDtypeStruct(dw_shape, F32)] * 2,
        grid=(rows,),
        in_specs=[row_spec, pl.BlockSpec((1, 1, seq, hidden), lambda b: (layer, b, 0, 0)), h_spec, h_spec]
        + [w_spec] * 4 + [row_spec],
        out_specs=[row_spec] + [pl.BlockSpec(dw_shape, lambda b: (0, 0, 0), pipeline_mode=pl.Buffered(1))] * 2,
        compiler_params=pltpu.CompilerParams(dimension_semantics=("arbitrary",), vmem_limit_bytes=ALL_VMEM),
        cost_estimate=pl.CostEstimate(
            flops=16 * rows * seq * hidden * width, bytes_accessed=12 * rows * seq * hidden, transcendentals=2 * rows * seq * width),
    )(grad, x_saved, *h_pair, *ups, *downs, carry)


def small_body(has_init, finish, grad_ref, x_ref, h_a, h_b, down_a, down_b, *refs):
    refs = list(refs)
    carry_ref, early_ref, up_ref = (refs.pop(0) for _ in range(3)) if finish else (None,) * 3
    dw_pair, out_ref = refs[-3:-1], refs[-1]

    @pl.when(pl.program_id(0) == 0)
    def _():
        for i, dw in enumerate(dw_pair):
            dw[...] = refs[i][...] if has_init else jnp.zeros_like(dw)

    h_pair = swap_lanes(h_a[0].astype(F32), h_b[0].astype(F32))
    down = jnp.concatenate([down_a[...], down_b[...]])
    for r, h in enumerate(h_pair):
        grad, x = grad_ref[r, 0], x_ref[0, r, 0]
        pre, act = unit_grads(grad, h, down)
        for kind, part in enumerate((dot(pre, x, 0, 0), dot(act, grad, 0, 0))):
            dw_pair[0][kind] += part[:SMALL]
            dw_pair[1][kind] += part[SMALL:]
        if finish:
            total = carry_ref[r, 0] + dot(jnp.concatenate([early_ref[r, 0], pre], axis=1), up_ref[...], 1, 1)
            out_ref[r, 0] = total.astype(BF16)
        else:
            out_ref[r, 0] = pre


def paired(value, axis=0):
    shape = value.shape
    return value.reshape(shape[:axis] + (2, shape[axis] // 2) + shape[axis + 1 :])


def small_call(layer, grad, x_saved, h_pair, down_pair, start, first_pair, init, finish):
    _, _, seq, hidden = grad.shape
    pairs = h_pair[0].shape[0]
    row_spec = pl.BlockSpec((2, 1, seq, hidden), lambda b: (0, b + first_pair, 0, 0))
    pre_spec = pl.BlockSpec((2, 1, seq, LANES), lambda b: (0, b, 0, 0))
    h_spec = pl.BlockSpec((1, seq, LANES), lambda b: (b, 0, 0))
    down_spec = pl.BlockSpec((SMALL, hidden), lambda b: (start // SMALL, 0))
    dw_shape = (2, SMALL, hidden)
    dw_spec = pl.BlockSpec(dw_shape, lambda b: (0, 0, 0))
    in_specs = [row_spec, pl.BlockSpec((1, 2, 1, seq, hidden), lambda b: (layer, 0, b + first_pair, 0, 0)), h_spec, h_spec, down_spec, down_spec]
    if finish:
        in_specs += [row_spec, pre_spec, pl.BlockSpec(finish[2].shape, lambda b: (0, 0))]
    if init:
        in_specs += [dw_spec] * 2
    return pl.pallas_call(
        functools.partial(small_body, init is not None, finish is not None),
        out_shape=[jax.ShapeDtypeStruct(dw_shape, F32)] * 2
        + [jax.ShapeDtypeStruct(grad.shape if finish else (2, pairs, seq, LANES), BF16)],
        grid=(pairs,),
        in_specs=in_specs,
        out_specs=[dw_spec, dw_spec, row_spec if finish else pre_spec],
        compiler_params=pltpu.CompilerParams(dimension_semantics=("arbitrary",), vmem_limit_bytes=ALL_VMEM),
        cost_estimate=pl.CostEstimate(
            flops=24 * pairs * seq * hidden * SMALL, bytes_accessed=8 * pairs * seq * hidden, transcendentals=4 * pairs * seq * SMALL),
    )(grad, x_saved, *h_pair, *down_pair, *(finish or ()), *(init or ()))


def join_body(up_a, up_b, out_ref):
    first, second = swap_lanes(up_a[...].astype(F32), up_b[...].astype(F32))
    out_ref[:, :LANES], out_ref[:, LANES:] = first.astype(BF16), second.astype(BF16)


def join_call(up_pair, start):
    hidden = up_pair[0].shape[0]
    up_spec = pl.BlockSpec((hidden, LANES), lambda i: (0, start // LANES))
    return pl.pallas_call(
        join_body,
        out_shape=jax.ShapeDtypeStruct((hidden, 2 * LANES), BF16),
        grid=(1,),
        in_specs=[up_spec, up_spec],
        out_specs=pl.BlockSpec((hidden, 2 * LANES), lambda i: (0, 0)),
        compiler_params=pltpu.CompilerParams(dimension_semantics=("arbitrary",), vmem_limit_bytes=ALL_VMEM),
        cost_estimate=pl.CostEstimate(flops=hidden * LANES, bytes_accessed=8 * hidden * LANES, transcendentals=0),
    )(*up_pair)


def finish_body(carry_ref, pre_a, pre_b, up_ref, _, out_ref):
    total = carry_ref[0, 0] + dot(jnp.concatenate([pre_a[0, 0], pre_b[0, 0]], axis=1), up_ref[...], 1, 1)
    out_ref[0, 0] = total.astype(BF16)


def finish_call(carry, pre_pair, ups, half, out):
    _, pairs, seq, hidden = carry.shape
    count = pairs - EARLY
    row_spec = pl.BlockSpec((1, 1, seq, hidden), lambda b: (half, b + EARLY, 0, 0))
    pre_specs = [pl.BlockSpec((1, 1, seq, LANES), lambda b, first=first: (half, b + first, 0, 0)) for first in (EARLY, 0)]
    return pl.pallas_call(
        finish_body,
        out_shape=jax.ShapeDtypeStruct(carry.shape, BF16),
        grid=(count,),
        in_specs=[row_spec, *pre_specs, pl.BlockSpec(ups.shape, lambda b: (0, 0)), pl.BlockSpec(memory_space=pl.ANY)],
        out_specs=row_spec,
        input_output_aliases={4: 0},
        compiler_params=pltpu.CompilerParams(dimension_semantics=("arbitrary",), vmem_limit_bytes=ALL_VMEM),
        cost_estimate=pl.CostEstimate(flops=4 * count * seq * hidden * LANES, bytes_accessed=7 * count * seq * hidden, transcendentals=0),
    )(carry, *pre_pair, ups, out)


def pair_body(first_ref, mine_ref, theirs_ref, stay_ref, away_ref):
    first = first_ref[0] == 1
    up, down = mine_ref[0] + theirs_ref[0], mine_ref[1] + theirs_ref[1]
    stay_ref[...] = jnp.where(first, up, down)
    away_ref[...] = jnp.where(first, down, up)


def pair_call(first, mine, theirs):
    _, size, hidden = mine.shape
    step = min(size, LANES)
    both_spec = pl.BlockSpec((2, step, hidden), lambda i, first: (0, i, 0))
    one_spec = pl.BlockSpec((step, hidden), lambda i, first: (i, 0))
    return pl.pallas_call(
        pair_body,
        out_shape=[jax.ShapeDtypeStruct((size, hidden), F32)] * 2,
        grid_spec=pltpu.PrefetchScalarGridSpec(
            num_scalar_prefetch=1, grid=(size // step,), in_specs=[both_spec] * 2, out_specs=[one_spec] * 2),
        compiler_params=pltpu.CompilerParams(dimension_semantics=("arbitrary",), vmem_limit_bytes=ALL_VMEM),
        cost_estimate=pl.CostEstimate(flops=4 * mine.size, bytes_accessed=12 * mine.size, transcendentals=0),
    )(first, mine, theirs)


def place_body(pieces, first_ref, *refs):
    up_ref, down_ref = refs[-2:]
    first = first_ref[0] == 1
    kept = jnp.concatenate([r[...] for r in refs[:pieces]])
    other = jnp.concatenate([r[...] for r in refs[pieces : 2 * pieces]])
    up_ref[0] = jnp.where(first, kept, other).T
    down_ref[0] = jnp.where(first, other, kept)


def place_call(first, kept, other, layer, start, layers, width, bufs):
    hidden = kept[0].shape[1]
    size = sum(k.shape[0] for k in kept)
    step = LANES if len(kept) == 1 else size
    out_shape = [jax.ShapeDtypeStruct((layers, hidden, width), F32), jax.ShapeDtypeStruct((layers, width, hidden), F32)]
    any_spec = pl.BlockSpec(memory_space=pl.ANY)
    count = 2 * len(kept)
    piece_specs = [pl.BlockSpec((min(k.shape[0], step) if len(kept) == 1 else k.shape[0], hidden), lambda i, first: (i, 0)) for k in kept]
    return pl.pallas_call(
        functools.partial(place_body, len(kept)),
        out_shape=out_shape,
        grid_spec=pltpu.PrefetchScalarGridSpec(
            num_scalar_prefetch=1,
            grid=(size // step,),
            in_specs=piece_specs * 2 + ([any_spec, any_spec] if bufs is not None else []),
            out_specs=[
                pl.BlockSpec((1, hidden, step), lambda i, first: (layer, 0, start // step + i)),
                pl.BlockSpec((1, step, hidden), lambda i, first: (layer, start // step + i, 0)),
            ],
        ),
        input_output_aliases={1 + count: 0, 2 + count: 1} if bufs is not None else {},
        compiler_params=pltpu.CompilerParams(dimension_semantics=("arbitrary",), vmem_limit_bytes=ALL_VMEM),
        cost_estimate=pl.CostEstimate(flops=4 * size * hidden, bytes_accessed=16 * size * hidden, transcendentals=0),
    )(first, *kept, *other, *(bufs or ()))


def solution(mesh):
    n_model = mesh.shape["model"]

    def to_model(value, flip):
        return lax.ppermute(value, "model", [(i, i ^ flip) for i in range(n_model)])

    def to_data(value):
        return lax.ppermute(value, "data", [(0, 1), (1, 0)])

    def all_blocks(x_saved, h_saved, w_up, w_down, grad_out):
        me = lax.axis_index("model")
        first = lax.axis_index("data") == 0
        first_flag = jnp.reshape(first, (1,)).astype(jnp.int32)
        quarter = jnp.reshape(me, (1,)).astype(jnp.int32)
        layers = w_up.shape[0]
        rows, seq = grad_out.shape[:2]
        width = h_saved.shape[-1]

        held = [h_saved, None]

        def h_from(layer, flip, start=0, size=width):
            held[0], held[1] = lax.optimization_barrier((held[0], held[1]))
            begin = (me ^ flip) * seq
            held[1] = lax.dynamic_slice(held[0], (layer, 0, begin, start), (1, rows, seq, size))[0]
            return to_model(held[1], flip)

        held[1] = jnp.where(first, w_up[1], w_down[1])
        far_w = [None, to_model(held[1], 2)]
        h_one = [h_from(1, 2), h_from(1, 3)]
        h_near = [None, h_from(1, 1)]
        w_pair = lax.optimization_barrier((w_up, w_down, held[1]))
        far_w[0] = jnp.where(first, w_pair[0][0], w_pair[1][0])
        far_w[0] = to_model(far_w[0], 2)
        h_near[0] = h_from(0, 1)
        h_zero = []
        for j, size in enumerate(BLOCKS):
            start = sum(BLOCKS[:j])
            h_zero.append([h_from(0, 2, start, size), h_from(0, 3, start, size)])
        small_start = width - LANES
        packed = []
        for flip in (2, 3):
            packed.append(pack_call(jnp.reshape(me ^ flip, (1,)).astype(jnp.int32), h_saved, 0, small_start, seq))
        h_small = [[to_model(packed[0][j], 2), to_model(packed[1][j], 3)] for j in range(3)]

        up, down = [{0: w_up} for _ in range(layers)], [{0: w_down} for _ in range(layers)]
        near_up, near_down = to_model(w_up, 1), to_model(w_down, 1)
        for layer in range(layers):
            other = to_data(far_w[layer])
            up[layer][1], down[layer][1] = near_up, near_down
            up[layer][2], down[layer][2] = jnp.where(first, far_w[layer], other), jnp.where(first, other, far_w[layer])
            up[layer][3] = to_model(up[layer][2], 1)
            down[layer][3] = to_model(down[layer][2], 1)

        def call(layer, grad, hs, flips, carry, final, start=0, size=width):
            ups, downs = [up[layer][f] for f in flips], [down[layer][f] for f in flips]
            return block_call(quarter, layer, grad, x_saved, hs, ups, downs, start, size, carry, final)

        def partial_sum(keep, give):
            theirs = to_model(give, 1)
            stay, away = pair_call(first_flag, keep, theirs)
            return stay + to_data(away)

        def place(pieces, layer, start, bufs):
            kept, other = zip(*pieces)
            return place_call(first_flag, kept, other, layer, start, layers, width, bufs)

        carry, dw_0, dw_1 = call(1, grad_out, [h_saved, h_near[1]], (0, 1), None, False)
        near = partial_sum(dw_0, dw_1)
        grad_mid, dw_2, dw_3 = call(1, grad_out, h_one, (2, 3), carry, True)
        far = partial_sum(dw_2, dw_3)
        kept = near + to_model(far, 2)
        bufs = place([(kept, to_data(kept))], 1, 0, None)

        carry, dw_0, dw_1 = call(0, grad_mid, [h_saved, h_near[0]], (0, 1), None, False)
        near = partial_sum(dw_0, dw_1)
        bounds = [0, 384, 512, width - SMALL, width]
        near_part = lax.optimization_barrier(tuple(near[a:b] for a, b in zip(bounds, bounds[1:])))
        pieces = []

        def exchange(unit, far):
            part = to_model(far, 2)
            kept = near_part[unit] + part
            pieces.append((kept, to_data(kept)))

        down_pair, up_pair = [down[0][f] for f in (2, 3)], [up[0][f] for f in (2, 3)]
        small_up = join_call(up_pair, small_start)
        carry, dw_2, dw_3 = call(0, grad_mid, h_zero[0], (2, 3), carry, False, 0, BLOCKS[0])
        exchange(0, partial_sum(dw_2, dw_3))
        carry, dw_2, dw_3 = wide_call(0, grad_mid, x_saved, h_zero[1], up_pair, down_pair, BLOCKS[0], carry)
        far = partial_sum(dw_2, dw_3)
        exchange(1, far[: bounds[2] - bounds[1]])
        carry, grad_mid, x_saved = paired(carry), paired(grad_mid), paired(x_saved, 1)
        dw_2, dw_3, pre_1 = small_call(0, grad_mid, x_saved, h_small[0], down_pair, small_start, 0, None, None)
        exchange(2, jnp.concatenate([far[bounds[2] - bounds[1] :], partial_sum(dw_2, dw_3)]))
        dw_2, dw_3, grad_x = small_call(
            0, grad_mid, x_saved, h_small[1], down_pair, small_start + SMALL, 0, None, (carry, pre_1, small_up))
        dw_2, dw_3, pre_2 = small_call(
            0, grad_mid, x_saved, h_small[2], down_pair, small_start + SMALL, EARLY, (dw_2, dw_3), None)
        exchange(3, partial_sum(dw_2, dw_3))
        for half in range(2):
            grad_x = finish_call(carry, (pre_1, pre_2), small_up, half, grad_x)
        for unit in range(2):
            bufs = place([pieces[unit]], 0, bounds[unit], bufs)
        bufs = place(pieces[2:], 0, bounds[2], bufs)
        grad_x = grad_x.reshape(grad_out.shape)
        return grad_x, bufs[0], bufs[1]

    return jax.shard_map(
        all_blocks,
        mesh=mesh,
        in_specs=(P(None, "data", "model", None), P(None, "data", None, "model"), P(None, None, "model"), P(None, "model", None), P("data", "model", None)),
        out_specs=(P("data", "model", None), P(None, None, "model"), P(None, "model", None)),
        check_vma=False,
    )
```

```python
import functools

import jax
import jax.numpy as jnp
from jax import lax
from jax.experimental import pallas as pl
from jax.experimental.pallas import tpu as pltpu
from jax.sharding import PartitionSpec as P


BF16 = jnp.bfloat16
F32 = jnp.float32
BLOCKS = (384, 256)
LANES = 128
SMALL = 64
CHUNKS = (3, 3, 2)
FIRST = 192
ALL_VMEM = 66_000_000


def gelu_parts(pre_act):
    root = 0.7978845608028654
    cubic = (0.134145 * pre_act) * pre_act
    gate = 0.5 + 0.5 * jnp.tanh(pre_act * (root + (root / 3) * cubic))
    gelu_out = pre_act * gate
    gelu_slope = gate + gelu_out * (1.0 - gate) * (2 * root + (2 * root) * cubic)
    return gelu_out, gelu_slope


def dot(lhs, rhs, lhs_dim, rhs_dim):
    return lax.dot_general(lhs, rhs, (((lhs_dim,), (rhs_dim,)), ((), ())), preferred_element_type=F32)


def unit_grads(grad, h, down):
    d_act = dot(grad, down, 1, 1)
    gelu_out, gelu_slope = gelu_parts(h.astype(F32))
    return (d_act * gelu_slope).astype(BF16), gelu_out.astype(BF16)


def block_body(has_carry, final, rows, start, _, *refs):
    refs = list(refs)
    grad_ref, x_ref, h_a, h_b, up_a, up_b, down_a, down_b = (refs.pop(0) for _ in range(8))
    carry_ref = refs.pop(0) if has_carry else None
    out_ref, dw_a, dw_b, h_ref, pre_ref, act_ref, sum_ref, dw_ref, up_ref, down_ref, sem = refs
    row, source = pl.program_id(0), pl.program_id(1)
    width = pre_ref.shape[1]

    @pl.when((row == 0) & (source == 0))
    def _():
        dw_ref[...] = jnp.zeros_like(dw_ref)
        for s, (up, down) in enumerate(((up_a, down_a), (up_b, down_b))):
            up_ref[s] = up[(0,) * (len(up.shape) - 2) + (slice(None), slice(start, start + width))]
            down_ref[s] = down[(0,) * (len(down.shape) - 2) + (slice(start, start + width),)]

    for s, ref in enumerate((h_a, h_b)):
        @pl.when(source == s)
        def _():
            h_ref[...] = ref[(0,) * (len(ref.shape) - 2)]

    grad = grad_ref[0]
    x = x_ref[0, 0]
    for low in range(0, width, 256):
        cols = slice(low, min(low + 256, width))
        pre_ref[:, cols], act_ref[:, cols] = unit_grads(grad, h_ref[:, cols], down_ref[source, cols, :])
    pre, act = pre_ref[...], act_ref[...]
    dw_ref[source, 0] += dot(pre, x, 0, 0)
    dw_ref[source, 1] += dot(act, grad, 0, 0)
    part = dot(pre, up_ref[source], 1, 1)

    @pl.when(source == 0)
    def _():
        sum_ref[...] = part + carry_ref[0] if has_carry else part

    @pl.when(source == 1)
    def _():
        total = sum_ref[...] + part
        out_ref[0] = (grad.astype(F32) + total).astype(BF16) if final else total

    copies = [pltpu.make_async_copy(dw_ref.at[s], dw, sem.at[s]) for s, dw in enumerate((dw_a, dw_b))]
    for s in range(2):
        @pl.when((row == rows - 1) & (source == s))
        def _():
            copies[s].start()

    @pl.when((row == rows - 1) & (source == 1))
    def _():
        copies[0].wait()
        copies[1].wait()


def block_call(quarter, layer, grad, x_saved, h_pair, ups, downs, start, width, carry, final):
    rows, seq, hidden = grad.shape

    def h_spec(h):
        if h.ndim == 4:
            return pl.BlockSpec((1, 1, seq, width), lambda b, s, ids: (layer, b, ids[0], 0))
        return pl.BlockSpec((1, seq, width), lambda b, s, ids: (b, 0, 0))

    def w_spec(w):
        shape = (1,) * (w.ndim - 2) + w.shape[-2:]
        return pl.BlockSpec(shape, lambda b, s, ids: (layer,) * (w.ndim - 2) + (0, 0), pipeline_mode=pl.Buffered(1))

    row_spec = pl.BlockSpec((1, seq, hidden), lambda b, s, ids: (b, 0, 0))
    any_spec = pl.BlockSpec(memory_space=pl.ANY)
    in_specs = [row_spec, pl.BlockSpec((1, 1, seq, hidden), lambda b, s, ids: (layer, b, 0, 0))]
    in_specs += [h_spec(h) for h in h_pair]
    in_specs += [w_spec(w) for w in (*ups, *downs)]
    operands = [grad, x_saved, *h_pair, *ups, *downs]
    if carry is not None:
        in_specs.append(row_spec)
        operands.append(carry)
    dw_shape = (2, width, hidden)
    return pl.pallas_call(
        functools.partial(block_body, carry is not None, final, rows, start),
        out_shape=[jax.ShapeDtypeStruct(grad.shape, BF16 if final else F32)] + [jax.ShapeDtypeStruct(dw_shape, F32)] * 2,
        grid_spec=pltpu.PrefetchScalarGridSpec(
            num_scalar_prefetch=1,
            grid=(rows, 2),
            in_specs=in_specs,
            out_specs=[row_spec, any_spec, any_spec],
            scratch_shapes=[pltpu.VMEM((seq, width), BF16)] * 3
            + [pltpu.VMEM((seq, hidden), F32), pltpu.VMEM((2,) + dw_shape, F32)]
            + [pltpu.VMEM((2, hidden, width), BF16), pltpu.VMEM((2, width, hidden), BF16), pltpu.SemaphoreType.DMA((2,))],
        ),
        compiler_params=pltpu.CompilerParams(dimension_semantics=("arbitrary", "arbitrary"), vmem_limit_bytes=ALL_VMEM),
        cost_estimate=pl.CostEstimate(
            flops=16 * rows * seq * hidden * width, bytes_accessed=8 * rows * seq * hidden, transcendentals=2 * rows * seq * width),
    )(quarter, *operands)


def swap_lanes(a, b):
    left = lax.broadcasted_iota(jnp.int32, a.shape, 1) < SMALL
    return jnp.where(left, a, pltpu.roll(b, SMALL, 1)), jnp.where(left, pltpu.roll(a, SMALL, 1), b)


def pack_body(_, lo_ref, hi_ref, left_ref, *right_refs):
    left, right = swap_lanes(lo_ref[0, 0].astype(F32), hi_ref[0, 0].astype(F32))
    left_ref[0] = left.astype(BF16)
    for j, ref in enumerate(right_refs):
        low = sum(CHUNKS[:j])

        @pl.when((pl.program_id(0) >= low) & (pl.program_id(0) < low + CHUNKS[j]))
        def _():
            ref[0] = right.astype(BF16)


def pack_call(target, h_saved, layer, start, seq):
    pairs = h_saved.shape[1] // 2
    specs = [pl.BlockSpec((1, 1, seq, LANES), lambda b, ids, r=r: (layer, b + r * pairs, ids[0], start // LANES)) for r in range(2)]
    block = (1, seq, LANES)
    chunk_specs = [
        pl.BlockSpec(block, lambda b, ids, low=sum(CHUNKS[:j]), n=n: (jnp.clip(b - low, 0, n - 1), 0, 0)) for j, n in enumerate(CHUNKS)]
    return pl.pallas_call(
        pack_body,
        out_shape=[jax.ShapeDtypeStruct((n, seq, LANES), BF16) for n in (pairs, *CHUNKS)],
        grid_spec=pltpu.PrefetchScalarGridSpec(
            num_scalar_prefetch=1,
            grid=(pairs,),
            in_specs=specs,
            out_specs=[pl.BlockSpec(block, lambda b, ids: (b, 0, 0)), *chunk_specs],
        ),
        compiler_params=pltpu.CompilerParams(dimension_semantics=("arbitrary",), vmem_limit_bytes=ALL_VMEM),
        cost_estimate=pl.CostEstimate(flops=pairs * seq * LANES, bytes_accessed=8 * pairs * seq * LANES, transcendentals=0),
    )(target, h_saved, h_saved)


def wide_body(start, grad_ref, x_ref, h_a, h_b, up_a, up_b, down_a, down_b, carry_ref, out_ref, dw_a, dw_b):
    @pl.when(pl.program_id(0) == 0)
    def _():
        dw_a[...] = jnp.zeros_like(dw_a)
        dw_b[...] = jnp.zeros_like(dw_b)

    grad, x = grad_ref[0], x_ref[0, 0]
    cols = slice(start, start + h_a.shape[2])
    total = grad.astype(F32) + carry_ref[0]
    for h, up, down, dw in ((h_a, up_a, down_a, dw_a), (h_b, up_b, down_b, dw_b)):
        pre, act = unit_grads(grad, h[0], down[cols, :])
        dw[0] += dot(pre, x, 0, 0)
        dw[1] += dot(act, grad, 0, 0)
        total += dot(pre, up[:, cols], 1, 1)
    out_ref[0] = total


def wide_call(layer, grad, x_saved, h_pair, ups, downs, start, carry):
    rows, seq, hidden = grad.shape
    width = h_pair[0].shape[2]
    row_spec = pl.BlockSpec((1, seq, hidden), lambda b: (b, 0, 0))
    h_spec = pl.BlockSpec((1, seq, width), lambda b: (b, 0, 0))
    w_spec = pl.BlockSpec(ups[0].shape, lambda b: (0, 0), pipeline_mode=pl.Buffered(1))
    dw_shape = (2, width, hidden)
    return pl.pallas_call(
        functools.partial(wide_body, start),
        out_shape=[jax.ShapeDtypeStruct(grad.shape, F32)] + [jax.ShapeDtypeStruct(dw_shape, F32)] * 2,
        grid=(rows,),
        in_specs=[row_spec, pl.BlockSpec((1, 1, seq, hidden), lambda b: (layer, b, 0, 0)), h_spec, h_spec]
        + [w_spec] * 4 + [row_spec],
        out_specs=[row_spec] + [pl.BlockSpec(dw_shape, lambda b: (0, 0, 0), pipeline_mode=pl.Buffered(1))] * 2,
        compiler_params=pltpu.CompilerParams(dimension_semantics=("arbitrary",), vmem_limit_bytes=ALL_VMEM),
        cost_estimate=pl.CostEstimate(
            flops=16 * rows * seq * hidden * width, bytes_accessed=12 * rows * seq * hidden, transcendentals=2 * rows * seq * width),
    )(grad, x_saved, *h_pair, *ups, *downs, carry)


def small_body(has_init, finish, grad_ref, x_ref, h_a, h_b, down_a, down_b, *refs):
    refs = list(refs)
    carry_ref, early_ref, up_ref = (refs.pop(0) for _ in range(3)) if finish else (None,) * 3
    dw_pair, out_ref = refs[-3:-1], refs[-1]

    @pl.when(pl.program_id(0) == 0)
    def _():
        for i, dw in enumerate(dw_pair):
            dw[...] = refs[i][...] if has_init else jnp.zeros_like(dw)

    h_pair = swap_lanes(h_a[0].astype(F32), h_b[0].astype(F32))
    down = jnp.concatenate([down_a[...], down_b[...]])
    for r, h in enumerate(h_pair):
        grad, x = grad_ref[r, 0], x_ref[0, r, 0]
        pre, act = unit_grads(grad, h, down)
        for kind, part in enumerate((dot(pre, x, 0, 0), dot(act, grad, 0, 0))):
            dw_pair[0][kind] += part[:SMALL]
            dw_pair[1][kind] += part[SMALL:]
        if finish:
            total = carry_ref[r, 0] + dot(jnp.concatenate([early_ref[r, 0], pre], axis=1), up_ref[...], 1, 1)
            out_ref[r, 0] = total.astype(BF16)
        else:
            out_ref[r, 0] = pre


def paired(value, axis=0):
    shape = value.shape
    return value.reshape(shape[:axis] + (2, shape[axis] // 2) + shape[axis + 1 :])


def small_call(layer, grad, x_saved, h_pair, down_pair, start, first_pair, init, finish):
    _, _, seq, hidden = grad.shape
    pairs = h_pair[0].shape[0]
    row_spec = pl.BlockSpec((2, 1, seq, hidden), lambda b: (0, b + first_pair, 0, 0))
    pre_spec = pl.BlockSpec((2, 1, seq, LANES), lambda b: (0, b, 0, 0))
    h_spec = pl.BlockSpec((1, seq, LANES), lambda b: (b, 0, 0))
    down_spec = pl.BlockSpec((SMALL, hidden), lambda b: (start // SMALL, 0))
    dw_shape = (2, SMALL, hidden)
    dw_spec = pl.BlockSpec(dw_shape, lambda b: (0, 0, 0))
    in_specs = [row_spec, pl.BlockSpec((1, 2, 1, seq, hidden), lambda b: (layer, 0, b + first_pair, 0, 0)), h_spec, h_spec, down_spec, down_spec]
    if finish:
        in_specs += [row_spec, pre_spec, pl.BlockSpec(finish[2].shape, lambda b: (0, 0))]
    if init:
        in_specs += [dw_spec] * 2
    return pl.pallas_call(
        functools.partial(small_body, init is not None, finish is not None),
        out_shape=[jax.ShapeDtypeStruct(dw_shape, F32)] * 2
        + [jax.ShapeDtypeStruct(grad.shape if finish else (2, pairs, seq, LANES), BF16)],
        grid=(pairs,),
        in_specs=in_specs,
        out_specs=[dw_spec, dw_spec, row_spec if finish else pre_spec],
        compiler_params=pltpu.CompilerParams(dimension_semantics=("arbitrary",), vmem_limit_bytes=ALL_VMEM),
        cost_estimate=pl.CostEstimate(
            flops=24 * pairs * seq * hidden * SMALL, bytes_accessed=8 * pairs * seq * hidden, transcendentals=4 * pairs * seq * SMALL),
    )(grad, x_saved, *h_pair, *down_pair, *(finish or ()), *(init or ()))


def join_body(up_a, up_b, out_ref):
    first, second = swap_lanes(up_a[...].astype(F32), up_b[...].astype(F32))
    out_ref[:, :LANES], out_ref[:, LANES:] = first.astype(BF16), second.astype(BF16)


def join_call(up_pair, start):
    hidden = up_pair[0].shape[0]
    up_spec = pl.BlockSpec((hidden, LANES), lambda i: (0, start // LANES))
    return pl.pallas_call(
        join_body,
        out_shape=jax.ShapeDtypeStruct((hidden, 2 * LANES), BF16),
        grid=(1,),
        in_specs=[up_spec, up_spec],
        out_specs=pl.BlockSpec((hidden, 2 * LANES), lambda i: (0, 0)),
        compiler_params=pltpu.CompilerParams(dimension_semantics=("arbitrary",), vmem_limit_bytes=ALL_VMEM),
        cost_estimate=pl.CostEstimate(flops=hidden * LANES, bytes_accessed=8 * hidden * LANES, transcendentals=0),
    )(*up_pair)


def finish_body(carry_ref, pre_a, pre_b, up_ref, _, out_ref):
    total = carry_ref[0, 0] + dot(jnp.concatenate([pre_a[0, 0], pre_b[0, 0]], axis=1), up_ref[...], 1, 1)
    out_ref[0, 0] = total.astype(BF16)


def finish_call(carry, pre_pair, ups, first_pair, first_half, halves, out):
    _, _, seq, hidden = carry.shape
    count = pre_pair[1].shape[1]
    row_spec = pl.BlockSpec((1, 1, seq, hidden), lambda r, b: (r + first_half, b + first_pair, 0, 0))
    pre_specs = [pl.BlockSpec((1, 1, seq, LANES), lambda r, b, first=first: (r + first_half, b + first, 0, 0)) for first in (first_pair, 0)]
    rows = halves * count
    return pl.pallas_call(
        finish_body,
        out_shape=jax.ShapeDtypeStruct(carry.shape, BF16),
        grid=(halves, count),
        in_specs=[row_spec, *pre_specs, pl.BlockSpec(ups.shape, lambda r, b: (0, 0)), pl.BlockSpec(memory_space=pl.ANY)],
        out_specs=row_spec,
        input_output_aliases={4: 0},
        compiler_params=pltpu.CompilerParams(dimension_semantics=("arbitrary", "arbitrary"), vmem_limit_bytes=ALL_VMEM),
        cost_estimate=pl.CostEstimate(flops=4 * rows * seq * hidden * LANES, bytes_accessed=7 * rows * seq * hidden, transcendentals=0),
    )(carry, *pre_pair, ups, out)


def pair_body(first_ref, mine_ref, theirs_ref, stay_ref, away_ref):
    first = first_ref[0] == 1
    up, down = mine_ref[0] + theirs_ref[0], mine_ref[1] + theirs_ref[1]
    stay_ref[...] = jnp.where(first, up, down)
    away_ref[...] = jnp.where(first, down, up)


def pair_call(first, mine, theirs):
    _, size, hidden = mine.shape
    step = min(size, LANES)
    both_spec = pl.BlockSpec((2, step, hidden), lambda i, first: (0, i, 0))
    one_spec = pl.BlockSpec((step, hidden), lambda i, first: (i, 0))
    return pl.pallas_call(
        pair_body,
        out_shape=[jax.ShapeDtypeStruct((size, hidden), F32)] * 2,
        grid_spec=pltpu.PrefetchScalarGridSpec(
            num_scalar_prefetch=1, grid=(size // step,), in_specs=[both_spec] * 2, out_specs=[one_spec] * 2),
        compiler_params=pltpu.CompilerParams(dimension_semantics=("arbitrary",), vmem_limit_bytes=ALL_VMEM),
        cost_estimate=pl.CostEstimate(flops=4 * mine.size, bytes_accessed=12 * mine.size, transcendentals=0),
    )(first, mine, theirs)


def place_body(first_ref, kept_ref, other_ref, *refs):
    up_ref, down_ref = refs[-2:]
    first = first_ref[0] == 1
    kept, other = kept_ref[...], other_ref[...]
    up_ref[0] = jnp.where(first, kept, other).T
    down_ref[0] = jnp.where(first, other, kept)


def place_call(first, kept, other, layer, start, layers, width, bufs):
    size, hidden = kept.shape
    row_spec = pl.BlockSpec((LANES, hidden), lambda i, first: (i, 0))
    out_shape = [jax.ShapeDtypeStruct((layers, hidden, width), F32), jax.ShapeDtypeStruct((layers, width, hidden), F32)]
    any_spec = pl.BlockSpec(memory_space=pl.ANY)
    return pl.pallas_call(
        place_body,
        out_shape=out_shape,
        grid_spec=pltpu.PrefetchScalarGridSpec(
            num_scalar_prefetch=1,
            grid=(size // LANES,),
            in_specs=[row_spec, row_spec] + ([any_spec, any_spec] if bufs is not None else []),
            out_specs=[
                pl.BlockSpec((1, hidden, LANES), lambda i, first: (layer, 0, start // LANES + i)),
                pl.BlockSpec((1, LANES, hidden), lambda i, first: (layer, start // LANES + i, 0)),
            ],
        ),
        input_output_aliases={3: 0, 4: 1} if bufs is not None else {},
        compiler_params=pltpu.CompilerParams(dimension_semantics=("arbitrary",), vmem_limit_bytes=ALL_VMEM),
        cost_estimate=pl.CostEstimate(flops=4 * size * hidden, bytes_accessed=16 * size * hidden, transcendentals=0),
    )(first, kept, other, *(bufs or ()))


def join_place_body(count, layer, start, first_ref, *refs):
    up_out, down_out, up_ref, down_ref, sem = refs[-5:]
    first = first_ref[0] == 1
    kept = jnp.concatenate([r[...] for r in refs[:count]])
    other = jnp.concatenate([r[...] for r in refs[count : 2 * count]])
    size = kept.shape[0]
    down_ref[...] = jnp.where(first, other, kept)
    down_copy = pltpu.make_async_copy(down_ref, down_out.at[layer, pl.ds(start, size), :], sem.at[0])
    down_copy.start()
    up_ref[...] = jnp.where(first, kept, other).T
    up_copy = pltpu.make_async_copy(up_ref, up_out.at[layer, :, pl.ds(start, size)], sem.at[1])
    up_copy.start()
    down_copy.wait()
    up_copy.wait()


def join_place_call(first, pieces, layer, start, bufs):
    hidden = pieces[0][0].shape[1]
    size = sum(n for _, _, _, n in pieces)
    piece_specs = [pl.BlockSpec((n, hidden), lambda i, first, block=low // n: (block, 0)) for _, _, low, n in pieces]
    any_spec = pl.BlockSpec(memory_space=pl.ANY)
    count = len(pieces)
    return pl.pallas_call(
        functools.partial(join_place_body, count, layer, start),
        out_shape=[jax.ShapeDtypeStruct(b.shape, b.dtype) for b in bufs],
        grid_spec=pltpu.PrefetchScalarGridSpec(
            num_scalar_prefetch=1,
            grid=(1,),
            in_specs=piece_specs * 2 + [any_spec] * 2,
            out_specs=[any_spec] * 2,
            scratch_shapes=[pltpu.VMEM((hidden, size), F32), pltpu.VMEM((size, hidden), F32), pltpu.SemaphoreType.DMA((2,))],
        ),
        input_output_aliases={1 + 2 * count: 0, 2 + 2 * count: 1},
        compiler_params=pltpu.CompilerParams(dimension_semantics=("arbitrary",), vmem_limit_bytes=ALL_VMEM),
        cost_estimate=pl.CostEstimate(flops=4 * size * hidden, bytes_accessed=16 * size * hidden, transcendentals=0),
    )(first, *[p[0] for p in pieces], *[p[1] for p in pieces], *bufs)


def solution(mesh):
    n_model = mesh.shape["model"]

    def to_model(value, flip):
        return lax.ppermute(value, "model", [(i, i ^ flip) for i in range(n_model)])

    def to_data(value):
        return lax.ppermute(value, "data", [(0, 1), (1, 0)])

    def all_blocks(x_saved, h_saved, w_up, w_down, grad_out):
        me = lax.axis_index("model")
        first = lax.axis_index("data") == 0
        first_flag = jnp.reshape(first, (1,)).astype(jnp.int32)
        quarter = jnp.reshape(me, (1,)).astype(jnp.int32)
        layers = w_up.shape[0]
        rows, seq = grad_out.shape[:2]
        width = h_saved.shape[-1]

        held = [h_saved, None]

        def h_from(layer, flip, start=0, size=width):
            held[0], held[1] = lax.optimization_barrier((held[0], held[1]))
            begin = (me ^ flip) * seq
            held[1] = lax.dynamic_slice(held[0], (layer, 0, begin, start), (1, rows, seq, size))[0]
            return to_model(held[1], flip)

        head = jnp.where(first, w_up[1, :FIRST], w_down[1, :FIRST])
        w_pair = lax.optimization_barrier((w_up, w_down, head))
        held[1] = jnp.where(first, w_pair[0][1, FIRST:], w_pair[1][1, FIRST:])
        far_w = [None, jnp.concatenate([to_model(head, 2), to_model(held[1], 2)])]
        h_one = [h_from(1, 2), h_from(1, 3)]
        h_near = [None, h_from(1, 1)]
        w_pair = lax.optimization_barrier((w_up, w_down, held[1]))
        far_w[0] = jnp.where(first, w_pair[0][0], w_pair[1][0])
        far_w[0] = to_model(far_w[0], 2)
        h_near[0] = h_from(0, 1)
        h_zero = []
        for j, size in enumerate(BLOCKS):
            start = sum(BLOCKS[:j])
            h_zero.append([h_from(0, 2, start, size), h_from(0, 3, start, size)])
        small_start = width - LANES
        packed = []
        for flip in (2, 3):
            packed.append(pack_call(jnp.reshape(me ^ flip, (1,)).astype(jnp.int32), h_saved, 0, small_start, seq))
        h_small = [[to_model(packed[0][j], 2), to_model(packed[1][j], 3)] for j in range(4)]

        up, down = [{0: w_up} for _ in range(layers)], [{0: w_down} for _ in range(layers)]
        near_up, near_down = to_model(w_up, 1), to_model(w_down, 1)
        for layer in range(layers):
            other = to_data(far_w[layer])
            up[layer][1], down[layer][1] = near_up, near_down
            up[layer][2], down[layer][2] = jnp.where(first, far_w[layer], other), jnp.where(first, other, far_w[layer])
            up[layer][3] = to_model(up[layer][2], 1)
            down[layer][3] = to_model(down[layer][2], 1)

        def call(layer, grad, hs, flips, carry, final, start=0, size=width):
            ups, downs = [up[layer][f] for f in flips], [down[layer][f] for f in flips]
            return block_call(quarter, layer, grad, x_saved, hs, ups, downs, start, size, carry, final)

        def partial_sum(keep, give):
            theirs = to_model(give, 1)
            stay, away = pair_call(first_flag, keep, theirs)
            return stay + to_data(away)

        def place(pieces, layer, start, bufs):
            if len(pieces) > 1:
                return join_place_call(first_flag, pieces, layer, start, bufs)
            return place_call(first_flag, *pieces[0], layer, start, layers, width, bufs)

        carry, dw_0, dw_1 = call(1, grad_out, [h_saved, h_near[1]], (0, 1), None, False)
        near = partial_sum(dw_0, dw_1)
        grad_mid, dw_2, dw_3 = call(1, grad_out, h_one, (2, 3), carry, True)
        far = partial_sum(dw_2, dw_3)
        kept = near + to_model(far, 2)
        bufs = place([(kept, to_data(kept))], 1, 0, None)

        carry, dw_0, dw_1 = call(0, grad_mid, [h_saved, h_near[0]], (0, 1), None, False)
        near = partial_sum(dw_0, dw_1)
        bounds = [0, 384, 448, 576, width - SMALL, width]
        near_part = lax.optimization_barrier(tuple(near[a:b] for a, b in zip(bounds, bounds[1:])))
        pieces = []

        def exchange(unit, far):
            part = to_model(far, 2)
            kept = near_part[unit] + part
            pieces.append((kept, to_data(kept)))

        down_pair, up_pair = [down[0][f] for f in (2, 3)], [up[0][f] for f in (2, 3)]
        small_up = join_call(up_pair, small_start)
        carry, dw_2, dw_3 = call(0, grad_mid, h_zero[0], (2, 3), carry, False, 0, BLOCKS[0])
        exchange(0, partial_sum(dw_2, dw_3))
        carry, dw_2, dw_3 = wide_call(0, grad_mid, x_saved, h_zero[1], up_pair, down_pair, BLOCKS[0], carry)
        far = partial_sum(dw_2, dw_3)
        exchange(1, far[: bounds[2] - bounds[1]])
        exchange(2, far[bounds[2] - bounds[1] : bounds[3] - bounds[1]])
        carry, grad_mid, x_saved = paired(carry), paired(grad_mid), paired(x_saved, 1)
        dw_2, dw_3, pre_1 = small_call(0, grad_mid, x_saved, h_small[0], down_pair, small_start, 0, None, None)
        exchange(3, jnp.concatenate([far[bounds[3] - bounds[1] :], partial_sum(dw_2, dw_3)]))
        last = small_start + SMALL
        early, late = CHUNKS[0], CHUNKS[0] + CHUNKS[1]
        dw_2, dw_3, grad_x = small_call(0, grad_mid, x_saved, h_small[1], down_pair, last, 0, None, (carry, pre_1, small_up))
        dw_2, dw_3, pre_2 = small_call(0, grad_mid, x_saved, h_small[2], down_pair, last, early, (dw_2, dw_3), None)
        grad_x = finish_call(carry, (pre_1, pre_2), small_up, early, 0, 1, grad_x)
        dw_2, dw_3, pre_3 = small_call(0, grad_mid, x_saved, h_small[3], down_pair, last, late, (dw_2, dw_3), None)
        exchange(4, partial_sum(dw_2, dw_3))
        grad_x = finish_call(carry, (pre_1, pre_2), small_up, early, 1, 1, grad_x)
        grad_x = finish_call(carry, (pre_1, pre_3), small_up, late, 0, 2, grad_x)
        bufs = place([pieces[0]], 0, 0, bufs)
        middle = [(*pieces[1], 0, 64), (*pieces[2], 0, 128), (*pieces[3], 0, 64)]
        bufs = place(middle, 0, bounds[1], bufs)
        bufs = place([(*pieces[3], 64, 64), (*pieces[4], 0, 64)], 0, small_start, bufs)
        grad_x = grad_x.reshape(grad_out.shape)
        return grad_x, bufs[0], bufs[1]

    return jax.shard_map(
        all_blocks,
        mesh=mesh,
        in_specs=(P(None, "data", "model", None), P(None, "data", None, "model"), P(None, None, "model"), P(None, "model", None), P("data", "model", None)),
        out_specs=(P("data", "model", None), P(None, None, "model"), P(None, "model", None)),
        check_vma=False,
    )
```

```python
import functools

import jax
import jax.numpy as jnp
from jax import lax
from jax.experimental import pallas as pl
from jax.experimental.pallas import tpu as pltpu
from jax.sharding import PartitionSpec as P


BF16 = jnp.bfloat16
F32 = jnp.float32
BLOCKS = (384, 256)
LANES = 128
SMALL = 64
CHUNKS = (4, 2, 2)
FIRST = 192
ALL_VMEM = 66_000_000


def gelu_parts(pre_act):
    root = 0.7978845608028654
    cubic = (0.134145 * pre_act) * pre_act
    gate = 0.5 + 0.5 * jnp.tanh(pre_act * (root + (root / 3) * cubic))
    gelu_out = pre_act * gate
    gelu_slope = gate + gelu_out * (1.0 - gate) * (2 * root + (2 * root) * cubic)
    return gelu_out, gelu_slope


def dot(lhs, rhs, lhs_dim, rhs_dim):
    return lax.dot_general(lhs, rhs, (((lhs_dim,), (rhs_dim,)), ((), ())), preferred_element_type=F32)


def unit_grads(grad, h, down):
    d_act = dot(grad, down, 1, 1)
    gelu_out, gelu_slope = gelu_parts(h.astype(F32))
    return (d_act * gelu_slope).astype(BF16), gelu_out.astype(BF16)


def block_body(has_carry, final, rows, start, _, *refs):
    refs = list(refs)
    grad_ref, x_ref, h_a, h_b, up_a, up_b, down_a, down_b = (refs.pop(0) for _ in range(8))
    carry_ref = refs.pop(0) if has_carry else None
    out_ref, dw_a, dw_b, h_ref, pre_ref, act_ref, sum_ref, dw_ref, up_ref, down_ref, sem = refs
    row, source = pl.program_id(0), pl.program_id(1)
    width = pre_ref.shape[1]

    @pl.when((row == 0) & (source == 0))
    def _():
        dw_ref[...] = jnp.zeros_like(dw_ref)
        for s, (up, down) in enumerate(((up_a, down_a), (up_b, down_b))):
            up_ref[s] = up[(0,) * (len(up.shape) - 2) + (slice(None), slice(start, start + width))]
            down_ref[s] = down[(0,) * (len(down.shape) - 2) + (slice(start, start + width),)]

    for s, ref in enumerate((h_a, h_b)):
        @pl.when(source == s)
        def _():
            h_ref[...] = ref[(0,) * (len(ref.shape) - 2)]

    grad = grad_ref[0]
    x = x_ref[0, 0]
    for low in range(0, width, 256):
        cols = slice(low, min(low + 256, width))
        pre_ref[:, cols], act_ref[:, cols] = unit_grads(grad, h_ref[:, cols], down_ref[source, cols, :])
    pre, act = pre_ref[...], act_ref[...]
    dw_ref[source, 0] += dot(pre, x, 0, 0)
    dw_ref[source, 1] += dot(act, grad, 0, 0)
    part = dot(pre, up_ref[source], 1, 1)

    @pl.when(source == 0)
    def _():
        sum_ref[...] = part + carry_ref[0] if has_carry else part

    @pl.when(source == 1)
    def _():
        total = sum_ref[...] + part
        out_ref[0] = (grad.astype(F32) + total).astype(BF16) if final else total

    copies = [pltpu.make_async_copy(dw_ref.at[s], dw, sem.at[s]) for s, dw in enumerate((dw_a, dw_b))]
    for s in range(2):
        @pl.when((row == rows - 1) & (source == s))
        def _():
            copies[s].start()

    @pl.when((row == rows - 1) & (source == 1))
    def _():
        copies[0].wait()
        copies[1].wait()


def block_call(quarter, layer, grad, x_saved, h_pair, ups, downs, start, width, carry, final):
    rows, seq, hidden = grad.shape

    def h_spec(h):
        if h.ndim == 4:
            return pl.BlockSpec((1, 1, seq, width), lambda b, s, ids: (layer, b, ids[0], 0))
        return pl.BlockSpec((1, seq, width), lambda b, s, ids: (b, 0, 0))

    def w_spec(w):
        shape = (1,) * (w.ndim - 2) + w.shape[-2:]
        return pl.BlockSpec(shape, lambda b, s, ids: (layer,) * (w.ndim - 2) + (0, 0), pipeline_mode=pl.Buffered(1))

    row_spec = pl.BlockSpec((1, seq, hidden), lambda b, s, ids: (b, 0, 0))
    any_spec = pl.BlockSpec(memory_space=pl.ANY)
    in_specs = [row_spec, pl.BlockSpec((1, 1, seq, hidden), lambda b, s, ids: (layer, b, 0, 0))]
    in_specs += [h_spec(h) for h in h_pair]
    in_specs += [w_spec(w) for w in (*ups, *downs)]
    operands = [grad, x_saved, *h_pair, *ups, *downs]
    if carry is not None:
        in_specs.append(row_spec)
        operands.append(carry)
    dw_shape = (2, width, hidden)
    return pl.pallas_call(
        functools.partial(block_body, carry is not None, final, rows, start),
        out_shape=[jax.ShapeDtypeStruct(grad.shape, BF16 if final else F32)] + [jax.ShapeDtypeStruct(dw_shape, F32)] * 2,
        grid_spec=pltpu.PrefetchScalarGridSpec(
            num_scalar_prefetch=1,
            grid=(rows, 2),
            in_specs=in_specs,
            out_specs=[row_spec, any_spec, any_spec],
            scratch_shapes=[pltpu.VMEM((seq, width), BF16)] * 3
            + [pltpu.VMEM((seq, hidden), F32), pltpu.VMEM((2,) + dw_shape, F32)]
            + [pltpu.VMEM((2, hidden, width), BF16), pltpu.VMEM((2, width, hidden), BF16), pltpu.SemaphoreType.DMA((2,))],
        ),
        compiler_params=pltpu.CompilerParams(dimension_semantics=("arbitrary", "arbitrary"), vmem_limit_bytes=ALL_VMEM),
        cost_estimate=pl.CostEstimate(
            flops=16 * rows * seq * hidden * width, bytes_accessed=8 * rows * seq * hidden, transcendentals=2 * rows * seq * width),
    )(quarter, *operands)


def swap_lanes(a, b):
    left = lax.broadcasted_iota(jnp.int32, a.shape, 1) < SMALL
    return jnp.where(left, a, pltpu.roll(b, SMALL, 1)), jnp.where(left, pltpu.roll(a, SMALL, 1), b)


def pack_body(_, lo_ref, hi_ref, left_ref, *right_refs):
    left, right = swap_lanes(lo_ref[0, 0].astype(F32), hi_ref[0, 0].astype(F32))
    left_ref[0] = left.astype(BF16)
    for j, ref in enumerate(right_refs):
        low = sum(CHUNKS[:j])

        @pl.when((pl.program_id(0) >= low) & (pl.program_id(0) < low + CHUNKS[j]))
        def _():
            ref[0] = right.astype(BF16)


def pack_call(target, h_saved, layer, start, seq):
    pairs = h_saved.shape[1] // 2
    specs = [pl.BlockSpec((1, 1, seq, LANES), lambda b, ids, r=r: (layer, b + r * pairs, ids[0], start // LANES)) for r in range(2)]
    block = (1, seq, LANES)
    chunk_specs = [
        pl.BlockSpec(block, lambda b, ids, low=sum(CHUNKS[:j]), n=n: (jnp.clip(b - low, 0, n - 1), 0, 0)) for j, n in enumerate(CHUNKS)]
    return pl.pallas_call(
        pack_body,
        out_shape=[jax.ShapeDtypeStruct((n, seq, LANES), BF16) for n in (pairs, *CHUNKS)],
        grid_spec=pltpu.PrefetchScalarGridSpec(
            num_scalar_prefetch=1,
            grid=(pairs,),
            in_specs=specs,
            out_specs=[pl.BlockSpec(block, lambda b, ids: (b, 0, 0)), *chunk_specs],
        ),
        compiler_params=pltpu.CompilerParams(dimension_semantics=("arbitrary",), vmem_limit_bytes=ALL_VMEM),
        cost_estimate=pl.CostEstimate(flops=pairs * seq * LANES, bytes_accessed=8 * pairs * seq * LANES, transcendentals=0),
    )(target, h_saved, h_saved)


def wide_body(start, grad_ref, x_ref, h_a, h_b, up_a, up_b, down_a, down_b, carry_ref, out_ref, dw_a, dw_b):
    @pl.when(pl.program_id(0) == 0)
    def _():
        dw_a[...] = jnp.zeros_like(dw_a)
        dw_b[...] = jnp.zeros_like(dw_b)

    grad, x = grad_ref[0], x_ref[0, 0]
    cols = slice(start, start + h_a.shape[2])
    total = grad.astype(F32) + carry_ref[0]
    for h, up, down, dw in ((h_a, up_a, down_a, dw_a), (h_b, up_b, down_b, dw_b)):
        pre, act = unit_grads(grad, h[0], down[cols, :])
        dw[0] += dot(pre, x, 0, 0)
        dw[1] += dot(act, grad, 0, 0)
        total += dot(pre, up[:, cols], 1, 1)
    out_ref[0] = total


def wide_call(layer, grad, x_saved, h_pair, ups, downs, start, carry):
    rows, seq, hidden = grad.shape
    width = h_pair[0].shape[2]
    row_spec = pl.BlockSpec((1, seq, hidden), lambda b: (b, 0, 0))
    h_spec = pl.BlockSpec((1, seq, width), lambda b: (b, 0, 0))
    w_spec = pl.BlockSpec(ups[0].shape, lambda b: (0, 0), pipeline_mode=pl.Buffered(1))
    dw_shape = (2, width, hidden)
    return pl.pallas_call(
        functools.partial(wide_body, start),
        out_shape=[jax.ShapeDtypeStruct(grad.shape, F32)] + [jax.ShapeDtypeStruct(dw_shape, F32)] * 2,
        grid=(rows,),
        in_specs=[row_spec, pl.BlockSpec((1, 1, seq, hidden), lambda b: (layer, b, 0, 0)), h_spec, h_spec]
        + [w_spec] * 4 + [row_spec],
        out_specs=[row_spec] + [pl.BlockSpec(dw_shape, lambda b: (0, 0, 0), pipeline_mode=pl.Buffered(1))] * 2,
        compiler_params=pltpu.CompilerParams(dimension_semantics=("arbitrary",), vmem_limit_bytes=ALL_VMEM),
        cost_estimate=pl.CostEstimate(
            flops=16 * rows * seq * hidden * width, bytes_accessed=12 * rows * seq * hidden, transcendentals=2 * rows * seq * width),
    )(grad, x_saved, *h_pair, *ups, *downs, carry)


def small_body(has_init, finish, grad_ref, x_ref, h_a, h_b, down_a, down_b, *refs):
    refs = list(refs)
    carry_ref, early_ref, up_ref = (refs.pop(0) for _ in range(3)) if finish else (None,) * 3
    dw_pair, out_ref = refs[-3:-1], refs[-1]
    seq, hidden = grad_ref.shape[2:]

    @pl.when(pl.program_id(0) == 0)
    def _():
        for i, dw in enumerate(dw_pair):
            dw[...] = refs[i][...] if has_init else jnp.zeros_like(dw)

    h = jnp.concatenate(swap_lanes(h_a[0].astype(F32), h_b[0].astype(F32)))
    grad, x = grad_ref[...].reshape(2 * seq, hidden), x_ref[...].reshape(2 * seq, hidden)
    pre, act = unit_grads(grad, h, jnp.concatenate([down_a[...], down_b[...]]))
    for kind, part in enumerate((dot(pre, x, 0, 0), dot(act, grad, 0, 0))):
        dw_pair[0][kind] += part[:SMALL]
        dw_pair[1][kind] += part[SMALL:]
    for r in range(2):
        row = pre[r * seq : (r + 1) * seq]
        if finish:
            total = carry_ref[r, 0] + dot(jnp.concatenate([early_ref[r, 0], row], axis=1), up_ref[...], 1, 1)
            out_ref[r, 0] = total.astype(BF16)
        else:
            out_ref[r, 0] = row


def paired(value, axis=0):
    shape = value.shape
    return value.reshape(shape[:axis] + (2, shape[axis] // 2) + shape[axis + 1 :])


def small_call(layer, grad, x_saved, h_pair, down_pair, start, first_pair, init=None, finish=None, pre=None, pre_pairs=None, pre_first=0):
    _, _, seq, hidden = grad.shape
    pairs = h_pair[0].shape[0]
    row_spec = pl.BlockSpec((2, 1, seq, hidden), lambda b: (0, b + first_pair, 0, 0))
    early_spec = pl.BlockSpec((2, 1, seq, LANES), lambda b: (0, b + first_pair, 0, 0))
    pre_spec = pl.BlockSpec((2, 1, seq, LANES), lambda b: (0, b + pre_first, 0, 0))
    h_spec = pl.BlockSpec((1, seq, LANES), lambda b: (b, 0, 0))
    down_spec = pl.BlockSpec((SMALL, hidden), lambda b: (start // SMALL, 0))
    dw_shape = (2, SMALL, hidden)
    dw_spec = pl.BlockSpec(dw_shape, lambda b: (0, 0, 0))
    in_specs = [row_spec, pl.BlockSpec((1, 2, 1, seq, hidden), lambda b: (layer, 0, b + first_pair, 0, 0)), h_spec, h_spec, down_spec, down_spec]
    if finish:
        in_specs += [row_spec, early_spec, pl.BlockSpec(finish[2].shape, lambda b: (0, 0))]
    if init:
        in_specs += [dw_spec] * 2
    if pre is not None:
        in_specs.append(pl.BlockSpec(memory_space=pl.ANY))
    return pl.pallas_call(
        functools.partial(small_body, init is not None, finish is not None),
        out_shape=[jax.ShapeDtypeStruct(dw_shape, F32)] * 2
        + [jax.ShapeDtypeStruct(grad.shape if finish else (2, pre_pairs or pairs, seq, LANES), BF16)],
        grid=(pairs,),
        in_specs=in_specs,
        out_specs=[dw_spec, dw_spec, row_spec if finish else pre_spec],
        input_output_aliases={} if pre is None else {len(in_specs) - 1: 2},
        compiler_params=pltpu.CompilerParams(dimension_semantics=("arbitrary",), vmem_limit_bytes=ALL_VMEM),
        cost_estimate=pl.CostEstimate(
            flops=24 * pairs * seq * hidden * SMALL, bytes_accessed=8 * pairs * seq * hidden, transcendentals=4 * pairs * seq * SMALL),
    )(grad, x_saved, *h_pair, *down_pair, *(finish or ()), *(init or ()), *(() if pre is None else (pre,)))


def join_body(up_a, up_b, out_ref):
    first, second = swap_lanes(up_a[...].astype(F32), up_b[...].astype(F32))
    out_ref[:, :LANES], out_ref[:, LANES:] = first.astype(BF16), second.astype(BF16)


def join_call(up_pair, start):
    hidden = up_pair[0].shape[0]
    up_spec = pl.BlockSpec((hidden, LANES), lambda i: (0, start // LANES))
    return pl.pallas_call(
        join_body,
        out_shape=jax.ShapeDtypeStruct((hidden, 2 * LANES), BF16),
        grid=(1,),
        in_specs=[up_spec, up_spec],
        out_specs=pl.BlockSpec((hidden, 2 * LANES), lambda i: (0, 0)),
        compiler_params=pltpu.CompilerParams(dimension_semantics=("arbitrary",), vmem_limit_bytes=ALL_VMEM),
        cost_estimate=pl.CostEstimate(flops=hidden * LANES, bytes_accessed=8 * hidden * LANES, transcendentals=0),
    )(*up_pair)


def finish_body(carry_ref, pre_a, pre_b, up_ref, _, out_ref):
    total = carry_ref[0, 0] + dot(jnp.concatenate([pre_a[0, 0], pre_b[0, 0]], axis=1), up_ref[...], 1, 1)
    out_ref[0, 0] = total.astype(BF16)


def finish_call(carry, pre_pair, ups, first_pair, first_half, halves, out):
    _, _, seq, hidden = carry.shape
    count = pre_pair[1].shape[1]
    row_spec = pl.BlockSpec((1, 1, seq, hidden), lambda r, b: (r + first_half, b + first_pair, 0, 0))
    pre_specs = [pl.BlockSpec((1, 1, seq, LANES), lambda r, b, first=first: (r + first_half, b + first, 0, 0)) for first in (first_pair, 0)]
    rows = halves * count
    return pl.pallas_call(
        finish_body,
        out_shape=jax.ShapeDtypeStruct(carry.shape, BF16),
        grid=(halves, count),
        in_specs=[row_spec, *pre_specs, pl.BlockSpec(ups.shape, lambda r, b: (0, 0)), pl.BlockSpec(memory_space=pl.ANY)],
        out_specs=row_spec,
        input_output_aliases={4: 0},
        compiler_params=pltpu.CompilerParams(dimension_semantics=("arbitrary", "arbitrary"), vmem_limit_bytes=ALL_VMEM),
        cost_estimate=pl.CostEstimate(flops=4 * rows * seq * hidden * LANES, bytes_accessed=7 * rows * seq * hidden, transcendentals=0),
    )(carry, *pre_pair, ups, out)


def pair_body(first_ref, mine_ref, theirs_ref, stay_ref, away_ref):
    first = first_ref[0] == 1
    up, down = mine_ref[0] + theirs_ref[0], mine_ref[1] + theirs_ref[1]
    stay_ref[...] = jnp.where(first, up, down)
    away_ref[...] = jnp.where(first, down, up)


def pair_call(first, mine, theirs):
    _, size, hidden = mine.shape
    step = min(size, LANES)
    both_spec = pl.BlockSpec((2, step, hidden), lambda i, first: (0, i, 0))
    one_spec = pl.BlockSpec((step, hidden), lambda i, first: (i, 0))
    return pl.pallas_call(
        pair_body,
        out_shape=[jax.ShapeDtypeStruct((size, hidden), F32)] * 2,
        grid_spec=pltpu.PrefetchScalarGridSpec(
            num_scalar_prefetch=1, grid=(size // step,), in_specs=[both_spec] * 2, out_specs=[one_spec] * 2),
        compiler_params=pltpu.CompilerParams(dimension_semantics=("arbitrary",), vmem_limit_bytes=ALL_VMEM),
        cost_estimate=pl.CostEstimate(flops=4 * mine.size, bytes_accessed=12 * mine.size, transcendentals=0),
    )(first, mine, theirs)


def place_body(first_ref, kept_ref, other_ref, *refs):
    up_ref, down_ref = refs[-2:]
    first = first_ref[0] == 1
    kept, other = kept_ref[...], other_ref[...]
    up_ref[0] = jnp.where(first, kept, other).T
    down_ref[0] = jnp.where(first, other, kept)


def place_call(first, kept, other, layer, start, layers, width, bufs):
    size, hidden = kept.shape
    row_spec = pl.BlockSpec((LANES, hidden), lambda i, first: (i, 0))
    out_shape = [jax.ShapeDtypeStruct((layers, hidden, width), F32), jax.ShapeDtypeStruct((layers, width, hidden), F32)]
    any_spec = pl.BlockSpec(memory_space=pl.ANY)
    return pl.pallas_call(
        place_body,
        out_shape=out_shape,
        grid_spec=pltpu.PrefetchScalarGridSpec(
            num_scalar_prefetch=1,
            grid=(size // LANES,),
            in_specs=[row_spec, row_spec] + ([any_spec, any_spec] if bufs is not None else []),
            out_specs=[
                pl.BlockSpec((1, hidden, LANES), lambda i, first: (layer, 0, start // LANES + i)),
                pl.BlockSpec((1, LANES, hidden), lambda i, first: (layer, start // LANES + i, 0)),
            ],
        ),
        input_output_aliases={3: 0, 4: 1} if bufs is not None else {},
        compiler_params=pltpu.CompilerParams(dimension_semantics=("arbitrary",), vmem_limit_bytes=ALL_VMEM),
        cost_estimate=pl.CostEstimate(flops=4 * size * hidden, bytes_accessed=16 * size * hidden, transcendentals=0),
    )(first, kept, other, *(bufs or ()))


def join_place_body(count, layer, start, first_ref, *refs):
    up_out, down_out, up_ref, down_ref, sem = refs[-5:]
    first = first_ref[0] == 1
    kept = jnp.concatenate([r[...] for r in refs[:count]])
    other = jnp.concatenate([r[...] for r in refs[count : 2 * count]])
    size = kept.shape[0]
    down_ref[...] = jnp.where(first, other, kept)
    down_copy = pltpu.make_async_copy(down_ref, down_out.at[layer, pl.ds(start, size), :], sem.at[0])
    down_copy.start()
    up_ref[...] = jnp.where(first, kept, other).T
    up_copy = pltpu.make_async_copy(up_ref, up_out.at[layer, :, pl.ds(start, size)], sem.at[1])
    up_copy.start()
    down_copy.wait()
    up_copy.wait()


def join_place_call(first, pieces, layer, start, bufs):
    hidden = pieces[0][0].shape[1]
    size = sum(n for _, _, _, n in pieces)
    piece_specs = [pl.BlockSpec((n, hidden), lambda i, first, block=low // n: (block, 0)) for _, _, low, n in pieces]
    any_spec = pl.BlockSpec(memory_space=pl.ANY)
    count = len(pieces)
    return pl.pallas_call(
        functools.partial(join_place_body, count, layer, start),
        out_shape=[jax.ShapeDtypeStruct(b.shape, b.dtype) for b in bufs],
        grid_spec=pltpu.PrefetchScalarGridSpec(
            num_scalar_prefetch=1,
            grid=(1,),
            in_specs=piece_specs * 2 + [any_spec] * 2,
            out_specs=[any_spec] * 2,
            scratch_shapes=[pltpu.VMEM((hidden, size), F32), pltpu.VMEM((size, hidden), F32), pltpu.SemaphoreType.DMA((2,))],
        ),
        input_output_aliases={1 + 2 * count: 0, 2 + 2 * count: 1},
        compiler_params=pltpu.CompilerParams(dimension_semantics=("arbitrary",), vmem_limit_bytes=ALL_VMEM),
        cost_estimate=pl.CostEstimate(flops=4 * size * hidden, bytes_accessed=16 * size * hidden, transcendentals=0),
    )(first, *[p[0] for p in pieces], *[p[1] for p in pieces], *bufs)


def solution(mesh):
    n_model = mesh.shape["model"]

    def to_model(value, flip):
        return lax.ppermute(value, "model", [(i, i ^ flip) for i in range(n_model)])

    def to_data(value):
        return lax.ppermute(value, "data", [(0, 1), (1, 0)])

    def all_blocks(x_saved, h_saved, w_up, w_down, grad_out):
        me = lax.axis_index("model")
        first = lax.axis_index("data") == 0
        first_flag = jnp.reshape(first, (1,)).astype(jnp.int32)
        quarter = jnp.reshape(me, (1,)).astype(jnp.int32)
        layers = w_up.shape[0]
        rows, seq = grad_out.shape[:2]
        width = h_saved.shape[-1]

        held = [h_saved, None]

        def h_from(layer, flip, start=0, size=width):
            held[0], held[1] = lax.optimization_barrier((held[0], held[1]))
            begin = (me ^ flip) * seq
            held[1] = lax.dynamic_slice(held[0], (layer, 0, begin, start), (1, rows, seq, size))[0]
            return to_model(held[1], flip)

        head = jnp.where(first, w_up[1, :FIRST], w_down[1, :FIRST])
        w_pair = lax.optimization_barrier((w_up, w_down, head))
        held[1] = jnp.where(first, w_pair[0][1, FIRST:], w_pair[1][1, FIRST:])
        far_w = [None, jnp.concatenate([to_model(head, 2), to_model(held[1], 2)])]
        h_one = [h_from(1, 2), h_from(1, 3)]
        h_near = [None, h_from(1, 1)]
        w_pair = lax.optimization_barrier((w_up, w_down, held[1]))
        far_w[0] = jnp.where(first, w_pair[0][0], w_pair[1][0])
        far_w[0] = to_model(far_w[0], 2)
        h_near[0] = h_from(0, 1)
        h_zero = []
        for j, size in enumerate(BLOCKS):
            start = sum(BLOCKS[:j])
            h_zero.append([h_from(0, 2, start, size), h_from(0, 3, start, size)])
        small_start = width - LANES
        packed = []
        for flip in (2, 3):
            packed.append(pack_call(jnp.reshape(me ^ flip, (1,)).astype(jnp.int32), h_saved, 0, small_start, seq))
        h_small = [[to_model(packed[0][j], 2), to_model(packed[1][j], 3)] for j in range(4)]

        up, down = [{0: w_up} for _ in range(layers)], [{0: w_down} for _ in range(layers)]
        near_up, near_down = to_model(w_up, 1), to_model(w_down, 1)
        for layer in range(layers):
            other = to_data(far_w[layer])
            up[layer][1], down[layer][1] = near_up, near_down
            up[layer][2], down[layer][2] = jnp.where(first, far_w[layer], other), jnp.where(first, other, far_w[layer])
            up[layer][3] = to_model(up[layer][2], 1)
            down[layer][3] = to_model(down[layer][2], 1)

        def call(layer, grad, hs, flips, carry, final, start=0, size=width):
            ups, downs = [up[layer][f] for f in flips], [down[layer][f] for f in flips]
            return block_call(quarter, layer, grad, x_saved, hs, ups, downs, start, size, carry, final)

        def partial_sum(keep, give):
            theirs = to_model(give, 1)
            stay, away = pair_call(first_flag, keep, theirs)
            return stay + to_data(away)

        def place(pieces, layer, start, bufs):
            if len(pieces) > 1:
                return join_place_call(first_flag, pieces, layer, start, bufs)
            return place_call(first_flag, *pieces[0], layer, start, layers, width, bufs)

        carry, dw_0, dw_1 = call(1, grad_out, [h_saved, h_near[1]], (0, 1), None, False)
        near = partial_sum(dw_0, dw_1)
        grad_mid, dw_2, dw_3 = call(1, grad_out, h_one, (2, 3), carry, True)
        far = partial_sum(dw_2, dw_3)
        near, part = lax.optimization_barrier(near), to_model(far, 2)
        kept = near + part
        bufs = place([(kept, to_data(kept))], 1, 0, None)

        carry, dw_0, dw_1 = call(0, grad_mid, [h_saved, h_near[0]], (0, 1), None, False)
        near = partial_sum(dw_0, dw_1)
        bounds = [0, 384, 448, 576, width - SMALL, width]
        near_part = lax.optimization_barrier(tuple(near[a:b] for a, b in zip(bounds, bounds[1:])))
        pieces = []

        def exchange(unit, far):
            part = to_model(far, 2)
            kept = near_part[unit] + part
            pieces.append((kept, to_data(kept)))

        down_pair, up_pair = [down[0][f] for f in (2, 3)], [up[0][f] for f in (2, 3)]
        small_up = join_call(up_pair, small_start)
        carry, dw_2, dw_3 = call(0, grad_mid, h_zero[0], (2, 3), carry, False, 0, BLOCKS[0])
        exchange(0, partial_sum(dw_2, dw_3))
        carry, dw_2, dw_3 = wide_call(0, grad_mid, x_saved, h_zero[1], up_pair, down_pair, BLOCKS[0], carry)
        far = partial_sum(dw_2, dw_3)
        exchange(1, far[: bounds[2] - bounds[1]])
        exchange(2, far[bounds[2] - bounds[1] : bounds[3] - bounds[1]])
        carry, grad_mid, x_saved = paired(carry), paired(grad_mid), paired(x_saved, 1)
        dw_2, dw_3, pre_1 = small_call(0, grad_mid, x_saved, h_small[0], down_pair, small_start, 0)
        exchange(3, jnp.concatenate([far[bounds[3] - bounds[1] :], partial_sum(dw_2, dw_3)]))
        last = small_start + SMALL
        early, late = CHUNKS[0], CHUNKS[1] + CHUNKS[2]
        dw_2, dw_3, grad_x = small_call(
            0, grad_mid, x_saved, h_small[1], down_pair, last, 0, finish=(carry, pre_1, small_up))
        dw_2, dw_3, pre_2 = small_call(
            0, grad_mid, x_saved, h_small[2], down_pair, last, early, init=(dw_2, dw_3), pre_pairs=late)
        dw_2, dw_3, pre_2 = small_call(
            0, grad_mid, x_saved, h_small[3], down_pair, last, early + CHUNKS[1], init=(dw_2, dw_3),
            pre=pre_2, pre_pairs=late, pre_first=CHUNKS[1])
        exchange(4, partial_sum(dw_2, dw_3))
        grad_x = finish_call(carry, (pre_1, pre_2), small_up, early, 0, 2, grad_x)
        bufs = place([pieces[0]], 0, 0, bufs)
        middle = [(*pieces[1], 0, 64), (*pieces[2], 0, 128), (*pieces[3], 0, 64)]
        bufs = place(middle, 0, bounds[1], bufs)
        bufs = place([(*pieces[3], 64, 64), (*pieces[4], 0, 64)], 0, small_start, bufs)
        grad_x = grad_x.reshape(grad_out.shape)
        return grad_x, bufs[0], bufs[1]

    return jax.shard_map(
        all_blocks,
        mesh=mesh,
        in_specs=(P(None, "data", "model", None), P(None, "data", None, "model"), P(None, None, "model"), P(None, "model", None), P("data", "model", None)),
        out_specs=(P("data", "model", None), P(None, None, "model"), P(None, "model", None)),
        check_vma=False,
    )
```

```python
import functools

import jax
import jax.numpy as jnp
from jax import lax
from jax.experimental import pallas as pl
from jax.experimental.pallas import tpu as pltpu
from jax.sharding import PartitionSpec as P


BF16 = jnp.bfloat16
F32 = jnp.float32
BLOCKS = (384, 256)
LANES = 128
SMALL = 64
CHUNKS = (5, 3)
FIRST = 192
ALL_VMEM = 66_000_000


def gelu_parts(pre_act):
    root = 0.7978845608028654
    cubic = (0.134145 * pre_act) * pre_act
    gate = 0.5 + 0.5 * jnp.tanh(pre_act * (root + (root / 3) * cubic))
    gelu_out = pre_act * gate
    gelu_slope = gate + gelu_out * (1.0 - gate) * (2 * root + (2 * root) * cubic)
    return gelu_out, gelu_slope


def dot(lhs, rhs, lhs_dim, rhs_dim):
    return lax.dot_general(lhs, rhs, (((lhs_dim,), (rhs_dim,)), ((), ())), preferred_element_type=F32)


def unit_grads(grad, h, down):
    d_act = dot(grad, down, 1, 1)
    gelu_out, gelu_slope = gelu_parts(h.astype(F32))
    return (d_act * gelu_slope).astype(BF16), gelu_out.astype(BF16)


def block_body(has_carry, final, rows, start, _, *refs):
    refs = list(refs)
    grad_ref, x_ref, h_a, h_b, up_a, up_b, down_a, down_b = (refs.pop(0) for _ in range(8))
    carry_ref = refs.pop(0) if has_carry else None
    out_ref, dw_a, dw_b, h_ref, pre_ref, act_ref, sum_ref, dw_ref, up_ref, down_ref, sem = refs
    row, source = pl.program_id(0), pl.program_id(1)
    width = pre_ref.shape[1]

    @pl.when((row == 0) & (source == 0))
    def _():
        dw_ref[...] = jnp.zeros_like(dw_ref)
        for s, (up, down) in enumerate(((up_a, down_a), (up_b, down_b))):
            up_ref[s] = up[(0,) * (len(up.shape) - 2) + (slice(None), slice(start, start + width))]
            down_ref[s] = down[(0,) * (len(down.shape) - 2) + (slice(start, start + width),)]

    for s, ref in enumerate((h_a, h_b)):
        @pl.when(source == s)
        def _():
            h_ref[...] = ref[(0,) * (len(ref.shape) - 2)]

    grad = grad_ref[0]
    x = x_ref[0, 0]
    for low in range(0, width, 256):
        cols = slice(low, min(low + 256, width))
        pre_ref[:, cols], act_ref[:, cols] = unit_grads(grad, h_ref[:, cols], down_ref[source, cols, :])
    pre, act = pre_ref[...], act_ref[...]
    dw_ref[source, 0] += dot(pre, x, 0, 0)
    dw_ref[source, 1] += dot(act, grad, 0, 0)
    part = dot(pre, up_ref[source], 1, 1)

    @pl.when(source == 0)
    def _():
        sum_ref[...] = part + carry_ref[0] if has_carry else part

    @pl.when(source == 1)
    def _():
        total = sum_ref[...] + part
        out_ref[0] = (grad.astype(F32) + total).astype(BF16) if final else total

    copies = [pltpu.make_async_copy(dw_ref.at[s], dw, sem.at[s]) for s, dw in enumerate((dw_a, dw_b))]
    for s in range(2):
        @pl.when((row == rows - 1) & (source == s))
        def _():
            copies[s].start()

    @pl.when((row == rows - 1) & (source == 1))
    def _():
        copies[0].wait()
        copies[1].wait()


def block_call(quarter, layer, grad, x_saved, h_pair, ups, downs, start, width, carry, final):
    rows, seq, hidden = grad.shape

    def h_spec(h):
        if h.ndim == 4:
            return pl.BlockSpec((1, 1, seq, width), lambda b, s, ids: (layer, b, ids[0], 0))
        return pl.BlockSpec((1, seq, width), lambda b, s, ids: (b, 0, 0))

    def w_spec(w):
        shape = (1,) * (w.ndim - 2) + w.shape[-2:]
        return pl.BlockSpec(shape, lambda b, s, ids: (layer,) * (w.ndim - 2) + (0, 0), pipeline_mode=pl.Buffered(1))

    row_spec = pl.BlockSpec((1, seq, hidden), lambda b, s, ids: (b, 0, 0))
    any_spec = pl.BlockSpec(memory_space=pl.ANY)
    in_specs = [row_spec, pl.BlockSpec((1, 1, seq, hidden), lambda b, s, ids: (layer, b, 0, 0))]
    in_specs += [h_spec(h) for h in h_pair]
    in_specs += [w_spec(w) for w in (*ups, *downs)]
    operands = [grad, x_saved, *h_pair, *ups, *downs]
    if carry is not None:
        in_specs.append(row_spec)
        operands.append(carry)
    dw_shape = (2, width, hidden)
    return pl.pallas_call(
        functools.partial(block_body, carry is not None, final, rows, start),
        out_shape=[jax.ShapeDtypeStruct(grad.shape, BF16 if final else F32)] + [jax.ShapeDtypeStruct(dw_shape, F32)] * 2,
        grid_spec=pltpu.PrefetchScalarGridSpec(
            num_scalar_prefetch=1,
            grid=(rows, 2),
            in_specs=in_specs,
            out_specs=[row_spec, any_spec, any_spec],
            scratch_shapes=[pltpu.VMEM((seq, width), BF16)] * 3
            + [pltpu.VMEM((seq, hidden), F32), pltpu.VMEM((2,) + dw_shape, F32)]
            + [pltpu.VMEM((2, hidden, width), BF16), pltpu.VMEM((2, width, hidden), BF16), pltpu.SemaphoreType.DMA((2,))],
        ),
        compiler_params=pltpu.CompilerParams(dimension_semantics=("arbitrary", "arbitrary"), vmem_limit_bytes=ALL_VMEM),
        cost_estimate=pl.CostEstimate(
            flops=16 * rows * seq * hidden * width, bytes_accessed=8 * rows * seq * hidden, transcendentals=2 * rows * seq * width),
    )(quarter, *operands)


def swap_lanes(a, b):
    left = lax.broadcasted_iota(jnp.int32, a.shape, 1) < SMALL
    return jnp.where(left, a, pltpu.roll(b, SMALL, 1)), jnp.where(left, pltpu.roll(a, SMALL, 1), b)


def pack_body(_, lo_ref, hi_ref, left_ref, *right_refs):
    left, right = swap_lanes(lo_ref[0, 0].astype(F32), hi_ref[0, 0].astype(F32))
    left_ref[0] = left.astype(BF16)
    for j, ref in enumerate(right_refs):
        low = sum(CHUNKS[:j])

        @pl.when((pl.program_id(0) >= low) & (pl.program_id(0) < low + CHUNKS[j]))
        def _():
            ref[0] = right.astype(BF16)


def pack_call(target, h_saved, layer, start, seq):
    pairs = h_saved.shape[1] // 2
    specs = [pl.BlockSpec((1, 1, seq, LANES), lambda b, ids, r=r: (layer, b + r * pairs, ids[0], start // LANES)) for r in range(2)]
    block = (1, seq, LANES)
    chunk_specs = [
        pl.BlockSpec(block, lambda b, ids, low=sum(CHUNKS[:j]), n=n: (jnp.clip(b - low, 0, n - 1), 0, 0)) for j, n in enumerate(CHUNKS)]
    return pl.pallas_call(
        pack_body,
        out_shape=[jax.ShapeDtypeStruct((n, seq, LANES), BF16) for n in (pairs, *CHUNKS)],
        grid_spec=pltpu.PrefetchScalarGridSpec(
            num_scalar_prefetch=1,
            grid=(pairs,),
            in_specs=specs,
            out_specs=[pl.BlockSpec(block, lambda b, ids: (b, 0, 0)), *chunk_specs],
        ),
        compiler_params=pltpu.CompilerParams(dimension_semantics=("arbitrary",), vmem_limit_bytes=ALL_VMEM),
        cost_estimate=pl.CostEstimate(flops=pairs * seq * LANES, bytes_accessed=8 * pairs * seq * LANES, transcendentals=0),
    )(target, h_saved, h_saved)


def wide_body(start, grad_ref, x_ref, h_a, h_b, up_a, up_b, down_a, down_b, carry_ref, out_ref, dw_a, dw_b):
    @pl.when(pl.program_id(0) == 0)
    def _():
        dw_a[...] = jnp.zeros_like(dw_a)
        dw_b[...] = jnp.zeros_like(dw_b)

    grad, x = grad_ref[0], x_ref[0, 0]
    cols = slice(start, start + h_a.shape[2])
    total = grad.astype(F32) + carry_ref[0]
    for h, up, down, dw in ((h_a, up_a, down_a, dw_a), (h_b, up_b, down_b, dw_b)):
        pre, act = unit_grads(grad, h[0], down[cols, :])
        dw[0] += dot(pre, x, 0, 0)
        dw[1] += dot(act, grad, 0, 0)
        total += dot(pre, up[:, cols], 1, 1)
    out_ref[0] = total


def wide_call(layer, grad, x_saved, h_pair, ups, downs, start, carry):
    rows, seq, hidden = grad.shape
    width = h_pair[0].shape[2]
    row_spec = pl.BlockSpec((1, seq, hidden), lambda b: (b, 0, 0))
    h_spec = pl.BlockSpec((1, seq, width), lambda b: (b, 0, 0))
    w_spec = pl.BlockSpec(ups[0].shape, lambda b: (0, 0), pipeline_mode=pl.Buffered(1))
    dw_shape = (2, width, hidden)
    return pl.pallas_call(
        functools.partial(wide_body, start),
        out_shape=[jax.ShapeDtypeStruct(grad.shape, F32)] + [jax.ShapeDtypeStruct(dw_shape, F32)] * 2,
        grid=(rows,),
        in_specs=[row_spec, pl.BlockSpec((1, 1, seq, hidden), lambda b: (layer, b, 0, 0)), h_spec, h_spec]
        + [w_spec] * 4 + [row_spec],
        out_specs=[row_spec] + [pl.BlockSpec(dw_shape, lambda b: (0, 0, 0), pipeline_mode=pl.Buffered(1))] * 2,
        compiler_params=pltpu.CompilerParams(dimension_semantics=("arbitrary",), vmem_limit_bytes=ALL_VMEM),
        cost_estimate=pl.CostEstimate(
            flops=16 * rows * seq * hidden * width, bytes_accessed=12 * rows * seq * hidden, transcendentals=2 * rows * seq * width),
    )(grad, x_saved, *h_pair, *ups, *downs, carry)


def small_body(has_init, finish, grad_ref, x_ref, h_a, h_b, down_a, down_b, *refs):
    refs = list(refs)
    carry_ref, early_ref, up_ref = (refs.pop(0) for _ in range(3)) if finish else (None,) * 3
    dw_pair, out_ref = refs[-3:-1], refs[-1]

    @pl.when(pl.program_id(0) == 0)
    def _():
        for i, dw in enumerate(dw_pair):
            dw[...] = refs[i][...] if has_init else jnp.zeros_like(dw)

    h_pair = swap_lanes(h_a[0].astype(F32), h_b[0].astype(F32))
    down = jnp.concatenate([down_a[...], down_b[...]])
    for r, h in enumerate(h_pair):
        grad, x = grad_ref[r, 0], x_ref[0, r, 0]
        pre, act = unit_grads(grad, h, down)
        for kind, part in enumerate((dot(pre, x, 0, 0), dot(act, grad, 0, 0))):
            dw_pair[0][kind] += part[:SMALL]
            dw_pair[1][kind] += part[SMALL:]
        if finish:
            total = carry_ref[r, 0] + dot(jnp.concatenate([early_ref[r, 0], pre], axis=1), up_ref[...], 1, 1)
            out_ref[r, 0] = total.astype(BF16)
        else:
            out_ref[r, 0] = pre


def paired(value, axis=0):
    shape = value.shape
    return value.reshape(shape[:axis] + (2, shape[axis] // 2) + shape[axis + 1 :])


def small_call(layer, grad, x_saved, h_pair, down_pair, start, first_pair, init=None, finish=None):
    _, _, seq, hidden = grad.shape
    pairs = h_pair[0].shape[0]
    row_spec = pl.BlockSpec((2, 1, seq, hidden), lambda b: (0, b + first_pair, 0, 0))
    early_spec = pl.BlockSpec((2, 1, seq, LANES), lambda b: (0, b + first_pair, 0, 0))
    pre_spec = pl.BlockSpec((2, 1, seq, LANES), lambda b: (0, b, 0, 0))
    h_spec = pl.BlockSpec((1, seq, LANES), lambda b: (b, 0, 0))
    down_spec = pl.BlockSpec((SMALL, hidden), lambda b: (start // SMALL, 0))
    dw_shape = (2, SMALL, hidden)
    dw_spec = pl.BlockSpec(dw_shape, lambda b: (0, 0, 0))
    in_specs = [row_spec, pl.BlockSpec((1, 2, 1, seq, hidden), lambda b: (layer, 0, b + first_pair, 0, 0)), h_spec, h_spec, down_spec, down_spec]
    if finish:
        in_specs += [row_spec, early_spec, pl.BlockSpec(finish[2].shape, lambda b: (0, 0))]
    if init:
        in_specs += [dw_spec] * 2
    return pl.pallas_call(
        functools.partial(small_body, init is not None, finish is not None),
        out_shape=[jax.ShapeDtypeStruct(dw_shape, F32)] * 2
        + [jax.ShapeDtypeStruct(grad.shape if finish else (2, pairs, seq, LANES), BF16)],
        grid=(pairs,),
        in_specs=in_specs,
        out_specs=[dw_spec, dw_spec, row_spec if finish else pre_spec],
        compiler_params=pltpu.CompilerParams(dimension_semantics=("arbitrary",), vmem_limit_bytes=ALL_VMEM),
        cost_estimate=pl.CostEstimate(
            flops=24 * pairs * seq * hidden * SMALL, bytes_accessed=8 * pairs * seq * hidden, transcendentals=4 * pairs * seq * SMALL),
    )(grad, x_saved, *h_pair, *down_pair, *(finish or ()), *(init or ()))


def join_body(up_a, up_b, out_ref):
    first, second = swap_lanes(up_a[...].astype(F32), up_b[...].astype(F32))
    out_ref[:, :LANES], out_ref[:, LANES:] = first.astype(BF16), second.astype(BF16)


def join_call(up_pair, start):
    hidden = up_pair[0].shape[0]
    up_spec = pl.BlockSpec((hidden, LANES), lambda i: (0, start // LANES))
    return pl.pallas_call(
        join_body,
        out_shape=jax.ShapeDtypeStruct((hidden, 2 * LANES), BF16),
        grid=(1,),
        in_specs=[up_spec, up_spec],
        out_specs=pl.BlockSpec((hidden, 2 * LANES), lambda i: (0, 0)),
        compiler_params=pltpu.CompilerParams(dimension_semantics=("arbitrary",), vmem_limit_bytes=ALL_VMEM),
        cost_estimate=pl.CostEstimate(flops=hidden * LANES, bytes_accessed=8 * hidden * LANES, transcendentals=0),
    )(*up_pair)


def finish_body(carry_ref, pre_a, pre_b, up_ref, _, out_ref):
    total = carry_ref[0, 0] + dot(jnp.concatenate([pre_a[0, 0], pre_b[0, 0]], axis=1), up_ref[...], 1, 1)
    out_ref[0, 0] = total.astype(BF16)


def finish_call(carry, pre_pair, ups, first_pair, first_half, halves, out):
    _, _, seq, hidden = carry.shape
    count = pre_pair[1].shape[1]
    row_spec = pl.BlockSpec((1, 1, seq, hidden), lambda r, b: (r + first_half, b + first_pair, 0, 0))
    pre_specs = [pl.BlockSpec((1, 1, seq, LANES), lambda r, b, first=first: (r + first_half, b + first, 0, 0)) for first in (first_pair, 0)]
    rows = halves * count
    return pl.pallas_call(
        finish_body,
        out_shape=jax.ShapeDtypeStruct(carry.shape, BF16),
        grid=(halves, count),
        in_specs=[row_spec, *pre_specs, pl.BlockSpec(ups.shape, lambda r, b: (0, 0)), pl.BlockSpec(memory_space=pl.ANY)],
        out_specs=row_spec,
        input_output_aliases={4: 0},
        compiler_params=pltpu.CompilerParams(dimension_semantics=("arbitrary", "arbitrary"), vmem_limit_bytes=ALL_VMEM),
        cost_estimate=pl.CostEstimate(flops=4 * rows * seq * hidden * LANES, bytes_accessed=7 * rows * seq * hidden, transcendentals=0),
    )(carry, *pre_pair, ups, out)


def pair_body(first_ref, mine_ref, theirs_ref, stay_ref, away_ref):
    first = first_ref[0] == 1
    up, down = mine_ref[0] + theirs_ref[0], mine_ref[1] + theirs_ref[1]
    stay_ref[...] = jnp.where(first, up, down)
    away_ref[...] = jnp.where(first, down, up)


def pair_call(first, mine, theirs):
    _, size, hidden = mine.shape
    step = min(size, LANES)
    both_spec = pl.BlockSpec((2, step, hidden), lambda i, first: (0, i, 0))
    one_spec = pl.BlockSpec((step, hidden), lambda i, first: (i, 0))
    return pl.pallas_call(
        pair_body,
        out_shape=[jax.ShapeDtypeStruct((size, hidden), F32)] * 2,
        grid_spec=pltpu.PrefetchScalarGridSpec(
            num_scalar_prefetch=1, grid=(size // step,), in_specs=[both_spec] * 2, out_specs=[one_spec] * 2),
        compiler_params=pltpu.CompilerParams(dimension_semantics=("arbitrary",), vmem_limit_bytes=ALL_VMEM),
        cost_estimate=pl.CostEstimate(flops=4 * mine.size, bytes_accessed=12 * mine.size, transcendentals=0),
    )(first, mine, theirs)


def place_body(first_ref, kept_ref, other_ref, *refs):
    up_ref, down_ref = refs[-2:]
    first = first_ref[0] == 1
    kept, other = kept_ref[...], other_ref[...]
    up_ref[0] = jnp.where(first, kept, other).T
    down_ref[0] = jnp.where(first, other, kept)


def place_call(first, kept, other, layer, start, layers, width, bufs):
    size, hidden = kept.shape
    row_spec = pl.BlockSpec((LANES, hidden), lambda i, first: (i, 0))
    out_shape = [jax.ShapeDtypeStruct((layers, hidden, width), F32), jax.ShapeDtypeStruct((layers, width, hidden), F32)]
    any_spec = pl.BlockSpec(memory_space=pl.ANY)
    return pl.pallas_call(
        place_body,
        out_shape=out_shape,
        grid_spec=pltpu.PrefetchScalarGridSpec(
            num_scalar_prefetch=1,
            grid=(size // LANES,),
            in_specs=[row_spec, row_spec] + ([any_spec, any_spec] if bufs is not None else []),
            out_specs=[
                pl.BlockSpec((1, hidden, LANES), lambda i, first: (layer, 0, start // LANES + i)),
                pl.BlockSpec((1, LANES, hidden), lambda i, first: (layer, start // LANES + i, 0)),
            ],
        ),
        input_output_aliases={3: 0, 4: 1} if bufs is not None else {},
        compiler_params=pltpu.CompilerParams(dimension_semantics=("arbitrary",), vmem_limit_bytes=ALL_VMEM),
        cost_estimate=pl.CostEstimate(flops=4 * size * hidden, bytes_accessed=16 * size * hidden, transcendentals=0),
    )(first, kept, other, *(bufs or ()))


def join_place_body(count, layer, start, first_ref, *refs):
    up_out, down_out, up_ref, down_ref, sem = refs[-5:]
    first = first_ref[0] == 1
    kept = jnp.concatenate([r[...] for r in refs[:count]])
    other = jnp.concatenate([r[...] for r in refs[count : 2 * count]])
    size = kept.shape[0]
    down_ref[...] = jnp.where(first, other, kept)
    down_copy = pltpu.make_async_copy(down_ref, down_out.at[layer, pl.ds(start, size), :], sem.at[0])
    down_copy.start()
    up_ref[...] = jnp.where(first, kept, other).T
    up_copy = pltpu.make_async_copy(up_ref, up_out.at[layer, :, pl.ds(start, size)], sem.at[1])
    up_copy.start()
    down_copy.wait()
    up_copy.wait()


def join_place_call(first, pieces, layer, start, bufs):
    hidden = pieces[0][0].shape[1]
    size = sum(n for _, _, _, n in pieces)
    piece_specs = [pl.BlockSpec((n, hidden), lambda i, first, block=low // n: (block, 0)) for _, _, low, n in pieces]
    any_spec = pl.BlockSpec(memory_space=pl.ANY)
    count = len(pieces)
    return pl.pallas_call(
        functools.partial(join_place_body, count, layer, start),
        out_shape=[jax.ShapeDtypeStruct(b.shape, b.dtype) for b in bufs],
        grid_spec=pltpu.PrefetchScalarGridSpec(
            num_scalar_prefetch=1,
            grid=(1,),
            in_specs=piece_specs * 2 + [any_spec] * 2,
            out_specs=[any_spec] * 2,
            scratch_shapes=[pltpu.VMEM((hidden, size), F32), pltpu.VMEM((size, hidden), F32), pltpu.SemaphoreType.DMA((2,))],
        ),
        input_output_aliases={1 + 2 * count: 0, 2 + 2 * count: 1},
        compiler_params=pltpu.CompilerParams(dimension_semantics=("arbitrary",), vmem_limit_bytes=ALL_VMEM),
        cost_estimate=pl.CostEstimate(flops=4 * size * hidden, bytes_accessed=16 * size * hidden, transcendentals=0),
    )(first, *[p[0] for p in pieces], *[p[1] for p in pieces], *bufs)


def solution(mesh):
    n_model = mesh.shape["model"]

    def to_model(value, flip):
        return lax.ppermute(value, "model", [(i, i ^ flip) for i in range(n_model)])

    def to_data(value):
        return lax.ppermute(value, "data", [(0, 1), (1, 0)])

    def all_blocks(x_saved, h_saved, w_up, w_down, grad_out):
        me = lax.axis_index("model")
        first = lax.axis_index("data") == 0
        first_flag = jnp.reshape(first, (1,)).astype(jnp.int32)
        quarter = jnp.reshape(me, (1,)).astype(jnp.int32)
        layers = w_up.shape[0]
        rows, seq = grad_out.shape[:2]
        width = h_saved.shape[-1]

        held = [h_saved, None]

        def h_from(layer, flip, start=0, size=width):
            held[0], held[1] = lax.optimization_barrier((held[0], held[1]))
            begin = (me ^ flip) * seq
            held[1] = lax.dynamic_slice(held[0], (layer, 0, begin, start), (1, rows, seq, size))[0]
            return to_model(held[1], flip)

        head = jnp.where(first, w_up[1, :FIRST], w_down[1, :FIRST])
        w_pair = lax.optimization_barrier((w_up, w_down, head))
        held[1] = jnp.where(first, w_pair[0][1, FIRST:], w_pair[1][1, FIRST:])
        far_w = [None, jnp.concatenate([to_model(head, 2), to_model(held[1], 2)])]
        h_one = [h_from(1, 2), h_from(1, 3)]
        h_near = [None, h_from(1, 1)]
        w_pair = lax.optimization_barrier((w_up, w_down, held[1]))
        far_w[0] = jnp.where(first, w_pair[0][0], w_pair[1][0])
        far_w[0] = to_model(far_w[0], 2)
        h_near[0] = h_from(0, 1)
        h_zero = []
        for j, size in enumerate(BLOCKS):
            start = sum(BLOCKS[:j])
            h_zero.append([h_from(0, 2, start, size), h_from(0, 3, start, size)])
        small_start = width - LANES
        packed = []
        for flip in (2, 3):
            packed.append(pack_call(jnp.reshape(me ^ flip, (1,)).astype(jnp.int32), h_saved, 0, small_start, seq))
        h_small = [[to_model(packed[0][j], 2), to_model(packed[1][j], 3)] for j in range(3)]

        up, down = [{0: w_up} for _ in range(layers)], [{0: w_down} for _ in range(layers)]
        near_up, near_down = to_model(w_up, 1), to_model(w_down, 1)
        for layer in range(layers):
            other = to_data(far_w[layer])
            up[layer][1], down[layer][1] = near_up, near_down
            up[layer][2], down[layer][2] = jnp.where(first, far_w[layer], other), jnp.where(first, other, far_w[layer])
            up[layer][3] = to_model(up[layer][2], 1)
            down[layer][3] = to_model(down[layer][2], 1)

        def call(layer, grad, hs, flips, carry, final, start=0, size=width):
            ups, downs = [up[layer][f] for f in flips], [down[layer][f] for f in flips]
            return block_call(quarter, layer, grad, x_saved, hs, ups, downs, start, size, carry, final)

        def partial_sum(keep, give):
            theirs = to_model(give, 1)
            stay, away = pair_call(first_flag, keep, theirs)
            theirs = to_data(away)
            return stay + theirs

        def place(pieces, layer, start, bufs):
            if len(pieces) > 1:
                return join_place_call(first_flag, pieces, layer, start, bufs)
            return place_call(first_flag, *pieces[0], layer, start, layers, width, bufs)

        carry, dw_0, dw_1 = call(1, grad_out, [h_saved, h_near[1]], (0, 1), None, False)
        near = partial_sum(dw_0, dw_1)
        grad_mid, dw_2, dw_3 = call(1, grad_out, h_one, (2, 3), carry, True)
        far = partial_sum(dw_2, dw_3)
        near, part = lax.optimization_barrier(near), to_model(far, 2)
        kept = near + part
        bufs = place([(kept, to_data(kept))], 1, 0, None)

        carry, dw_0, dw_1 = call(0, grad_mid, [h_saved, h_near[0]], (0, 1), None, False)
        near = partial_sum(dw_0, dw_1)
        bounds = [0, 384, 448, 576, width - SMALL, width]
        near_part = lax.optimization_barrier(tuple(near[a:b] for a, b in zip(bounds, bounds[1:])))
        pieces = []

        def exchange(unit, far):
            part = to_model(far, 2)
            kept = near_part[unit] + part
            pieces.append((kept, to_data(kept)))

        down_pair, up_pair = [down[0][f] for f in (2, 3)], [up[0][f] for f in (2, 3)]
        small_up = join_call(up_pair, small_start)
        carry, dw_2, dw_3 = call(0, grad_mid, h_zero[0], (2, 3), carry, False, 0, BLOCKS[0])
        exchange(0, partial_sum(dw_2, dw_3))
        carry, dw_2, dw_3 = wide_call(0, grad_mid, x_saved, h_zero[1], up_pair, down_pair, BLOCKS[0], carry)
        far = partial_sum(dw_2, dw_3)
        exchange(1, far[: bounds[2] - bounds[1]])
        exchange(2, far[bounds[2] - bounds[1] : bounds[3] - bounds[1]])
        carry, grad_mid, x_saved = paired(carry), paired(grad_mid), paired(x_saved, 1)
        dw_2, dw_3, pre_1 = small_call(0, grad_mid, x_saved, h_small[0], down_pair, small_start, 0)
        exchange(3, jnp.concatenate([far[bounds[3] - bounds[1] :], partial_sum(dw_2, dw_3)]))
        last = small_start + SMALL
        early = CHUNKS[0]
        dw_2, dw_3, grad_x = small_call(
            0, grad_mid, x_saved, h_small[1], down_pair, last, 0, finish=(carry, pre_1, small_up))
        dw_2, dw_3, pre_2 = small_call(
            0, grad_mid, x_saved, h_small[2], down_pair, last, early, init=(dw_2, dw_3))
        exchange(4, partial_sum(dw_2, dw_3))
        grad_x = finish_call(carry, (pre_1, pre_2), small_up, early, 0, 2, grad_x)
        bufs = place([pieces[0]], 0, 0, bufs)
        middle = [(*pieces[1], 0, 64), (*pieces[2], 0, 128), (*pieces[3], 0, 64)]
        bufs = place(middle, 0, bounds[1], bufs)
        bufs = place([(*pieces[3], 64, 64), (*pieces[4], 0, 64)], 0, small_start, bufs)
        grad_x = grad_x.reshape(grad_out.shape)
        return grad_x, bufs[0], bufs[1]

    return jax.shard_map(
        all_blocks,
        mesh=mesh,
        in_specs=(P(None, "data", "model", None), P(None, "data", None, "model"), P(None, None, "model"), P(None, "model", None), P("data", "model", None)),
        out_specs=(P("data", "model", None), P(None, None, "model"), P(None, "model", None)),
        check_vma=False,
    )
```

```python
import functools

import jax
import jax.numpy as jnp
from jax import lax
from jax.experimental import pallas as pl
from jax.experimental.pallas import tpu as pltpu
from jax.sharding import PartitionSpec as P


BF16 = jnp.bfloat16
F32 = jnp.float32
BLOCKS = (384, 256)
LANES = 128
SMALL = 64
CHUNKS = (3, 3, 2)
FIRST = 192
ALL_VMEM = 66_000_000


def gelu_parts(pre_act):
    root = 0.7978845608028654
    cubic = (0.134145 * pre_act) * pre_act
    gate = 0.5 + 0.5 * jnp.tanh(pre_act * (root + (root / 3) * cubic))
    gelu_out = pre_act * gate
    gelu_slope = gate + gelu_out * (1.0 - gate) * (2 * root + (2 * root) * cubic)
    return gelu_out, gelu_slope


def dot(lhs, rhs, lhs_dim, rhs_dim):
    return lax.dot_general(lhs, rhs, (((lhs_dim,), (rhs_dim,)), ((), ())), preferred_element_type=F32)


def unit_grads(grad, h, down):
    d_act = dot(grad, down, 1, 1)
    gelu_out, gelu_slope = gelu_parts(h.astype(F32))
    return (d_act * gelu_slope).astype(BF16), gelu_out.astype(BF16)


def block_body(has_carry, final, rows, start, _, *refs):
    refs = list(refs)
    grad_ref, x_ref, h_a, h_b, up_a, up_b, down_a, down_b = (refs.pop(0) for _ in range(8))
    carry_ref = refs.pop(0) if has_carry else None
    out_ref, dw_a, dw_b, h_ref, pre_ref, act_ref, sum_ref, dw_ref, up_ref, down_ref, sem = refs
    row, source = pl.program_id(0), pl.program_id(1)
    width = pre_ref.shape[1]

    @pl.when((row == 0) & (source == 0))
    def _():
        dw_ref[...] = jnp.zeros_like(dw_ref)
        for s, (up, down) in enumerate(((up_a, down_a), (up_b, down_b))):
            up_ref[s] = up[(0,) * (len(up.shape) - 2) + (slice(None), slice(start, start + width))]
            down_ref[s] = down[(0,) * (len(down.shape) - 2) + (slice(start, start + width),)]

    for s, ref in enumerate((h_a, h_b)):
        @pl.when(source == s)
        def _():
            h_ref[...] = ref[(0,) * (len(ref.shape) - 2)]

    grad = grad_ref[0]
    x = x_ref[0, 0]
    for low in range(0, width, 256):
        cols = slice(low, min(low + 256, width))
        pre_ref[:, cols], act_ref[:, cols] = unit_grads(grad, h_ref[:, cols], down_ref[source, cols, :])
    pre, act = pre_ref[...], act_ref[...]
    dw_ref[source, 0] += dot(pre, x, 0, 0)
    dw_ref[source, 1] += dot(act, grad, 0, 0)
    part = dot(pre, up_ref[source], 1, 1)

    @pl.when(source == 0)
    def _():
        sum_ref[...] = part + carry_ref[0] if has_carry else part

    @pl.when(source == 1)
    def _():
        total = sum_ref[...] + part
        out_ref[0] = (grad.astype(F32) + total).astype(BF16) if final else total

    copies = [pltpu.make_async_copy(dw_ref.at[s], dw, sem.at[s]) for s, dw in enumerate((dw_a, dw_b))]
    for s in range(2):
        @pl.when((row == rows - 1) & (source == s))
        def _():
            copies[s].start()

    @pl.when((row == rows - 1) & (source == 1))
    def _():
        copies[0].wait()
        copies[1].wait()


def block_call(quarter, layer, grad, x_saved, h_pair, ups, downs, start, width, carry, final):
    rows, seq, hidden = grad.shape

    def h_spec(h):
        if h.ndim == 4:
            return pl.BlockSpec((1, 1, seq, width), lambda b, s, ids: (layer, b, ids[0], 0))
        return pl.BlockSpec((1, seq, width), lambda b, s, ids: (b, 0, 0))

    def w_spec(w):
        shape = (1,) * (w.ndim - 2) + w.shape[-2:]
        return pl.BlockSpec(shape, lambda b, s, ids: (layer,) * (w.ndim - 2) + (0, 0), pipeline_mode=pl.Buffered(1))

    row_spec = pl.BlockSpec((1, seq, hidden), lambda b, s, ids: (b, 0, 0))
    any_spec = pl.BlockSpec(memory_space=pl.ANY)
    in_specs = [row_spec, pl.BlockSpec((1, 1, seq, hidden), lambda b, s, ids: (layer, b, 0, 0))]
    in_specs += [h_spec(h) for h in h_pair]
    in_specs += [w_spec(w) for w in (*ups, *downs)]
    operands = [grad, x_saved, *h_pair, *ups, *downs]
    if carry is not None:
        in_specs.append(row_spec)
        operands.append(carry)
    dw_shape = (2, width, hidden)
    return pl.pallas_call(
        functools.partial(block_body, carry is not None, final, rows, start),
        out_shape=[jax.ShapeDtypeStruct(grad.shape, BF16 if final else F32)] + [jax.ShapeDtypeStruct(dw_shape, F32)] * 2,
        grid_spec=pltpu.PrefetchScalarGridSpec(
            num_scalar_prefetch=1,
            grid=(rows, 2),
            in_specs=in_specs,
            out_specs=[row_spec, any_spec, any_spec],
            scratch_shapes=[pltpu.VMEM((seq, width), BF16)] * 3
            + [pltpu.VMEM((seq, hidden), F32), pltpu.VMEM((2,) + dw_shape, F32)]
            + [pltpu.VMEM((2, hidden, width), BF16), pltpu.VMEM((2, width, hidden), BF16), pltpu.SemaphoreType.DMA((2,))],
        ),
        compiler_params=pltpu.CompilerParams(dimension_semantics=("arbitrary", "arbitrary"), vmem_limit_bytes=ALL_VMEM),
        cost_estimate=pl.CostEstimate(
            flops=16 * rows * seq * hidden * width, bytes_accessed=8 * rows * seq * hidden, transcendentals=2 * rows * seq * width),
    )(quarter, *operands)


def swap_lanes(a, b):
    left = lax.broadcasted_iota(jnp.int32, a.shape, 1) < SMALL
    return jnp.where(left, a, pltpu.roll(b, SMALL, 1)), jnp.where(left, pltpu.roll(a, SMALL, 1), b)


def pack_body(_, lo_ref, hi_ref, left_ref, *right_refs):
    left, right = swap_lanes(lo_ref[0, 0].astype(F32), hi_ref[0, 0].astype(F32))
    left_ref[0] = left.astype(BF16)
    for j, ref in enumerate(right_refs):
        low = sum(CHUNKS[:j])

        @pl.when((pl.program_id(0) >= low) & (pl.program_id(0) < low + CHUNKS[j]))
        def _():
            ref[0] = right.astype(BF16)


def pack_call(target, h_saved, layer, start, seq):
    pairs = h_saved.shape[1] // 2
    specs = [pl.BlockSpec((1, 1, seq, LANES), lambda b, ids, r=r: (layer, b + r * pairs, ids[0], start // LANES)) for r in range(2)]
    block = (1, seq, LANES)
    chunk_specs = [
        pl.BlockSpec(block, lambda b, ids, low=sum(CHUNKS[:j]), n=n: (jnp.clip(b - low, 0, n - 1), 0, 0)) for j, n in enumerate(CHUNKS)]
    return pl.pallas_call(
        pack_body,
        out_shape=[jax.ShapeDtypeStruct((n, seq, LANES), BF16) for n in (pairs, *CHUNKS)],
        grid_spec=pltpu.PrefetchScalarGridSpec(
            num_scalar_prefetch=1,
            grid=(pairs,),
            in_specs=specs,
            out_specs=[pl.BlockSpec(block, lambda b, ids: (b, 0, 0)), *chunk_specs],
        ),
        compiler_params=pltpu.CompilerParams(dimension_semantics=("arbitrary",), vmem_limit_bytes=ALL_VMEM),
        cost_estimate=pl.CostEstimate(flops=pairs * seq * LANES, bytes_accessed=8 * pairs * seq * LANES, transcendentals=0),
    )(target, h_saved, h_saved)


def wide_body(start, grad_ref, x_ref, h_a, h_b, up_a, up_b, down_a, down_b, carry_ref, out_ref, dw_a, dw_b):
    @pl.when(pl.program_id(0) == 0)
    def _():
        dw_a[...] = jnp.zeros_like(dw_a)
        dw_b[...] = jnp.zeros_like(dw_b)

    grad, x = grad_ref[0], x_ref[0, 0]
    cols = slice(start, start + h_a.shape[2])
    total = grad.astype(F32) + carry_ref[0]
    for h, up, down, dw in ((h_a, up_a, down_a, dw_a), (h_b, up_b, down_b, dw_b)):
        pre, act = unit_grads(grad, h[0], down[cols, :])
        dw[0] += dot(pre, x, 0, 0)
        dw[1] += dot(act, grad, 0, 0)
        total += dot(pre, up[:, cols], 1, 1)
    out_ref[0] = total


def wide_call(layer, grad, x_saved, h_pair, ups, downs, start, carry):
    rows, seq, hidden = grad.shape
    width = h_pair[0].shape[2]
    row_spec = pl.BlockSpec((1, seq, hidden), lambda b: (b, 0, 0))
    h_spec = pl.BlockSpec((1, seq, width), lambda b: (b, 0, 0))
    w_spec = pl.BlockSpec(ups[0].shape, lambda b: (0, 0), pipeline_mode=pl.Buffered(1))
    dw_shape = (2, width, hidden)
    return pl.pallas_call(
        functools.partial(wide_body, start),
        out_shape=[jax.ShapeDtypeStruct(grad.shape, F32)] + [jax.ShapeDtypeStruct(dw_shape, F32)] * 2,
        grid=(rows,),
        in_specs=[row_spec, pl.BlockSpec((1, 1, seq, hidden), lambda b: (layer, b, 0, 0)), h_spec, h_spec]
        + [w_spec] * 4 + [row_spec],
        out_specs=[row_spec] + [pl.BlockSpec(dw_shape, lambda b: (0, 0, 0), pipeline_mode=pl.Buffered(1))] * 2,
        compiler_params=pltpu.CompilerParams(dimension_semantics=("arbitrary",), vmem_limit_bytes=ALL_VMEM),
        cost_estimate=pl.CostEstimate(
            flops=16 * rows * seq * hidden * width, bytes_accessed=12 * rows * seq * hidden, transcendentals=2 * rows * seq * width),
    )(grad, x_saved, *h_pair, *ups, *downs, carry)


def small_body(has_init, finish, grad_ref, x_ref, h_a, h_b, down_a, down_b, *refs):
    refs = list(refs)
    carry_ref, early_ref, up_ref = (refs.pop(0) for _ in range(3)) if finish else (None,) * 3
    dw_pair, out_ref = refs[-3:-1], refs[-1]

    @pl.when(pl.program_id(0) == 0)
    def _():
        for i, dw in enumerate(dw_pair):
            dw[...] = refs[i][...] if has_init else jnp.zeros_like(dw)

    h_pair = swap_lanes(h_a[0].astype(F32), h_b[0].astype(F32))
    down = jnp.concatenate([down_a[...], down_b[...]])
    for r, h in enumerate(h_pair):
        grad, x = grad_ref[r, 0], x_ref[0, r, 0]
        pre, act = unit_grads(grad, h, down)
        for kind, part in enumerate((dot(pre, x, 0, 0), dot(act, grad, 0, 0))):
            dw_pair[0][kind] += part[:SMALL]
            dw_pair[1][kind] += part[SMALL:]
        if finish:
            total = carry_ref[r, 0] + dot(jnp.concatenate([early_ref[r, 0], pre], axis=1), up_ref[...], 1, 1)
            out_ref[r, 0] = total.astype(BF16)
        else:
            out_ref[r, 0] = pre


def paired(value, axis=0):
    shape = value.shape
    return value.reshape(shape[:axis] + (2, shape[axis] // 2) + shape[axis + 1 :])


def small_call(layer, grad, x_saved, h_pair, down_pair, start, first_pair, init=None, finish=None):
    _, _, seq, hidden = grad.shape
    pairs = h_pair[0].shape[0]
    row_spec = pl.BlockSpec((2, 1, seq, hidden), lambda b: (0, b + first_pair, 0, 0))
    early_spec = pl.BlockSpec((2, 1, seq, LANES), lambda b: (0, b + first_pair, 0, 0))
    pre_spec = pl.BlockSpec((2, 1, seq, LANES), lambda b: (0, b, 0, 0))
    h_spec = pl.BlockSpec((1, seq, LANES), lambda b: (b, 0, 0))
    down_spec = pl.BlockSpec((SMALL, hidden), lambda b: (start // SMALL, 0))
    dw_shape = (2, SMALL, hidden)
    dw_spec = pl.BlockSpec(dw_shape, lambda b: (0, 0, 0))
    in_specs = [row_spec, pl.BlockSpec((1, 2, 1, seq, hidden), lambda b: (layer, 0, b + first_pair, 0, 0)), h_spec, h_spec, down_spec, down_spec]
    if finish:
        in_specs += [row_spec, early_spec, pl.BlockSpec(finish[2].shape, lambda b: (0, 0))]
    if init:
        in_specs += [dw_spec] * 2
    return pl.pallas_call(
        functools.partial(small_body, init is not None, finish is not None),
        out_shape=[jax.ShapeDtypeStruct(dw_shape, F32)] * 2
        + [jax.ShapeDtypeStruct(grad.shape if finish else (2, pairs, seq, LANES), BF16)],
        grid=(pairs,),
        in_specs=in_specs,
        out_specs=[dw_spec, dw_spec, row_spec if finish else pre_spec],
        compiler_params=pltpu.CompilerParams(dimension_semantics=("arbitrary",), vmem_limit_bytes=ALL_VMEM),
        cost_estimate=pl.CostEstimate(
            flops=24 * pairs * seq * hidden * SMALL, bytes_accessed=8 * pairs * seq * hidden, transcendentals=4 * pairs * seq * SMALL),
    )(grad, x_saved, *h_pair, *down_pair, *(finish or ()), *(init or ()))


def join_body(up_a, up_b, out_ref):
    first, second = swap_lanes(up_a[...].astype(F32), up_b[...].astype(F32))
    out_ref[:, :LANES], out_ref[:, LANES:] = first.astype(BF16), second.astype(BF16)


def join_call(up_pair, start):
    hidden = up_pair[0].shape[0]
    up_spec = pl.BlockSpec((hidden, LANES), lambda i: (0, start // LANES))
    return pl.pallas_call(
        join_body,
        out_shape=jax.ShapeDtypeStruct((hidden, 2 * LANES), BF16),
        grid=(1,),
        in_specs=[up_spec, up_spec],
        out_specs=pl.BlockSpec((hidden, 2 * LANES), lambda i: (0, 0)),
        compiler_params=pltpu.CompilerParams(dimension_semantics=("arbitrary",), vmem_limit_bytes=ALL_VMEM),
        cost_estimate=pl.CostEstimate(flops=hidden * LANES, bytes_accessed=8 * hidden * LANES, transcendentals=0),
    )(*up_pair)


def finish_body(carry_ref, pre_a, pre_b, up_ref, _, out_ref):
    total = carry_ref[0, 0] + dot(jnp.concatenate([pre_a[0, 0], pre_b[0, 0]], axis=1), up_ref[...], 1, 1)
    out_ref[0, 0] = total.astype(BF16)


def finish_call(carry, pre_pair, ups, first_pair, first_half, halves, out):
    _, _, seq, hidden = carry.shape
    count = pre_pair[1].shape[1]
    row_spec = pl.BlockSpec((1, 1, seq, hidden), lambda r, b: (r + first_half, b + first_pair, 0, 0))
    pre_specs = [pl.BlockSpec((1, 1, seq, LANES), lambda r, b, first=first: (r + first_half, b + first, 0, 0)) for first in (first_pair, 0)]
    rows = halves * count
    return pl.pallas_call(
        finish_body,
        out_shape=jax.ShapeDtypeStruct(carry.shape, BF16),
        grid=(halves, count),
        in_specs=[row_spec, *pre_specs, pl.BlockSpec(ups.shape, lambda r, b: (0, 0)), pl.BlockSpec(memory_space=pl.ANY)],
        out_specs=row_spec,
        input_output_aliases={4: 0},
        compiler_params=pltpu.CompilerParams(dimension_semantics=("arbitrary", "arbitrary"), vmem_limit_bytes=ALL_VMEM),
        cost_estimate=pl.CostEstimate(flops=4 * rows * seq * hidden * LANES, bytes_accessed=7 * rows * seq * hidden, transcendentals=0),
    )(carry, *pre_pair, ups, out)


def pair_body(first_ref, mine_ref, theirs_ref, stay_ref, away_ref):
    first = first_ref[0] == 1
    up, down = mine_ref[0] + theirs_ref[0], mine_ref[1] + theirs_ref[1]
    stay_ref[...] = jnp.where(first, up, down)
    away_ref[...] = jnp.where(first, down, up)


def pair_call(first, mine, theirs):
    _, size, hidden = mine.shape
    step = min(size, LANES)
    both_spec = pl.BlockSpec((2, step, hidden), lambda i, first: (0, i, 0))
    one_spec = pl.BlockSpec((step, hidden), lambda i, first: (i, 0))
    return pl.pallas_call(
        pair_body,
        out_shape=[jax.ShapeDtypeStruct((size, hidden), F32)] * 2,
        grid_spec=pltpu.PrefetchScalarGridSpec(
            num_scalar_prefetch=1, grid=(size // step,), in_specs=[both_spec] * 2, out_specs=[one_spec] * 2),
        compiler_params=pltpu.CompilerParams(dimension_semantics=("arbitrary",), vmem_limit_bytes=ALL_VMEM),
        cost_estimate=pl.CostEstimate(flops=4 * mine.size, bytes_accessed=12 * mine.size, transcendentals=0),
    )(first, mine, theirs)


def place_body(first_ref, kept_ref, other_ref, *refs):
    up_ref, down_ref = refs[-2:]
    first = first_ref[0] == 1
    kept, other = kept_ref[...], other_ref[...]
    up_ref[0] = jnp.where(first, kept, other).T
    down_ref[0] = jnp.where(first, other, kept)


def place_call(first, kept, other, layer, start, layers, width, bufs):
    size, hidden = kept.shape
    row_spec = pl.BlockSpec((LANES, hidden), lambda i, first: (i, 0))
    out_shape = [jax.ShapeDtypeStruct((layers, hidden, width), F32), jax.ShapeDtypeStruct((layers, width, hidden), F32)]
    any_spec = pl.BlockSpec(memory_space=pl.ANY)
    return pl.pallas_call(
        place_body,
        out_shape=out_shape,
        grid_spec=pltpu.PrefetchScalarGridSpec(
            num_scalar_prefetch=1,
            grid=(size // LANES,),
            in_specs=[row_spec, row_spec] + ([any_spec, any_spec] if bufs is not None else []),
            out_specs=[
                pl.BlockSpec((1, hidden, LANES), lambda i, first: (layer, 0, start // LANES + i)),
                pl.BlockSpec((1, LANES, hidden), lambda i, first: (layer, start // LANES + i, 0)),
            ],
        ),
        input_output_aliases={3: 0, 4: 1} if bufs is not None else {},
        compiler_params=pltpu.CompilerParams(dimension_semantics=("arbitrary",), vmem_limit_bytes=ALL_VMEM),
        cost_estimate=pl.CostEstimate(flops=4 * size * hidden, bytes_accessed=16 * size * hidden, transcendentals=0),
    )(first, kept, other, *(bufs or ()))


def join_place_body(spans, layer, start, first_ref, *refs):
    count = len(spans)
    size = sum(n for _, n in spans)
    mine_ref, theirs_ref = refs[2 * count : 2 * count + 2]
    up_out, down_out, near_ref, far_ref, up_ref, down_ref, sem = refs[-7:]
    loads = [(ref.at[pl.ds(start, size)], near_ref.at[k]) for k, ref in enumerate((mine_ref, theirs_ref))]
    for k in range(2):
        place = 0
        for (low, n), ref in zip(spans, refs[k * count : (k + 1) * count]):
            loads.append((ref.at[pl.ds(low, n)], far_ref.at[k, pl.ds(place, n)]))
            place += n
    copies = [pltpu.make_async_copy(src, dst, sem.at[i]) for i, (src, dst) in enumerate(loads)]
    for copy in copies:
        copy.start()
    for copy in copies:
        copy.wait()
    first = first_ref[0] == 1
    kept, other = near_ref[0] + far_ref[0], near_ref[1] + far_ref[1]
    down_ref[...] = jnp.where(first, other, kept)
    down_copy = pltpu.make_async_copy(down_ref, down_out.at[layer, pl.ds(start, size), :], sem.at[0])
    down_copy.start()
    up_ref[...] = jnp.where(first, kept, other).T
    up_copy = pltpu.make_async_copy(up_ref, up_out.at[layer, :, pl.ds(start, size)], sem.at[1])
    up_copy.start()
    down_copy.wait()
    up_copy.wait()


def join_place_call(first, pieces, near_pair, layer, start, bufs):
    hidden = near_pair[0].shape[1]
    spans = [(low, n) for _, _, low, n in pieces]
    size = sum(n for _, n in spans)
    any_spec = pl.BlockSpec(memory_space=pl.ANY)
    count = 2 * len(pieces) + 2
    return pl.pallas_call(
        functools.partial(join_place_body, spans, layer, start),
        out_shape=[jax.ShapeDtypeStruct(b.shape, b.dtype) for b in bufs],
        grid_spec=pltpu.PrefetchScalarGridSpec(
            num_scalar_prefetch=1,
            grid=(1,),
            in_specs=[any_spec] * (count + 2),
            out_specs=[any_spec] * 2,
            scratch_shapes=[pltpu.VMEM((2, size, hidden), F32)] * 2
            + [pltpu.VMEM((hidden, size), F32), pltpu.VMEM((size, hidden), F32), pltpu.SemaphoreType.DMA((count,))],
        ),
        input_output_aliases={1 + count: 0, 2 + count: 1},
        compiler_params=pltpu.CompilerParams(dimension_semantics=("arbitrary",), vmem_limit_bytes=ALL_VMEM),
        cost_estimate=pl.CostEstimate(flops=4 * size * hidden, bytes_accessed=24 * size * hidden, transcendentals=0),
    )(first, *[p[0] for p in pieces], *[p[1] for p in pieces], *near_pair, *bufs)


def solution(mesh):
    n_model = mesh.shape["model"]

    def to_model(value, flip):
        return lax.ppermute(value, "model", [(i, i ^ flip) for i in range(n_model)])

    def to_data(value):
        return lax.ppermute(value, "data", [(0, 1), (1, 0)])

    def all_blocks(x_saved, h_saved, w_up, w_down, grad_out):
        me = lax.axis_index("model")
        first = lax.axis_index("data") == 0
        first_flag = jnp.reshape(first, (1,)).astype(jnp.int32)
        quarter = jnp.reshape(me, (1,)).astype(jnp.int32)
        layers = w_up.shape[0]
        rows, seq = grad_out.shape[:2]
        width = h_saved.shape[-1]

        held = [h_saved, None]

        def h_from(layer, flip, start=0, size=width):
            held[0], held[1] = lax.optimization_barrier((held[0], held[1]))
            begin = (me ^ flip) * seq
            held[1] = lax.dynamic_slice(held[0], (layer, 0, begin, start), (1, rows, seq, size))[0]
            return to_model(held[1], flip)

        head = jnp.where(first, w_up[1, :FIRST], w_down[1, :FIRST])
        w_pair = lax.optimization_barrier((w_up, w_down, head))
        held[1] = jnp.where(first, w_pair[0][1, FIRST:], w_pair[1][1, FIRST:])
        far_w = [None, jnp.concatenate([to_model(head, 2), to_model(held[1], 2)])]
        h_one = [h_from(1, 2), h_from(1, 3)]
        h_near = [None, h_from(1, 1)]
        w_pair = lax.optimization_barrier((w_up, w_down, held[1]))
        far_w[0] = jnp.where(first, w_pair[0][0], w_pair[1][0])
        far_w[0] = to_model(far_w[0], 2)
        h_near[0] = h_from(0, 1)
        h_zero = []
        for j, size in enumerate(BLOCKS):
            start = sum(BLOCKS[:j])
            h_zero.append([h_from(0, 2, start, size), h_from(0, 3, start, size)])
        small_start = width - LANES
        packed = []
        for flip in (2, 3):
            packed.append(pack_call(jnp.reshape(me ^ flip, (1,)).astype(jnp.int32), h_saved, 0, small_start, seq))
        h_small = [[to_model(packed[0][j], 2), to_model(packed[1][j], 3)] for j in range(4)]

        up, down = [{0: w_up} for _ in range(layers)], [{0: w_down} for _ in range(layers)]
        near_up, near_down = to_model(w_up, 1), to_model(w_down, 1)
        for layer in range(layers):
            other = to_data(far_w[layer])
            up[layer][1], down[layer][1] = near_up, near_down
            up[layer][2], down[layer][2] = jnp.where(first, far_w[layer], other), jnp.where(first, other, far_w[layer])
            up[layer][3] = to_model(up[layer][2], 1)
            down[layer][3] = to_model(down[layer][2], 1)

        def call(layer, grad, hs, flips, carry, final, start=0, size=width):
            ups, downs = [up[layer][f] for f in flips], [down[layer][f] for f in flips]
            return block_call(quarter, layer, grad, x_saved, hs, ups, downs, start, size, carry, final)

        def partial_sum(keep, give):
            theirs = to_model(give, 1)
            stay, away = pair_call(first_flag, keep, theirs)
            theirs = to_data(away)
            return stay + theirs

        def place(pieces, layer, start, bufs, near_pair=None):
            if near_pair is not None:
                return join_place_call(first_flag, pieces, near_pair, layer, start, bufs)
            return place_call(first_flag, *pieces[0], layer, start, layers, width, bufs)

        carry, dw_0, dw_1 = call(1, grad_out, [h_saved, h_near[1]], (0, 1), None, False)
        near = partial_sum(dw_0, dw_1)
        grad_mid, dw_2, dw_3 = call(1, grad_out, h_one, (2, 3), carry, True)
        far = partial_sum(dw_2, dw_3)
        near, part = lax.optimization_barrier(near), to_model(far, 2)
        kept = near + part
        bufs = place([(kept, to_data(kept))], 1, 0, None)

        carry, dw_0, dw_1 = call(0, grad_mid, [h_saved, h_near[0]], (0, 1), None, False)
        near = partial_sum(dw_0, dw_1)
        bounds = [0, 384, 448, 576, width - SMALL, width]
        near_pair = (near, to_data(near))
        pieces = []

        def exchange(far):
            part = to_model(far, 2)
            pieces.append((part, to_data(part)))

        down_pair, up_pair = [down[0][f] for f in (2, 3)], [up[0][f] for f in (2, 3)]
        small_up = join_call(up_pair, small_start)
        carry, dw_2, dw_3 = call(0, grad_mid, h_zero[0], (2, 3), carry, False, 0, BLOCKS[0])
        exchange(partial_sum(dw_2, dw_3))
        carry, dw_2, dw_3 = wide_call(0, grad_mid, x_saved, h_zero[1], up_pair, down_pair, BLOCKS[0], carry)
        far = partial_sum(dw_2, dw_3)
        exchange(far[: bounds[2] - bounds[1]])
        exchange(far[bounds[2] - bounds[1] : bounds[3] - bounds[1]])
        carry, grad_mid, x_saved = paired(carry), paired(grad_mid), paired(x_saved, 1)
        dw_2, dw_3, pre_1 = small_call(0, grad_mid, x_saved, h_small[0], down_pair, small_start, 0)
        exchange(jnp.concatenate([far[bounds[3] - bounds[1] :], partial_sum(dw_2, dw_3)]))
        last = small_start + SMALL
        early, late = CHUNKS[0], CHUNKS[0] + CHUNKS[1]
        dw_2, dw_3, grad_x = small_call(
            0, grad_mid, x_saved, h_small[1], down_pair, last, 0, finish=(carry, pre_1, small_up))
        dw_2, dw_3, pre_2 = small_call(
            0, grad_mid, x_saved, h_small[2], down_pair, last, early, init=(dw_2, dw_3))
        dw_2, dw_3, pre_3 = small_call(
            0, grad_mid, x_saved, h_small[3], down_pair, last, late, init=(dw_2, dw_3))
        exchange(partial_sum(dw_2, dw_3))
        grad_x = finish_call(carry, (pre_1, pre_2), small_up, early, 0, 2, grad_x)
        grad_x = finish_call(carry, (pre_1, pre_3), small_up, late, 0, 2, grad_x)
        bufs = place([(*pieces[0], 0, bounds[1])], 0, 0, bufs, near_pair)
        middle = [(*pieces[1], 0, 64), (*pieces[2], 0, 128), (*pieces[3], 0, 64)]
        bufs = place(middle, 0, bounds[1], bufs, near_pair)
        bufs = place([(*pieces[3], 64, 64), (*pieces[4], 0, 64)], 0, small_start, bufs, near_pair)
        grad_x = grad_x.reshape(grad_out.shape)
        return grad_x, bufs[0], bufs[1]

    return jax.shard_map(
        all_blocks,
        mesh=mesh,
        in_specs=(P(None, "data", "model", None), P(None, "data", None, "model"), P(None, None, "model"), P(None, "model", None), P("data", "model", None)),
        out_specs=(P("data", "model", None), P(None, None, "model"), P(None, "model", None)),
        check_vma=False,
    )
```

```python
import functools

import jax
import jax.numpy as jnp
from jax import lax
from jax.experimental import pallas as pl
from jax.experimental.pallas import tpu as pltpu
from jax.sharding import PartitionSpec as P


BF16 = jnp.bfloat16
F32 = jnp.float32
BLOCKS = (384, 256)
LANES = 128
SMALL = 64
CHUNKS = (3, 3, 2)
FIRST = 192
ALL_VMEM = 66_000_000


def gelu_parts(pre_act):
    root = 0.7978845608028654
    cubic = (0.134145 * pre_act) * pre_act
    gate = 0.5 + 0.5 * jnp.tanh(pre_act * (root + (root / 3) * cubic))
    gelu_out = pre_act * gate
    gelu_slope = gate + gelu_out * (1.0 - gate) * (2 * root + (2 * root) * cubic)
    return gelu_out, gelu_slope


def dot(lhs, rhs, lhs_dim, rhs_dim):
    return lax.dot_general(lhs, rhs, (((lhs_dim,), (rhs_dim,)), ((), ())), preferred_element_type=F32)


def unit_grads(grad, h, down):
    d_act = dot(grad, down, 1, 1)
    gelu_out, gelu_slope = gelu_parts(h.astype(F32))
    return (d_act * gelu_slope).astype(BF16), gelu_out.astype(BF16)


def block_body(has_carry, final, rows, start, _, *refs):
    refs = list(refs)
    grad_ref, x_ref, h_a, h_b, up_a, up_b, down_a, down_b = (refs.pop(0) for _ in range(8))
    carry_ref = refs.pop(0) if has_carry else None
    out_ref, dw_a, dw_b, h_ref, pre_ref, act_ref, sum_ref, dw_ref, up_ref, down_ref, sem = refs
    row, source = pl.program_id(0), pl.program_id(1)
    width = pre_ref.shape[1]

    @pl.when((row == 0) & (source == 0))
    def _():
        dw_ref[...] = jnp.zeros_like(dw_ref)
        for s, (up, down) in enumerate(((up_a, down_a), (up_b, down_b))):
            up_ref[s] = up[(0,) * (len(up.shape) - 2) + (slice(None), slice(start, start + width))]
            down_ref[s] = down[(0,) * (len(down.shape) - 2) + (slice(start, start + width),)]

    for s, ref in enumerate((h_a, h_b)):
        @pl.when(source == s)
        def _():
            h_ref[...] = ref[(0,) * (len(ref.shape) - 2)]

    grad = grad_ref[0]
    x = x_ref[0, 0]
    for low in range(0, width, 256):
        cols = slice(low, min(low + 256, width))
        pre_ref[:, cols], act_ref[:, cols] = unit_grads(grad, h_ref[:, cols], down_ref[source, cols, :])
    pre, act = pre_ref[...], act_ref[...]
    dw_ref[source, 0] += dot(pre, x, 0, 0)
    dw_ref[source, 1] += dot(act, grad, 0, 0)
    part = dot(pre, up_ref[source], 1, 1)

    @pl.when(source == 0)
    def _():
        sum_ref[...] = part + carry_ref[0] if has_carry else part

    @pl.when(source == 1)
    def _():
        total = sum_ref[...] + part
        out_ref[0] = (grad.astype(F32) + total).astype(BF16) if final else total

    copies = [pltpu.make_async_copy(dw_ref.at[s], dw, sem.at[s]) for s, dw in enumerate((dw_a, dw_b))]
    for s in range(2):
        @pl.when((row == rows - 1) & (source == s))
        def _():
            copies[s].start()

    @pl.when((row == rows - 1) & (source == 1))
    def _():
        copies[0].wait()
        copies[1].wait()


def block_call(quarter, layer, grad, x_saved, h_pair, ups, downs, start, width, carry, final):
    rows, seq, hidden = grad.shape

    def h_spec(h):
        if h.ndim == 4:
            return pl.BlockSpec((1, 1, seq, width), lambda b, s, ids: (layer, b, ids[0], 0))
        return pl.BlockSpec((1, seq, width), lambda b, s, ids: (b, 0, 0))

    def w_spec(w):
        shape = (1,) * (w.ndim - 2) + w.shape[-2:]
        return pl.BlockSpec(shape, lambda b, s, ids: (layer,) * (w.ndim - 2) + (0, 0), pipeline_mode=pl.Buffered(1))

    row_spec = pl.BlockSpec((1, seq, hidden), lambda b, s, ids: (b, 0, 0))
    any_spec = pl.BlockSpec(memory_space=pl.ANY)
    in_specs = [row_spec, pl.BlockSpec((1, 1, seq, hidden), lambda b, s, ids: (layer, b, 0, 0))]
    in_specs += [h_spec(h) for h in h_pair]
    in_specs += [w_spec(w) for w in (*ups, *downs)]
    operands = [grad, x_saved, *h_pair, *ups, *downs]
    if carry is not None:
        in_specs.append(row_spec)
        operands.append(carry)
    dw_shape = (2, width, hidden)
    return pl.pallas_call(
        functools.partial(block_body, carry is not None, final, rows, start),
        out_shape=[jax.ShapeDtypeStruct(grad.shape, BF16 if final else F32)] + [jax.ShapeDtypeStruct(dw_shape, F32)] * 2,
        grid_spec=pltpu.PrefetchScalarGridSpec(
            num_scalar_prefetch=1,
            grid=(rows, 2),
            in_specs=in_specs,
            out_specs=[row_spec, any_spec, any_spec],
            scratch_shapes=[pltpu.VMEM((seq, width), BF16)] * 3
            + [pltpu.VMEM((seq, hidden), F32), pltpu.VMEM((2,) + dw_shape, F32)]
            + [pltpu.VMEM((2, hidden, width), BF16), pltpu.VMEM((2, width, hidden), BF16), pltpu.SemaphoreType.DMA((2,))],
        ),
        compiler_params=pltpu.CompilerParams(dimension_semantics=("arbitrary", "arbitrary"), vmem_limit_bytes=ALL_VMEM),
        cost_estimate=pl.CostEstimate(
            flops=16 * rows * seq * hidden * width, bytes_accessed=8 * rows * seq * hidden, transcendentals=2 * rows * seq * width),
    )(quarter, *operands)


def swap_lanes(a, b):
    left = lax.broadcasted_iota(jnp.int32, a.shape, 1) < SMALL
    return jnp.where(left, a, pltpu.roll(b, SMALL, 1)), jnp.where(left, pltpu.roll(a, SMALL, 1), b)


def pack_body(_, lo_ref, hi_ref, left_ref, *right_refs):
    left, right = swap_lanes(lo_ref[0, 0].astype(F32), hi_ref[0, 0].astype(F32))
    left_ref[0] = left.astype(BF16)
    for j, ref in enumerate(right_refs):
        low = sum(CHUNKS[:j])

        @pl.when((pl.program_id(0) >= low) & (pl.program_id(0) < low + CHUNKS[j]))
        def _():
            ref[0] = right.astype(BF16)


def pack_call(target, h_saved, layer, start, seq):
    pairs = h_saved.shape[1] // 2
    specs = [pl.BlockSpec((1, 1, seq, LANES), lambda b, ids, r=r: (layer, b + r * pairs, ids[0], start // LANES)) for r in range(2)]
    block = (1, seq, LANES)
    chunk_specs = [
        pl.BlockSpec(block, lambda b, ids, low=sum(CHUNKS[:j]), n=n: (jnp.clip(b - low, 0, n - 1), 0, 0)) for j, n in enumerate(CHUNKS)]
    return pl.pallas_call(
        pack_body,
        out_shape=[jax.ShapeDtypeStruct((n, seq, LANES), BF16) for n in (pairs, *CHUNKS)],
        grid_spec=pltpu.PrefetchScalarGridSpec(
            num_scalar_prefetch=1,
            grid=(pairs,),
            in_specs=specs,
            out_specs=[pl.BlockSpec(block, lambda b, ids: (b, 0, 0)), *chunk_specs],
        ),
        compiler_params=pltpu.CompilerParams(dimension_semantics=("arbitrary",), vmem_limit_bytes=ALL_VMEM),
        cost_estimate=pl.CostEstimate(flops=pairs * seq * LANES, bytes_accessed=8 * pairs * seq * LANES, transcendentals=0),
    )(target, h_saved, h_saved)


def wide_body(start, grad_ref, x_ref, h_a, h_b, up_a, up_b, down_a, down_b, carry_ref, out_ref, dw_a, dw_b):
    @pl.when(pl.program_id(0) == 0)
    def _():
        dw_a[...] = jnp.zeros_like(dw_a)
        dw_b[...] = jnp.zeros_like(dw_b)

    grad, x = grad_ref[0], x_ref[0, 0]
    cols = slice(start, start + h_a.shape[2])
    total = grad.astype(F32) + carry_ref[0]
    for h, up, down, dw in ((h_a, up_a, down_a, dw_a), (h_b, up_b, down_b, dw_b)):
        pre, act = unit_grads(grad, h[0], down[cols, :])
        dw[0] += dot(pre, x, 0, 0)
        dw[1] += dot(act, grad, 0, 0)
        total += dot(pre, up[:, cols], 1, 1)
    out_ref[0] = total


def wide_call(layer, grad, x_saved, h_pair, ups, downs, start, carry):
    rows, seq, hidden = grad.shape
    width = h_pair[0].shape[2]
    row_spec = pl.BlockSpec((1, seq, hidden), lambda b: (b, 0, 0))
    h_spec = pl.BlockSpec((1, seq, width), lambda b: (b, 0, 0))
    w_spec = pl.BlockSpec(ups[0].shape, lambda b: (0, 0), pipeline_mode=pl.Buffered(1))
    dw_shape = (2, width, hidden)
    return pl.pallas_call(
        functools.partial(wide_body, start),
        out_shape=[jax.ShapeDtypeStruct(grad.shape, F32)] + [jax.ShapeDtypeStruct(dw_shape, F32)] * 2,
        grid=(rows,),
        in_specs=[row_spec, pl.BlockSpec((1, 1, seq, hidden), lambda b: (layer, b, 0, 0)), h_spec, h_spec]
        + [w_spec] * 4 + [row_spec],
        out_specs=[row_spec] + [pl.BlockSpec(dw_shape, lambda b: (0, 0, 0), pipeline_mode=pl.Buffered(1))] * 2,
        compiler_params=pltpu.CompilerParams(dimension_semantics=("arbitrary",), vmem_limit_bytes=ALL_VMEM),
        cost_estimate=pl.CostEstimate(
            flops=16 * rows * seq * hidden * width, bytes_accessed=12 * rows * seq * hidden, transcendentals=2 * rows * seq * width),
    )(grad, x_saved, *h_pair, *ups, *downs, carry)


def small_body(has_init, finish, grad_ref, x_ref, h_a, h_b, down_a, down_b, *refs):
    refs = list(refs)
    carry_ref, early_ref, up_ref = (refs.pop(0) for _ in range(3)) if finish else (None,) * 3
    dw_pair, out_ref = refs[-3:-1], refs[-1]

    @pl.when(pl.program_id(0) == 0)
    def _():
        for i, dw in enumerate(dw_pair):
            dw[...] = refs[i][...] if has_init else jnp.zeros_like(dw)

    h_pair = swap_lanes(h_a[0].astype(F32), h_b[0].astype(F32))
    down = jnp.concatenate([down_a[...], down_b[...]])
    for r, h in enumerate(h_pair):
        grad, x = grad_ref[r, 0], x_ref[0, r, 0]
        pre, act = unit_grads(grad, h, down)
        for kind, part in enumerate((dot(pre, x, 0, 0), dot(act, grad, 0, 0))):
            dw_pair[0][kind] += part[:SMALL]
            dw_pair[1][kind] += part[SMALL:]
        if finish:
            total = carry_ref[r, 0] + dot(jnp.concatenate([early_ref[r, 0], pre], axis=1), up_ref[...], 1, 1)
            out_ref[r, 0] = total.astype(BF16)
        else:
            out_ref[r, 0] = pre


def paired(value, axis=0):
    shape = value.shape
    return value.reshape(shape[:axis] + (2, shape[axis] // 2) + shape[axis + 1 :])


def small_call(layer, grad, x_saved, h_pair, down_pair, start, first_pair, init=None, finish=None, pre=None, pre_pairs=None, pre_first=0):
    _, _, seq, hidden = grad.shape
    pairs = h_pair[0].shape[0]
    row_spec = pl.BlockSpec((2, 1, seq, hidden), lambda b: (0, b + first_pair, 0, 0))
    early_spec = pl.BlockSpec((2, 1, seq, LANES), lambda b: (0, b + first_pair, 0, 0))
    pre_spec = pl.BlockSpec((2, 1, seq, LANES), lambda b: (0, b + pre_first, 0, 0))
    h_spec = pl.BlockSpec((1, seq, LANES), lambda b: (b, 0, 0))
    down_spec = pl.BlockSpec((SMALL, hidden), lambda b: (start // SMALL, 0))
    dw_shape = (2, SMALL, hidden)
    dw_spec = pl.BlockSpec(dw_shape, lambda b: (0, 0, 0))
    in_specs = [row_spec, pl.BlockSpec((1, 2, 1, seq, hidden), lambda b: (layer, 0, b + first_pair, 0, 0)), h_spec, h_spec, down_spec, down_spec]
    if finish:
        in_specs += [row_spec, early_spec, pl.BlockSpec(finish[2].shape, lambda b: (0, 0))]
    if init:
        in_specs += [dw_spec] * 2
    if pre is not None:
        in_specs.append(pl.BlockSpec(memory_space=pl.ANY))
    return pl.pallas_call(
        functools.partial(small_body, init is not None, finish is not None),
        out_shape=[jax.ShapeDtypeStruct(dw_shape, F32)] * 2
        + [jax.ShapeDtypeStruct(grad.shape if finish else (2, pre_pairs or pairs, seq, LANES), BF16)],
        grid=(pairs,),
        in_specs=in_specs,
        out_specs=[dw_spec, dw_spec, row_spec if finish else pre_spec],
        input_output_aliases={} if pre is None else {len(in_specs) - 1: 2},
        compiler_params=pltpu.CompilerParams(dimension_semantics=("arbitrary",), vmem_limit_bytes=ALL_VMEM),
        cost_estimate=pl.CostEstimate(
            flops=24 * pairs * seq * hidden * SMALL, bytes_accessed=8 * pairs * seq * hidden, transcendentals=4 * pairs * seq * SMALL),
    )(grad, x_saved, *h_pair, *down_pair, *(finish or ()), *(init or ()), *(() if pre is None else (pre,)))


def join_body(up_a, up_b, out_ref):
    first, second = swap_lanes(up_a[...].astype(F32), up_b[...].astype(F32))
    out_ref[:, :LANES], out_ref[:, LANES:] = first.astype(BF16), second.astype(BF16)


def join_call(up_pair, start):
    hidden = up_pair[0].shape[0]
    up_spec = pl.BlockSpec((hidden, LANES), lambda i: (0, start // LANES))
    return pl.pallas_call(
        join_body,
        out_shape=jax.ShapeDtypeStruct((hidden, 2 * LANES), BF16),
        grid=(1,),
        in_specs=[up_spec, up_spec],
        out_specs=pl.BlockSpec((hidden, 2 * LANES), lambda i: (0, 0)),
        compiler_params=pltpu.CompilerParams(dimension_semantics=("arbitrary",), vmem_limit_bytes=ALL_VMEM),
        cost_estimate=pl.CostEstimate(flops=hidden * LANES, bytes_accessed=8 * hidden * LANES, transcendentals=0),
    )(*up_pair)


def finish_body(carry_ref, pre_a, pre_b, up_ref, _, out_ref):
    total = carry_ref[0, 0] + dot(jnp.concatenate([pre_a[0, 0], pre_b[0, 0]], axis=1), up_ref[...], 1, 1)
    out_ref[0, 0] = total.astype(BF16)


def finish_call(carry, pre_pair, ups, first_pair, first_half, halves, out):
    _, _, seq, hidden = carry.shape
    count = pre_pair[1].shape[1]
    row_spec = pl.BlockSpec((1, 1, seq, hidden), lambda r, b: (r + first_half, b + first_pair, 0, 0))
    pre_specs = [pl.BlockSpec((1, 1, seq, LANES), lambda r, b, first=first: (r + first_half, b + first, 0, 0)) for first in (first_pair, 0)]
    rows = halves * count
    return pl.pallas_call(
        finish_body,
        out_shape=jax.ShapeDtypeStruct(carry.shape, BF16),
        grid=(halves, count),
        in_specs=[row_spec, *pre_specs, pl.BlockSpec(ups.shape, lambda r, b: (0, 0)), pl.BlockSpec(memory_space=pl.ANY)],
        out_specs=row_spec,
        input_output_aliases={4: 0},
        compiler_params=pltpu.CompilerParams(dimension_semantics=("arbitrary", "arbitrary"), vmem_limit_bytes=ALL_VMEM),
        cost_estimate=pl.CostEstimate(flops=4 * rows * seq * hidden * LANES, bytes_accessed=7 * rows * seq * hidden, transcendentals=0),
    )(carry, *pre_pair, ups, out)


def pair_body(first_ref, mine_ref, theirs_ref, stay_ref, away_ref):
    first = first_ref[0] == 1
    up, down = mine_ref[0] + theirs_ref[0], mine_ref[1] + theirs_ref[1]
    stay_ref[...] = jnp.where(first, up, down)
    away_ref[...] = jnp.where(first, down, up)


def pair_call(first, mine, theirs):
    _, size, hidden = mine.shape
    step = min(size, LANES)
    both_spec = pl.BlockSpec((2, step, hidden), lambda i, first: (0, i, 0))
    one_spec = pl.BlockSpec((step, hidden), lambda i, first: (i, 0))
    return pl.pallas_call(
        pair_body,
        out_shape=[jax.ShapeDtypeStruct((size, hidden), F32)] * 2,
        grid_spec=pltpu.PrefetchScalarGridSpec(
            num_scalar_prefetch=1, grid=(size // step,), in_specs=[both_spec] * 2, out_specs=[one_spec] * 2),
        compiler_params=pltpu.CompilerParams(dimension_semantics=("arbitrary",), vmem_limit_bytes=ALL_VMEM),
        cost_estimate=pl.CostEstimate(flops=4 * mine.size, bytes_accessed=12 * mine.size, transcendentals=0),
    )(first, mine, theirs)


def place_body(first_ref, kept_ref, other_ref, *refs):
    up_ref, down_ref = refs[-2:]
    first = first_ref[0] == 1
    kept, other = kept_ref[...], other_ref[...]
    up_ref[0] = jnp.where(first, kept, other).T
    down_ref[0] = jnp.where(first, other, kept)


def place_call(first, kept, other, layer, start, layers, width, bufs):
    size, hidden = kept.shape
    row_spec = pl.BlockSpec((LANES, hidden), lambda i, first: (i, 0))
    out_shape = [jax.ShapeDtypeStruct((layers, hidden, width), F32), jax.ShapeDtypeStruct((layers, width, hidden), F32)]
    any_spec = pl.BlockSpec(memory_space=pl.ANY)
    return pl.pallas_call(
        place_body,
        out_shape=out_shape,
        grid_spec=pltpu.PrefetchScalarGridSpec(
            num_scalar_prefetch=1,
            grid=(size // LANES,),
            in_specs=[row_spec, row_spec] + ([any_spec, any_spec] if bufs is not None else []),
            out_specs=[
                pl.BlockSpec((1, hidden, LANES), lambda i, first: (layer, 0, start // LANES + i)),
                pl.BlockSpec((1, LANES, hidden), lambda i, first: (layer, start // LANES + i, 0)),
            ],
        ),
        input_output_aliases={3: 0, 4: 1} if bufs is not None else {},
        compiler_params=pltpu.CompilerParams(dimension_semantics=("arbitrary",), vmem_limit_bytes=ALL_VMEM),
        cost_estimate=pl.CostEstimate(flops=4 * size * hidden, bytes_accessed=16 * size * hidden, transcendentals=0),
    )(first, kept, other, *(bufs or ()))


def join_place_body(spans, layer, start, first_ref, *refs):
    count = len(spans)
    size = sum(n for _, n in spans)
    mine_ref, theirs_ref = refs[2 * count : 2 * count + 2]
    up_out, down_out, near_ref, far_ref, up_ref, down_ref, sem = refs[-7:]
    loads = [(ref.at[pl.ds(start, size)], near_ref.at[k]) for k, ref in enumerate((mine_ref, theirs_ref))]
    for k in range(2):
        place = 0
        for (low, n), ref in zip(spans, refs[k * count : (k + 1) * count]):
            loads.append((ref.at[pl.ds(low, n)], far_ref.at[k, pl.ds(place, n)]))
            place += n
    copies = [pltpu.make_async_copy(src, dst, sem.at[i]) for i, (src, dst) in enumerate(loads)]
    for copy in copies:
        copy.start()
    for copy in copies:
        copy.wait()
    first = first_ref[0] == 1
    kept, other = near_ref[0] + far_ref[0], near_ref[1] + far_ref[1]
    down_ref[...] = jnp.where(first, other, kept)
    down_copy = pltpu.make_async_copy(down_ref, down_out.at[layer, pl.ds(start, size), :], sem.at[0])
    down_copy.start()
    up_ref[...] = jnp.where(first, kept, other).T
    up_copy = pltpu.make_async_copy(up_ref, up_out.at[layer, :, pl.ds(start, size)], sem.at[1])
    up_copy.start()
    down_copy.wait()
    up_copy.wait()


def join_place_call(first, pieces, near_pair, layer, start, bufs):
    hidden = near_pair[0].shape[1]
    spans = [(low, n) for _, _, low, n in pieces]
    size = sum(n for _, n in spans)
    any_spec = pl.BlockSpec(memory_space=pl.ANY)
    count = 2 * len(pieces) + 2
    return pl.pallas_call(
        functools.partial(join_place_body, spans, layer, start),
        out_shape=[jax.ShapeDtypeStruct(b.shape, b.dtype) for b in bufs],
        grid_spec=pltpu.PrefetchScalarGridSpec(
            num_scalar_prefetch=1,
            grid=(1,),
            in_specs=[any_spec] * (count + 2),
            out_specs=[any_spec] * 2,
            scratch_shapes=[pltpu.VMEM((2, size, hidden), F32)] * 2
            + [pltpu.VMEM((hidden, size), F32), pltpu.VMEM((size, hidden), F32), pltpu.SemaphoreType.DMA((count,))],
        ),
        input_output_aliases={1 + count: 0, 2 + count: 1},
        compiler_params=pltpu.CompilerParams(dimension_semantics=("arbitrary",), vmem_limit_bytes=ALL_VMEM),
        cost_estimate=pl.CostEstimate(flops=4 * size * hidden, bytes_accessed=24 * size * hidden, transcendentals=0),
    )(first, *[p[0] for p in pieces], *[p[1] for p in pieces], *near_pair, *bufs)


def solution(mesh):
    n_model = mesh.shape["model"]

    def to_model(value, flip):
        return lax.ppermute(value, "model", [(i, i ^ flip) for i in range(n_model)])

    def to_data(value):
        return lax.ppermute(value, "data", [(0, 1), (1, 0)])

    def all_blocks(x_saved, h_saved, w_up, w_down, grad_out):
        me = lax.axis_index("model")
        first = lax.axis_index("data") == 0
        first_flag = jnp.reshape(first, (1,)).astype(jnp.int32)
        quarter = jnp.reshape(me, (1,)).astype(jnp.int32)
        layers = w_up.shape[0]
        rows, seq = grad_out.shape[:2]
        width = h_saved.shape[-1]

        held = [h_saved, None]

        def h_from(layer, flip, start=0, size=width):
            held[0], held[1] = lax.optimization_barrier((held[0], held[1]))
            begin = (me ^ flip) * seq
            held[1] = lax.dynamic_slice(held[0], (layer, 0, begin, start), (1, rows, seq, size))[0]
            return to_model(held[1], flip)

        head = jnp.where(first, w_up[1, :FIRST], w_down[1, :FIRST])
        w_pair = lax.optimization_barrier((w_up, w_down, head))
        held[1] = jnp.where(first, w_pair[0][1, FIRST:], w_pair[1][1, FIRST:])
        far_w = [None, jnp.concatenate([to_model(head, 2), to_model(held[1], 2)])]
        h_one = [h_from(1, 2), h_from(1, 3)]
        h_near = [None, h_from(1, 1)]
        w_pair = lax.optimization_barrier((w_up, w_down, held[1]))
        far_w[0] = jnp.where(first, w_pair[0][0], w_pair[1][0])
        far_w[0] = to_model(far_w[0], 2)
        h_near[0] = h_from(0, 1)
        h_zero = []
        for j, size in enumerate(BLOCKS):
            start = sum(BLOCKS[:j])
            h_zero.append([h_from(0, 2, start, size), h_from(0, 3, start, size)])
        small_start = width - LANES
        packed = []
        for flip in (2, 3):
            packed.append(pack_call(jnp.reshape(me ^ flip, (1,)).astype(jnp.int32), h_saved, 0, small_start, seq))
        h_small = [[to_model(packed[0][j], 2), to_model(packed[1][j], 3)] for j in range(4)]

        up, down = [{0: w_up} for _ in range(layers)], [{0: w_down} for _ in range(layers)]
        near_up, near_down = to_model(w_up, 1), to_model(w_down, 1)
        for layer in range(layers):
            other = to_data(far_w[layer])
            up[layer][1], down[layer][1] = near_up, near_down
            up[layer][2], down[layer][2] = jnp.where(first, far_w[layer], other), jnp.where(first, other, far_w[layer])
            up[layer][3] = to_model(up[layer][2], 1)
            down[layer][3] = to_model(down[layer][2], 1)

        def call(layer, grad, hs, flips, carry, final, start=0, size=width):
            ups, downs = [up[layer][f] for f in flips], [down[layer][f] for f in flips]
            return block_call(quarter, layer, grad, x_saved, hs, ups, downs, start, size, carry, final)

        def partial_sum(keep, give):
            theirs = to_model(give, 1)
            stay, away = pair_call(first_flag, keep, theirs)
            theirs = to_data(away)
            return stay + theirs

        def place(pieces, layer, start, bufs, near_pair=None):
            if near_pair is not None:
                return join_place_call(first_flag, pieces, near_pair, layer, start, bufs)
            return place_call(first_flag, *pieces[0], layer, start, layers, width, bufs)

        carry, dw_0, dw_1 = call(1, grad_out, [h_saved, h_near[1]], (0, 1), None, False)
        near = partial_sum(dw_0, dw_1)
        grad_mid, dw_2, dw_3 = call(1, grad_out, h_one, (2, 3), carry, True)
        far = partial_sum(dw_2, dw_3)
        near, part = lax.optimization_barrier(near), to_model(far, 2)
        kept = near + part
        bufs = place([(kept, to_data(kept))], 1, 0, None)

        carry, dw_0, dw_1 = call(0, grad_mid, [h_saved, h_near[0]], (0, 1), None, False)
        near = partial_sum(dw_0, dw_1)
        bounds = [0, 384, 448, 576, width - SMALL, width]
        near_pair = (near, to_data(near))
        pieces = []

        def exchange(far):
            part = to_model(far, 2)
            pieces.append((part, to_data(part)))

        down_pair, up_pair = [down[0][f] for f in (2, 3)], [up[0][f] for f in (2, 3)]
        small_up = join_call(up_pair, small_start)
        carry, dw_2, dw_3 = call(0, grad_mid, h_zero[0], (2, 3), carry, False, 0, BLOCKS[0])
        exchange(partial_sum(dw_2, dw_3))
        carry, dw_2, dw_3 = wide_call(0, grad_mid, x_saved, h_zero[1], up_pair, down_pair, BLOCKS[0], carry)
        far = partial_sum(dw_2, dw_3)
        exchange(far[: bounds[2] - bounds[1]])
        exchange(far[bounds[2] - bounds[1] : bounds[3] - bounds[1]])
        carry, grad_mid, x_saved = paired(carry), paired(grad_mid), paired(x_saved, 1)
        dw_2, dw_3, pre_1 = small_call(0, grad_mid, x_saved, h_small[0], down_pair, small_start, 0)
        exchange(jnp.concatenate([far[bounds[3] - bounds[1] :], partial_sum(dw_2, dw_3)]))
        last = small_start + SMALL
        early, late = CHUNKS[0], CHUNKS[0] + CHUNKS[1]
        dw_2, dw_3, grad_x = small_call(
            0, grad_mid, x_saved, h_small[1], down_pair, last, 0, finish=(carry, pre_1, small_up))
        dw_2, dw_3, pre_2 = small_call(
            0, grad_mid, x_saved, h_small[2], down_pair, last, early, init=(dw_2, dw_3), pre_pairs=rows // 2 - early)
        dw_2, dw_3, pre_2 = small_call(
            0, grad_mid, x_saved, h_small[3], down_pair, last, late, init=(dw_2, dw_3),
            pre=pre_2, pre_pairs=rows // 2 - early, pre_first=late - early)
        exchange(partial_sum(dw_2, dw_3))
        grad_x = finish_call(carry, (pre_1, pre_2), small_up, early, 0, 2, grad_x)
        bufs = place([(*pieces[0], 0, bounds[1])], 0, 0, bufs, near_pair)
        middle = [(*pieces[1], 0, 64), (*pieces[2], 0, 128), (*pieces[3], 0, 64)]
        bufs = place(middle, 0, bounds[1], bufs, near_pair)
        bufs = place([(*pieces[3], 64, 64), (*pieces[4], 0, 64)], 0, small_start, bufs, near_pair)
        grad_x = grad_x.reshape(grad_out.shape)
        return grad_x, bufs[0], bufs[1]

    return jax.shard_map(
        all_blocks,
        mesh=mesh,
        in_specs=(P(None, "data", "model", None), P(None, "data", None, "model"), P(None, None, "model"), P(None, "model", None), P("data", "model", None)),
        out_specs=(P("data", "model", None), P(None, None, "model"), P(None, "model", None)),
        check_vma=False,
    )
```

```python
import functools

import jax
import jax.numpy as jnp
from jax import lax
from jax.experimental import pallas as pl
from jax.experimental.pallas import tpu as pltpu
from jax.sharding import PartitionSpec as P


BF16 = jnp.bfloat16
F32 = jnp.float32
BLOCKS = (384, 256)
LANES = 128
SMALL = 64
CHUNKS = (3, 3, 2)
FIRST = 192
ALL_VMEM = 66_000_000
TAIL_VMEM = 24 * 2**20


def gelu_parts(pre_act):
    root = 0.7978845608028654
    cubic = (0.134145 * pre_act) * pre_act
    gate = 0.5 + 0.5 * jnp.tanh(pre_act * (root + (root / 3) * cubic))
    gelu_out = pre_act * gate
    gelu_slope = gate + gelu_out * (1.0 - gate) * (2 * root + (2 * root) * cubic)
    return gelu_out, gelu_slope


def dot(lhs, rhs, lhs_dim, rhs_dim):
    return lax.dot_general(lhs, rhs, (((lhs_dim,), (rhs_dim,)), ((), ())), preferred_element_type=F32)


def unit_grads(grad, h, down):
    d_act = dot(grad, down, 1, 1)
    gelu_out, gelu_slope = gelu_parts(h.astype(F32))
    return (d_act * gelu_slope).astype(BF16), gelu_out.astype(BF16)


def block_body(has_carry, final, rows, start, _, *refs):
    refs = list(refs)
    grad_ref, x_ref, h_a, h_b, up_a, up_b, down_a, down_b = (refs.pop(0) for _ in range(8))
    carry_ref = refs.pop(0) if has_carry else None
    out_ref, dw_a, dw_b, h_ref, pre_ref, act_ref, sum_ref, dw_ref, up_ref, down_ref, sem = refs
    row, source = pl.program_id(0), pl.program_id(1)
    width = pre_ref.shape[1]

    @pl.when((row == 0) & (source == 0))
    def _():
        dw_ref[...] = jnp.zeros_like(dw_ref)
        for s, (up, down) in enumerate(((up_a, down_a), (up_b, down_b))):
            up_ref[s] = up[(0,) * (len(up.shape) - 2) + (slice(None), slice(start, start + width))]
            down_ref[s] = down[(0,) * (len(down.shape) - 2) + (slice(start, start + width),)]

    for s, ref in enumerate((h_a, h_b)):
        @pl.when(source == s)
        def _():
            h_ref[...] = ref[(0,) * (len(ref.shape) - 2)]

    grad = grad_ref[0]
    x = x_ref[0, 0]
    for low in range(0, width, 256):
        cols = slice(low, min(low + 256, width))
        pre_ref[:, cols], act_ref[:, cols] = unit_grads(grad, h_ref[:, cols], down_ref[source, cols, :])
    pre, act = pre_ref[...], act_ref[...]
    dw_ref[source, 0] += dot(pre, x, 0, 0)
    dw_ref[source, 1] += dot(act, grad, 0, 0)
    part = dot(pre, up_ref[source], 1, 1)

    @pl.when(source == 0)
    def _():
        sum_ref[...] = part + carry_ref[0] if has_carry else part

    @pl.when(source == 1)
    def _():
        total = sum_ref[...] + part
        out_ref[0] = (grad.astype(F32) + total).astype(BF16) if final else total

    copies = [pltpu.make_async_copy(dw_ref.at[s], dw, sem.at[s]) for s, dw in enumerate((dw_a, dw_b))]
    for s in range(2):
        @pl.when((row == rows - 1) & (source == s))
        def _():
            copies[s].start()

    @pl.when((row == rows - 1) & (source == 1))
    def _():
        copies[0].wait()
        copies[1].wait()


def block_call(quarter, layer, grad, x_saved, h_pair, ups, downs, start, width, carry, final):
    rows, seq, hidden = grad.shape

    def h_spec(h):
        if h.ndim == 4:
            return pl.BlockSpec((1, 1, seq, width), lambda b, s, ids: (layer, b, ids[0], 0))
        return pl.BlockSpec((1, seq, width), lambda b, s, ids: (b, 0, 0))

    def w_spec(w):
        shape = (1,) * (w.ndim - 2) + w.shape[-2:]
        return pl.BlockSpec(shape, lambda b, s, ids: (layer,) * (w.ndim - 2) + (0, 0), pipeline_mode=pl.Buffered(1))

    row_spec = pl.BlockSpec((1, seq, hidden), lambda b, s, ids: (b, 0, 0))
    any_spec = pl.BlockSpec(memory_space=pl.ANY)
    in_specs = [row_spec, pl.BlockSpec((1, 1, seq, hidden), lambda b, s, ids: (layer, b, 0, 0))]
    in_specs += [h_spec(h) for h in h_pair]
    in_specs += [w_spec(w) for w in (*ups, *downs)]
    operands = [grad, x_saved, *h_pair, *ups, *downs]
    if carry is not None:
        in_specs.append(row_spec)
        operands.append(carry)
    dw_shape = (2, width, hidden)
    return pl.pallas_call(
        functools.partial(block_body, carry is not None, final, rows, start),
        out_shape=[jax.ShapeDtypeStruct(grad.shape, BF16 if final else F32)] + [jax.ShapeDtypeStruct(dw_shape, F32)] * 2,
        grid_spec=pltpu.PrefetchScalarGridSpec(
            num_scalar_prefetch=1,
            grid=(rows, 2),
            in_specs=in_specs,
            out_specs=[row_spec, any_spec, any_spec],
            scratch_shapes=[pltpu.VMEM((seq, width), BF16)] * 3
            + [pltpu.VMEM((seq, hidden), F32), pltpu.VMEM((2,) + dw_shape, F32)]
            + [pltpu.VMEM((2, hidden, width), BF16), pltpu.VMEM((2, width, hidden), BF16), pltpu.SemaphoreType.DMA((2,))],
        ),
        compiler_params=pltpu.CompilerParams(dimension_semantics=("arbitrary", "arbitrary"), vmem_limit_bytes=ALL_VMEM),
        cost_estimate=pl.CostEstimate(
            flops=16 * rows * seq * hidden * width, bytes_accessed=8 * rows * seq * hidden, transcendentals=2 * rows * seq * width),
    )(quarter, *operands)


def swap_lanes(a, b):
    left = lax.broadcasted_iota(jnp.int32, a.shape, 1) < SMALL
    return jnp.where(left, a, pltpu.roll(b, SMALL, 1)), jnp.where(left, pltpu.roll(a, SMALL, 1), b)


def pack_body(_, lo_ref, hi_ref, left_ref, *right_refs):
    left, right = swap_lanes(lo_ref[0, 0].astype(F32), hi_ref[0, 0].astype(F32))
    left_ref[0] = left.astype(BF16)
    for j, ref in enumerate(right_refs):
        low = sum(CHUNKS[:j])

        @pl.when((pl.program_id(0) >= low) & (pl.program_id(0) < low + CHUNKS[j]))
        def _():
            ref[0] = right.astype(BF16)


def pack_call(target, h_saved, layer, start, seq):
    pairs = h_saved.shape[1] // 2
    specs = [pl.BlockSpec((1, 1, seq, LANES), lambda b, ids, r=r: (layer, b + r * pairs, ids[0], start // LANES)) for r in range(2)]
    block = (1, seq, LANES)
    chunk_specs = [
        pl.BlockSpec(block, lambda b, ids, low=sum(CHUNKS[:j]), n=n: (jnp.clip(b - low, 0, n - 1), 0, 0)) for j, n in enumerate(CHUNKS)]
    return pl.pallas_call(
        pack_body,
        out_shape=[jax.ShapeDtypeStruct((n, seq, LANES), BF16) for n in (pairs, *CHUNKS)],
        grid_spec=pltpu.PrefetchScalarGridSpec(
            num_scalar_prefetch=1,
            grid=(pairs,),
            in_specs=specs,
            out_specs=[pl.BlockSpec(block, lambda b, ids: (b, 0, 0)), *chunk_specs],
        ),
        compiler_params=pltpu.CompilerParams(dimension_semantics=("arbitrary",), vmem_limit_bytes=ALL_VMEM),
        cost_estimate=pl.CostEstimate(flops=pairs * seq * LANES, bytes_accessed=8 * pairs * seq * LANES, transcendentals=0),
    )(target, h_saved, h_saved)


def wide_body(start, grad_ref, x_ref, h_a, h_b, up_a, up_b, down_a, down_b, carry_ref, out_ref, dw_a, dw_b):
    @pl.when(pl.program_id(0) == 0)
    def _():
        dw_a[...] = jnp.zeros_like(dw_a)
        dw_b[...] = jnp.zeros_like(dw_b)

    grad, x = grad_ref[0], x_ref[0, 0]
    cols = slice(start, start + h_a.shape[2])
    total = grad.astype(F32) + carry_ref[0]
    for h, up, down, dw in ((h_a, up_a, down_a, dw_a), (h_b, up_b, down_b, dw_b)):
        pre, act = unit_grads(grad, h[0], down[cols, :])
        dw[0] += dot(pre, x, 0, 0)
        dw[1] += dot(act, grad, 0, 0)
        total += dot(pre, up[:, cols], 1, 1)
    out_ref[0] = total


def wide_call(layer, grad, x_saved, h_pair, ups, downs, start, carry):
    rows, seq, hidden = grad.shape
    width = h_pair[0].shape[2]
    row_spec = pl.BlockSpec((1, seq, hidden), lambda b: (b, 0, 0))
    h_spec = pl.BlockSpec((1, seq, width), lambda b: (b, 0, 0))
    w_spec = pl.BlockSpec(ups[0].shape, lambda b: (0, 0), pipeline_mode=pl.Buffered(1))
    dw_shape = (2, width, hidden)
    return pl.pallas_call(
        functools.partial(wide_body, start),
        out_shape=[jax.ShapeDtypeStruct(grad.shape, F32)] + [jax.ShapeDtypeStruct(dw_shape, F32)] * 2,
        grid=(rows,),
        in_specs=[row_spec, pl.BlockSpec((1, 1, seq, hidden), lambda b: (layer, b, 0, 0)), h_spec, h_spec]
        + [w_spec] * 4 + [row_spec],
        out_specs=[row_spec] + [pl.BlockSpec(dw_shape, lambda b: (0, 0, 0), pipeline_mode=pl.Buffered(1))] * 2,
        compiler_params=pltpu.CompilerParams(dimension_semantics=("arbitrary",), vmem_limit_bytes=ALL_VMEM),
        cost_estimate=pl.CostEstimate(
            flops=16 * rows * seq * hidden * width, bytes_accessed=12 * rows * seq * hidden, transcendentals=2 * rows * seq * width),
    )(grad, x_saved, *h_pair, *ups, *downs, carry)


def small_body(has_init, finish, grad_ref, x_ref, h_a, h_b, down_a, down_b, *refs):
    refs = list(refs)
    carry_ref, early_ref, up_ref = (refs.pop(0) for _ in range(3)) if finish else (None,) * 3
    dw_pair, out_ref = refs[-3:-1], refs[-1]

    @pl.when(pl.program_id(0) == 0)
    def _():
        for i, dw in enumerate(dw_pair):
            dw[...] = refs[i][...] if has_init else jnp.zeros_like(dw)

    h_pair = swap_lanes(h_a[0].astype(F32), h_b[0].astype(F32))
    down = jnp.concatenate([down_a[...], down_b[...]])
    for r, h in enumerate(h_pair):
        grad, x = grad_ref[r, 0], x_ref[0, r, 0]
        pre, act = unit_grads(grad, h, down)
        for kind, part in enumerate((dot(pre, x, 0, 0), dot(act, grad, 0, 0))):
            dw_pair[0][kind] += part[:SMALL]
            dw_pair[1][kind] += part[SMALL:]
        if finish:
            total = carry_ref[r, 0] + dot(jnp.concatenate([early_ref[r, 0], pre], axis=1), up_ref[...], 1, 1)
            out_ref[r, 0] = total.astype(BF16)
        else:
            out_ref[r, 0] = pre


def paired(value, axis=0):
    shape = value.shape
    return value.reshape(shape[:axis] + (2, shape[axis] // 2) + shape[axis + 1 :])


def small_call(layer, grad, x_saved, h_pair, down_pair, start, first_pair, init=None, finish=None, pre=None, pre_pairs=None, pre_first=0, vmem=TAIL_VMEM):
    _, _, seq, hidden = grad.shape
    pairs = h_pair[0].shape[0]
    row_spec = pl.BlockSpec((2, 1, seq, hidden), lambda b: (0, b + first_pair, 0, 0))
    early_spec = pl.BlockSpec((2, 1, seq, LANES), lambda b: (0, b + first_pair, 0, 0))
    pre_spec = pl.BlockSpec((2, 1, seq, LANES), lambda b: (0, b + pre_first, 0, 0))
    h_spec = pl.BlockSpec((1, seq, LANES), lambda b: (b, 0, 0))
    down_spec = pl.BlockSpec((SMALL, hidden), lambda b: (start // SMALL, 0))
    dw_shape = (2, SMALL, hidden)
    dw_spec = pl.BlockSpec(dw_shape, lambda b: (0, 0, 0))
    in_specs = [row_spec, pl.BlockSpec((1, 2, 1, seq, hidden), lambda b: (layer, 0, b + first_pair, 0, 0)), h_spec, h_spec, down_spec, down_spec]
    if finish:
        in_specs += [row_spec, early_spec, pl.BlockSpec(finish[2].shape, lambda b: (0, 0))]
    if init:
        in_specs += [dw_spec] * 2
    if pre is not None:
        in_specs.append(pl.BlockSpec(memory_space=pl.ANY))
    return pl.pallas_call(
        functools.partial(small_body, init is not None, finish is not None),
        out_shape=[jax.ShapeDtypeStruct(dw_shape, F32)] * 2
        + [jax.ShapeDtypeStruct(grad.shape if finish else (2, pre_pairs or pairs, seq, LANES), BF16)],
        grid=(pairs,),
        in_specs=in_specs,
        out_specs=[dw_spec, dw_spec, row_spec if finish else pre_spec],
        input_output_aliases={} if pre is None else {len(in_specs) - 1: 2},
        compiler_params=pltpu.CompilerParams(dimension_semantics=("arbitrary",), vmem_limit_bytes=vmem),
        cost_estimate=pl.CostEstimate(
            flops=24 * pairs * seq * hidden * SMALL, bytes_accessed=8 * pairs * seq * hidden, transcendentals=4 * pairs * seq * SMALL),
    )(grad, x_saved, *h_pair, *down_pair, *(finish or ()), *(init or ()), *(() if pre is None else (pre,)))


def join_body(up_a, up_b, out_ref):
    first, second = swap_lanes(up_a[...].astype(F32), up_b[...].astype(F32))
    out_ref[:, :LANES], out_ref[:, LANES:] = first.astype(BF16), second.astype(BF16)


def join_call(up_pair, start):
    hidden = up_pair[0].shape[0]
    up_spec = pl.BlockSpec((hidden, LANES), lambda i: (0, start // LANES))
    return pl.pallas_call(
        join_body,
        out_shape=jax.ShapeDtypeStruct((hidden, 2 * LANES), BF16),
        grid=(1,),
        in_specs=[up_spec, up_spec],
        out_specs=pl.BlockSpec((hidden, 2 * LANES), lambda i: (0, 0)),
        compiler_params=pltpu.CompilerParams(dimension_semantics=("arbitrary",), vmem_limit_bytes=TAIL_VMEM),
        cost_estimate=pl.CostEstimate(flops=hidden * LANES, bytes_accessed=8 * hidden * LANES, transcendentals=0),
    )(*up_pair)


def finish_body(carry_ref, pre_a, pre_b, up_ref, _, out_ref):
    total = carry_ref[0, 0] + dot(jnp.concatenate([pre_a[0, 0], pre_b[0, 0]], axis=1), up_ref[...], 1, 1)
    out_ref[0, 0] = total.astype(BF16)


def finish_call(carry, pre_pair, ups, first_pair, pairs, late_first, out):
    _, _, seq, hidden = carry.shape
    row_spec = pl.BlockSpec((1, 1, seq, hidden), lambda r, b: (r, b + first_pair, 0, 0))
    pre_specs = [pl.BlockSpec((1, 1, seq, LANES), lambda r, b, first=first: (r, b + first, 0, 0)) for first in (first_pair, first_pair - late_first)]
    rows = 2 * pairs
    return pl.pallas_call(
        finish_body,
        out_shape=jax.ShapeDtypeStruct(carry.shape, BF16),
        grid=(2, pairs),
        in_specs=[row_spec, *pre_specs, pl.BlockSpec(ups.shape, lambda r, b: (0, 0)), pl.BlockSpec(memory_space=pl.ANY)],
        out_specs=row_spec,
        input_output_aliases={4: 0},
        compiler_params=pltpu.CompilerParams(dimension_semantics=("arbitrary", "arbitrary"), vmem_limit_bytes=44 * 2**20),
        cost_estimate=pl.CostEstimate(flops=4 * rows * seq * hidden * LANES, bytes_accessed=7 * rows * seq * hidden, transcendentals=0),
    )(carry, *pre_pair, ups, out)


def pair_body(first_ref, mine_ref, theirs_ref, stay_ref, away_ref):
    first = first_ref[0] == 1
    up, down = mine_ref[0] + theirs_ref[0], mine_ref[1] + theirs_ref[1]
    stay_ref[...] = jnp.where(first, up, down)
    away_ref[...] = jnp.where(first, down, up)


def pair_call(first, mine, theirs):
    _, size, hidden = mine.shape
    step = min(size, LANES)
    both_spec = pl.BlockSpec((2, step, hidden), lambda i, first: (0, i, 0))
    one_spec = pl.BlockSpec((step, hidden), lambda i, first: (i, 0))
    return pl.pallas_call(
        pair_body,
        out_shape=[jax.ShapeDtypeStruct((size, hidden), F32)] * 2,
        grid_spec=pltpu.PrefetchScalarGridSpec(
            num_scalar_prefetch=1, grid=(size // step,), in_specs=[both_spec] * 2, out_specs=[one_spec] * 2),
        compiler_params=pltpu.CompilerParams(dimension_semantics=("arbitrary",), vmem_limit_bytes=TAIL_VMEM),
        cost_estimate=pl.CostEstimate(flops=4 * mine.size, bytes_accessed=12 * mine.size, transcendentals=0),
    )(first, mine, theirs)


def place_body(first_ref, kept_ref, other_ref, *refs):
    up_ref, down_ref = refs[-2:]
    first = first_ref[0] == 1
    kept, other = kept_ref[...], other_ref[...]
    up_ref[0] = jnp.where(first, kept, other).T
    down_ref[0] = jnp.where(first, other, kept)


def place_call(first, kept, other, layer, start, layers, width, bufs):
    size, hidden = kept.shape
    row_spec = pl.BlockSpec((LANES, hidden), lambda i, first: (i, 0))
    out_shape = [jax.ShapeDtypeStruct((layers, hidden, width), F32), jax.ShapeDtypeStruct((layers, width, hidden), F32)]
    any_spec = pl.BlockSpec(memory_space=pl.ANY)
    return pl.pallas_call(
        place_body,
        out_shape=out_shape,
        grid_spec=pltpu.PrefetchScalarGridSpec(
            num_scalar_prefetch=1,
            grid=(size // LANES,),
            in_specs=[row_spec, row_spec] + ([any_spec, any_spec] if bufs is not None else []),
            out_specs=[
                pl.BlockSpec((1, hidden, LANES), lambda i, first: (layer, 0, start // LANES + i)),
                pl.BlockSpec((1, LANES, hidden), lambda i, first: (layer, start // LANES + i, 0)),
            ],
        ),
        input_output_aliases={3: 0, 4: 1} if bufs is not None else {},
        compiler_params=pltpu.CompilerParams(dimension_semantics=("arbitrary",), vmem_limit_bytes=TAIL_VMEM),
        cost_estimate=pl.CostEstimate(flops=4 * size * hidden, bytes_accessed=16 * size * hidden, transcendentals=0),
    )(first, kept, other, *(bufs or ()))


def join_place_body(blocks, pieces, layer, start, first_ref, *refs):
    refs = list(refs)
    mine, theirs, kept_far, other_far = (jnp.concatenate([refs.pop(0)[...] for _ in range(n)]) for n in (blocks, blocks, pieces, pieces))
    up_out, down_out, up_ref, down_ref, sem = refs[-5:]
    size = mine.shape[0]
    first = first_ref[0] == 1
    kept, other = mine + kept_far, theirs + other_far
    down_ref[...] = jnp.where(first, other, kept)
    down_copy = pltpu.make_async_copy(down_ref, down_out.at[layer, pl.ds(start, size), :], sem.at[0])
    down_copy.start()
    up_ref[...] = jnp.where(first, kept, other).T
    up_copy = pltpu.make_async_copy(up_ref, up_out.at[layer, :, pl.ds(start, size)], sem.at[1])
    up_copy.start()
    down_copy.wait()
    up_copy.wait()


def join_place_call(first, pieces, near_pair, layer, start, bufs):
    hidden = near_pair[0].shape[1]
    size = sum(n for _, _, _, n in pieces)
    block = size if start % size == 0 else LANES
    near_specs = [pl.BlockSpec((block, hidden), lambda i, first, at=at: (at, 0)) for at in range(start // block, (start + size) // block)]
    piece_specs = [pl.BlockSpec((n, hidden), lambda i, first, at=low // n: (at, 0)) for _, _, low, n in pieces]
    any_spec = pl.BlockSpec(memory_space=pl.ANY)
    blocks, count = len(near_specs), len(pieces)
    operands = [near_pair[0]] * blocks + [near_pair[1]] * blocks + [p[0] for p in pieces] + [p[1] for p in pieces]
    return pl.pallas_call(
        functools.partial(join_place_body, blocks, count, layer, start),
        out_shape=[jax.ShapeDtypeStruct(b.shape, b.dtype) for b in bufs],
        grid_spec=pltpu.PrefetchScalarGridSpec(
            num_scalar_prefetch=1,
            grid=(1,),
            in_specs=near_specs * 2 + piece_specs * 2 + [any_spec] * 2,
            out_specs=[any_spec] * 2,
            scratch_shapes=[pltpu.VMEM((hidden, size), F32), pltpu.VMEM((size, hidden), F32), pltpu.SemaphoreType.DMA((2,))],
        ),
        input_output_aliases={1 + len(operands): 0, 2 + len(operands): 1},
        compiler_params=pltpu.CompilerParams(dimension_semantics=("arbitrary",), vmem_limit_bytes=TAIL_VMEM),
        cost_estimate=pl.CostEstimate(flops=4 * size * hidden, bytes_accessed=24 * size * hidden, transcendentals=0),
    )(first, *operands, *bufs)


def solution(mesh):
    n_model = mesh.shape["model"]

    def to_model(value, flip):
        return lax.ppermute(value, "model", [(i, i ^ flip) for i in range(n_model)])

    def to_data(value):
        return lax.ppermute(value, "data", [(0, 1), (1, 0)])

    def all_blocks(x_saved, h_saved, w_up, w_down, grad_out):
        me = lax.axis_index("model")
        first = lax.axis_index("data") == 0
        first_flag = jnp.reshape(first, (1,)).astype(jnp.int32)
        quarter = jnp.reshape(me, (1,)).astype(jnp.int32)
        layers = w_up.shape[0]
        rows, seq = grad_out.shape[:2]
        width = h_saved.shape[-1]

        held = [h_saved, None]

        def h_from(layer, flip, start=0, size=width):
            held[0], held[1] = lax.optimization_barrier((held[0], held[1]))
            begin = (me ^ flip) * seq
            held[1] = lax.dynamic_slice(held[0], (layer, 0, begin, start), (1, rows, seq, size))[0]
            return to_model(held[1], flip)

        head = jnp.where(first, w_up[1, :FIRST], w_down[1, :FIRST])
        w_pair = lax.optimization_barrier((w_up, w_down, head))
        held[1] = jnp.where(first, w_pair[0][1, FIRST:], w_pair[1][1, FIRST:])
        far_w = [None, jnp.concatenate([to_model(head, 2), to_model(held[1], 2)])]
        h_one = [h_from(1, 2), h_from(1, 3)]
        h_near = [None, h_from(1, 1)]
        w_pair = lax.optimization_barrier((w_up, w_down, held[1]))
        far_w[0] = jnp.where(first, w_pair[0][0], w_pair[1][0])
        far_w[0] = to_model(far_w[0], 2)
        h_near[0] = h_from(0, 1)
        h_zero = []
        for j, size in enumerate(BLOCKS):
            start = sum(BLOCKS[:j])
            h_zero.append([h_from(0, 2, start, size), h_from(0, 3, start, size)])
        small_start = width - LANES
        packed = []
        for flip in (2, 3):
            packed.append(pack_call(jnp.reshape(me ^ flip, (1,)).astype(jnp.int32), h_saved, 0, small_start, seq))
        h_small = [[to_model(packed[0][j], 2), to_model(packed[1][j], 3)] for j in range(4)]

        up, down = [{0: w_up} for _ in range(layers)], [{0: w_down} for _ in range(layers)]
        near_up, near_down = to_model(w_up, 1), to_model(w_down, 1)
        for layer in range(layers):
            other = to_data(far_w[layer])
            up[layer][1], down[layer][1] = near_up, near_down
            up[layer][2], down[layer][2] = jnp.where(first, far_w[layer], other), jnp.where(first, other, far_w[layer])
            up[layer][3] = to_model(up[layer][2], 1)
            down[layer][3] = to_model(down[layer][2], 1)

        def call(layer, grad, hs, flips, carry, final, start=0, size=width):
            ups, downs = [up[layer][f] for f in flips], [down[layer][f] for f in flips]
            return block_call(quarter, layer, grad, x_saved, hs, ups, downs, start, size, carry, final)

        def partial_sum(keep, give):
            theirs = to_model(give, 1)
            stay, away = pair_call(first_flag, keep, theirs)
            theirs = to_data(away)
            return stay + theirs

        def place(pieces, layer, start, bufs, near_pair=None):
            if near_pair is not None:
                return join_place_call(first_flag, pieces, near_pair, layer, start, bufs)
            return place_call(first_flag, *pieces[0], layer, start, layers, width, bufs)

        carry, dw_0, dw_1 = call(1, grad_out, [h_saved, h_near[1]], (0, 1), None, False)
        near = partial_sum(dw_0, dw_1)
        grad_mid, dw_2, dw_3 = call(1, grad_out, h_one, (2, 3), carry, True)
        far = partial_sum(dw_2, dw_3)
        near, part = lax.optimization_barrier(near), to_model(far, 2)
        kept = near + part
        bufs = place([(kept, to_data(kept))], 1, 0, None)

        carry, dw_0, dw_1 = call(0, grad_mid, [h_saved, h_near[0]], (0, 1), None, False)
        near = partial_sum(dw_0, dw_1)
        bounds = [0, 384, 448, 576, width - SMALL, width]
        near_pair = (near, to_data(near))
        pieces = []

        def exchange(far):
            part = to_model(far, 2)
            pieces.append((part, to_data(part)))

        down_pair, up_pair = [down[0][f] for f in (2, 3)], [up[0][f] for f in (2, 3)]
        small_up = join_call(up_pair, small_start)
        carry, dw_2, dw_3 = call(0, grad_mid, h_zero[0], (2, 3), carry, False, 0, BLOCKS[0])
        exchange(partial_sum(dw_2, dw_3))
        carry, dw_2, dw_3 = wide_call(0, grad_mid, x_saved, h_zero[1], up_pair, down_pair, BLOCKS[0], carry)
        far = partial_sum(dw_2, dw_3)
        exchange(far[: bounds[2] - bounds[1]])
        exchange(far[bounds[2] - bounds[1] : bounds[3] - bounds[1]])
        carry, grad_mid, x_saved = paired(carry), paired(grad_mid), paired(x_saved, 1)
        dw_2, dw_3, pre_1 = small_call(0, grad_mid, x_saved, h_small[0], down_pair, small_start, 0)
        exchange(jnp.concatenate([far[bounds[3] - bounds[1] :], partial_sum(dw_2, dw_3)]))
        last = small_start + SMALL
        early, late = CHUNKS[0], CHUNKS[0] + CHUNKS[1]
        dw_2, dw_3, grad_x = small_call(
            0, grad_mid, x_saved, h_small[1], down_pair, last, 0, finish=(carry, pre_1, small_up))
        dw_2, dw_3, pre_2 = small_call(
            0, grad_mid, x_saved, h_small[2], down_pair, last, early, init=(dw_2, dw_3), vmem=TAIL_VMEM, pre_pairs=rows // 2 - early)
        dw_2, dw_3, pre_2 = small_call(
            0, grad_mid[:, late:], x_saved[:1, :, late:], h_small[3], down_pair, last, 0, init=(dw_2, dw_3), vmem=TAIL_VMEM,
            pre=pre_2, pre_pairs=rows // 2 - early, pre_first=late - early)
        exchange(partial_sum(dw_2, dw_3))
        for first_pair, pairs in ((early, 2), (early + 2, rows // 2 - early - 2)):
            grad_x = finish_call(carry, (pre_1, pre_2), small_up, first_pair, pairs, early, grad_x)
        bufs = place([(*pieces[0], 0, bounds[1])], 0, 0, bufs, near_pair)
        middle = [(*pieces[1], 0, 64), (*pieces[2], 0, 128), (*pieces[3], 0, 64)]
        bufs = place(middle, 0, bounds[1], bufs, near_pair)
        bufs = place([(*pieces[3], 64, 64), (*pieces[4], 0, 64)], 0, small_start, bufs, near_pair)
        grad_x = grad_x.reshape(grad_out.shape)
        return grad_x, bufs[0], bufs[1]

    return jax.shard_map(
        all_blocks,
        mesh=mesh,
        in_specs=(P(None, "data", "model", None), P(None, "data", None, "model"), P(None, None, "model"), P(None, "model", None), P("data", "model", None)),
        out_specs=(P("data", "model", None), P(None, None, "model"), P(None, "model", None)),
        check_vma=False,
    )
```
